32 devices in a mesh: dp: 4 (over y, z), tp: 8 (over x, core).
Axes of the slice: x: 4, y: 2, z: 2, core: 2. Of those that a mesh axis runs over, the one named last changes fastest.
The devices are a block of a 4x4x8 slice.
Arguments:
- x_in: bfloat16 [8192, 2048], P(('dp', 'tp')), parts along dimension 0
- grad_y: bfloat16 [8192, 2048], P(('dp', 'tp')), parts along dimension 0
- norm_gain: float32 [2, 2048], replicated
- w_qkv: bfloat16 [2, 2048, 6144], P(None, None, 'tp')
- w_out: bfloat16 [2, 2048, 2048], P(None, 'tp')
- w_gate: bfloat16 [2, 2048, 8192], P(None, None, 'tp')
- w_up: bfloat16 [2, 2048, 8192], P(None, None, 'tp')
- w_down: bfloat16 [2, 8192, 2048], P(None, 'tp')
Outputs:
- output 1: bfloat16 [8192, 2048], P(('dp', 'tp')), parts along dimension 0
- output 2: float32 [8, 2048], P('dp'), parts along dimension 0
- output 3: bfloat16 [8, 2048, 6144], P('dp', None, 'tp'), parts along dimension 0
- output 4: bfloat16 [8, 2048, 2048], P('dp', 'tp'), parts along dimension 0
- output 5: bfloat16 [8, 2048, 8192], P('dp', None, 'tp'), parts along dimension 0
- output 6: bfloat16 [8, 2048, 8192], P('dp', None, 'tp'), parts along dimension 0
- output 7: bfloat16 [8, 8192, 2048], P('dp', 'tp'), parts along dimension 0
There are 4 independent parts. The reference program is written for one: setup_inputs(seed, part) draws one part's arguments, and reference() takes and returns one part's arrays. A program takes and returns all parts, laid end to end along the dimension named above; an argument that names none is the same for every part.
All inputs are finite; a program needn't handle non-finite values.
Results may differ from the reference program's by a relative error of at most 0.0158804.
Values are sent between devices in bfloat16 or wider.
A program may use at most 768 MiB of HBM per device.

```python
import jax
import jax.numpy as jnp
from jax import lax

SEQ_LEN = 2048
D_MODEL = 2048
D_FF = 8192
HEADS = 16
KV_HEADS = 16
HEAD_DIM = 128
LAYERS = 2

GROUP_SIZE = HEADS // KV_HEADS
QKV_COLS = (HEADS + 2 * KV_HEADS) * HEAD_DIM
NORM_EPS = 1e-5
ROPE_BASE = 10000.0


def setup_inputs(seed: int = 0, part: int = 0) -> dict:
    data_keys = jax.random.split(jax.random.fold_in(jax.random.key(seed), part), 2)
    weight_keys = jax.random.split(jax.random.key(seed + 1), 6)
    x_in = jax.random.normal(data_keys[0], (SEQ_LEN, D_MODEL), jnp.float32)
    grad_y = jax.random.normal(data_keys[1], (SEQ_LEN, D_MODEL), jnp.float32)
    norm_gain = 1.0 + 0.3 * jax.random.normal(weight_keys[0], (LAYERS, D_MODEL), jnp.float32)
    w_qkv = jax.random.normal(weight_keys[1], (LAYERS, D_MODEL, QKV_COLS), jnp.float32) * D_MODEL ** -0.5
    w_out = jax.random.normal(weight_keys[2], (LAYERS, HEADS * HEAD_DIM, D_MODEL), jnp.float32) * (HEADS * HEAD_DIM) ** -0.5
    w_gate = jax.random.normal(weight_keys[3], (LAYERS, D_MODEL, D_FF), jnp.float32) * D_MODEL ** -0.5
    w_up = jax.random.normal(weight_keys[4], (LAYERS, D_MODEL, D_FF), jnp.float32) * D_MODEL ** -0.5
    w_down = jax.random.normal(weight_keys[5], (LAYERS, D_FF, D_MODEL), jnp.float32) * D_FF ** -0.5
    return {'x_in': x_in.astype(jnp.bfloat16), 'grad_y': grad_y.astype(jnp.bfloat16), 'norm_gain': norm_gain, 'w_qkv': w_qkv.astype(jnp.bfloat16), 'w_out': w_out.astype(jnp.bfloat16), 'w_gate': w_gate.astype(jnp.bfloat16), 'w_up': w_up.astype(jnp.bfloat16), 'w_down': w_down.astype(jnp.bfloat16)}


def rope_tables():
    half_dim = HEAD_DIM // 2
    freqs = ROPE_BASE ** (-2.0 * jnp.arange(half_dim, dtype=jnp.float32) / HEAD_DIM)
    angles = jnp.arange(SEQ_LEN, dtype=jnp.float32)[:, None] * freqs[None, :]
    return jnp.cos(angles)[:, None, None, :], jnp.sin(angles)[:, None, None, :]


def rotate(values, cos_tab, sin_tab):
    half_dim = values.shape[-1] // 2
    lower_half = values[..., :half_dim]
    upper_half = values[..., half_dim:]
    return jnp.concatenate([lower_half * cos_tab - upper_half * sin_tab, upper_half * cos_tab + lower_half * sin_tab], axis=-1)


def rms_scale(x_f32, gain_row):
    inv_rms = lax.rsqrt(jnp.mean(x_f32 * x_f32, axis=-1, keepdims=True) + NORM_EPS)
    return x_f32 * inv_rms * gain_row


def group_attention(operands):
    query, keys_rot, values_v = operands
    causal = jnp.arange(SEQ_LEN)[:, None] >= jnp.arange(SEQ_LEN)[None, :]
    scores = jnp.einsum('sgd,td->gst', query.astype(jnp.float32), keys_rot.astype(jnp.float32)) * HEAD_DIM ** -0.5
    attn_prob = jax.nn.softmax(jnp.where(causal, scores, -1e30), axis=-1).astype(jnp.bfloat16)
    return jnp.einsum('gst,td->sgd', attn_prob.astype(jnp.float32), values_v.astype(jnp.float32)).astype(jnp.bfloat16)


def decoder_block(x_cur, gain_row, w_qkv_l, w_out_l, w_gate_l, w_up_l, w_down_l, cos_tab, sin_tab):
    x_f32 = x_cur.astype(jnp.float32)
    normed = rms_scale(x_f32, gain_row).astype(jnp.bfloat16).astype(jnp.float32)
    qkv_all = jnp.dot(normed, w_qkv_l.astype(jnp.float32), preferred_element_type=jnp.float32).astype(jnp.bfloat16)
    qkv_all = qkv_all.reshape(SEQ_LEN, KV_HEADS, GROUP_SIZE + 2, HEAD_DIM)
    rotated = rotate(qkv_all[:, :, :GROUP_SIZE + 1].astype(jnp.float32), cos_tab, sin_tab).astype(jnp.bfloat16)
    operands = (jnp.moveaxis(rotated[:, :, :GROUP_SIZE], 1, 0), jnp.moveaxis(rotated[:, :, GROUP_SIZE], 1, 0), jnp.moveaxis(qkv_all[:, :, GROUP_SIZE + 1], 1, 0))
    attn_out = lax.map(jax.checkpoint(group_attention), operands)
    attn_out = jnp.moveaxis(attn_out, 0, 1).reshape(SEQ_LEN, HEADS * HEAD_DIM)
    gate_act = jnp.dot(normed, w_gate_l.astype(jnp.float32), preferred_element_type=jnp.float32).astype(jnp.bfloat16)
    up_act = jnp.dot(normed, w_up_l.astype(jnp.float32), preferred_element_type=jnp.float32).astype(jnp.bfloat16)
    hidden = (jax.nn.silu(gate_act.astype(jnp.float32)) * up_act.astype(jnp.float32)).astype(jnp.bfloat16)
    block_sum = x_f32 + jnp.dot(attn_out.astype(jnp.float32), w_out_l.astype(jnp.float32), preferred_element_type=jnp.float32) + jnp.dot(hidden.astype(jnp.float32), w_down_l.astype(jnp.float32), preferred_element_type=jnp.float32)
    return block_sum.astype(jnp.bfloat16)


def stack_forward(x_in, norm_gain, w_qkv, w_out, w_gate, w_up, w_down):
    cos_tab, sin_tab = rope_tables()

    def body(x_cur, layer_weights):
        gain_row, w_qkv_l, w_out_l, w_gate_l, w_up_l, w_down_l = layer_weights
        return decoder_block(x_cur, gain_row, w_qkv_l, w_out_l, w_gate_l, w_up_l, w_down_l, cos_tab, sin_tab), None

    return lax.scan(body, x_in, (norm_gain, w_qkv, w_out, w_gate, w_up, w_down))[0]


def reference(x_in, grad_y, norm_gain, w_qkv, w_out, w_gate, w_up, w_down):
    pullback = jax.vjp(stack_forward, x_in, norm_gain, w_qkv, w_out, w_gate, w_up, w_down)[1]
    grad_x, grad_gain, grad_qkv, grad_out, grad_gate, grad_up, grad_down = pullback(grad_y)
    return (grad_x, grad_gain, grad_qkv, grad_out, grad_gate, grad_up, grad_down)
```

```python
import functools

import jax
import jax.numpy as jnp
import numpy as np
from jax import lax
from jax.experimental import pallas as pl
from jax.experimental.pallas import tpu as pltpu
from jax.sharding import PartitionSpec as P

HEAD_DIM = 128
NORM_EPS = 1e-5
ROPE_BASE = 10000.0
SCALE = HEAD_DIM ** -0.5
LOG2E = 1.4426950408889634
VMEM_LIMIT = 64000 * 1024
N_CHIPS = 4
SUBS = 4
BF16 = jnp.bfloat16
F32 = jnp.float32
ANY = pl.BlockSpec(memory_space=pl.ANY)
VMEM = pl.BlockSpec(memory_space=pltpu.VMEM)
NT = (((1,), (1,)), ((), ()))
TN = (((0,), (0,)), ((), ()))


def dot(lhs, rhs):
    return jnp.dot(lhs, rhs, preferred_element_type=F32)


def dot_nt(lhs, rhs):
    return lax.dot_general(lhs, rhs, NT, preferred_element_type=F32)


def dot_tn(lhs, rhs):
    return lax.dot_general(lhs, rhs, TN, preferred_element_type=F32)


def params(collective_id=None, semantics=None):
    if collective_id is None:
        return pltpu.CompilerParams(vmem_limit_bytes=VMEM_LIMIT, dimension_semantics=semantics)
    return pltpu.CompilerParams(vmem_limit_bytes=VMEM_LIMIT, collective_id=collective_id, has_side_effects=True)


def cost(flops, bytes_accessed, transcendentals=0):
    return pl.CostEstimate(flops=flops, bytes_accessed=bytes_accessed, transcendentals=transcendentals)


def rope_tables(seq_len):
    half_dim = HEAD_DIM // 2
    freqs = np.float32(ROPE_BASE) ** (np.float32(-2.0) * np.arange(half_dim, dtype=np.float32) / np.float32(HEAD_DIM))
    angles = np.arange(seq_len, dtype=np.float32)[:, None] * freqs[None, :].astype(np.float32)
    cos_half, sin_half = np.cos(angles).astype(np.float32), np.sin(angles).astype(np.float32)
    return np.concatenate([cos_half, cos_half], axis=1), np.concatenate([-sin_half, sin_half], axis=1)


def rotate(values, cos_tab, sin_tab):
    return values * cos_tab + pltpu.roll(values, HEAD_DIM // 2, 1) * sin_tab


def rms_scale(x_f32, gain_row):
    inv_rms = lax.rsqrt(jnp.mean(x_f32 * x_f32, axis=-1, keepdims=True) + NORM_EPS)
    return x_f32 * inv_rms * gain_row


def ring_place():
    me = lax.axis_index('tp')
    chip = me // 2
    core = me % 2
    return me, chip, core


def device_at(chip, core):
    return ((chip + N_CHIPS) % N_CHIPS) * 2 + core


def remote_copy(src, dst, send_sem, recv_sem, peer):
    return pltpu.make_async_remote_copy(
        src_ref=src, dst_ref=dst, send_sem=send_sem, recv_sem=recv_sem, device_id={'tp': peer}, device_id_type=pl.DeviceIdType.MESH
    )


def meet(peers):
    barrier = pltpu.get_barrier_semaphore()
    for peer in peers:
        pl.semaphore_signal(barrier, inc=1, device_id={'tp': peer}, device_id_type=pl.DeviceIdType.MESH)
    pl.semaphore_wait(barrier, len(peers))


def gather_shards(local_hbm, full, send_sems, recv_sems, local_sem, before, compute):
    me, chip, core = ring_place()
    turn = 1 - 2 * core
    partner = device_at(chip, 1 - core)
    ahead = device_at(chip + turn, core)
    behind = device_at(chip - turn, core)
    rows = full.shape[1] // SUBS

    def piece(kind, shard, sub, peer):
        part = full.at[shard, pl.ds(sub * rows, rows)]
        return remote_copy(part, part, send_sems.at[kind, sub], recv_sems.at[shard, sub], peer)

    def send(kind, shard, peer):
        for sub in range(SUBS):
            piece(kind, shard, sub, peer).start()

    def sent(kind, shard, peer, subs):
        for sub in subs:
            piece(kind, shard, sub, peer).wait_send()

    def arrived(shard, pass_on=None):
        for sub in range(SUBS):
            piece(0, shard, sub, partner).wait_recv()
            if pass_on is not None:
                piece(pass_on, shard, sub, partner).start()

    first = device_at(chip - turn, core)
    second = device_at(chip + turn, core)
    third = device_at(chip + 2, core)
    own = pltpu.make_async_copy(local_hbm, full.at[me], local_sem)
    own.start()
    meet((partner, ahead, behind))
    own.wait()
    send(1, me, ahead)
    send(0, me, partner)
    before()

    def step_body(step, carry):
        pair = step // 2
        odd = step % 2
        side = turn * (1 - 2 * odd)
        hop = (3 * pair + (pair // 2) * (2 * pair - 5)) % N_CHIPS
        shard = device_at((chip + side * hop + 2 * N_CHIPS) % N_CHIPS, (core + odd) % 2)

        @pl.when(step == 1)
        def _():
            arrived(partner)

        @pl.when(step == 2)
        def _():
            sent(1, me, ahead, range(SUBS - 1))
            send(2, me, behind)
            arrived(first, 3)

        @pl.when(step == 3)
        def _():
            arrived(device_at(chip + turn, 1 - core))

        @pl.when(step == 4)
        def _():
            sent(2, me, behind, range(SUBS - 1))
            send(4, first, ahead)
            arrived(second, 5)

        @pl.when(step == 5)
        def _():
            arrived(device_at(chip - turn, 1 - core))

        @pl.when(step == 6)
        def _():
            arrived(third, 6)

        @pl.when(step == 7)
        def _():
            arrived(device_at(chip + 2, 1 - core))

        compute(step, shard)
        return carry

    lax.fori_loop(0, 2 * N_CHIPS, step_body, 0)
    sent(0, me, partner, range(SUBS))
    sent(1, me, ahead, (SUBS - 1,))
    sent(2, me, behind, (SUBS - 1,))
    sent(3, first, partner, range(SUBS))
    sent(4, first, ahead, range(SUBS))
    sent(5, second, partner, range(SUBS))
    sent(6, third, partner, range(SUBS))


def gather_scratch(tp_size, rows, width):
    return [
        pltpu.VMEM((tp_size, rows, width), BF16),
        pltpu.SemaphoreType.DMA((7, SUBS)),
        pltpu.SemaphoreType.DMA((tp_size, SUBS)),
        pltpu.SemaphoreType.DMA,
    ]


class RowWriter:
    def __init__(self, stages, outs, sems, rows):
        self.stages, self.outs, self.sems, self.rows = stages, outs, sems, rows

    def copy(self, idx, slot, shard):
        start = pl.multiple_of(shard * self.rows, self.rows)
        return pltpu.make_async_copy(self.stages[idx].at[slot], self.outs[idx].at[pl.ds(start, self.rows)], self.sems.at[idx, slot])

    def reuse(self, step, shard):
        @pl.when(step >= 2)
        def _():
            for idx in range(len(self.outs)):
                self.copy(idx, step % 2, shard).wait()

    def start(self, step, shard):
        for idx in range(len(self.outs)):
            self.copy(idx, step % 2, shard).start()

    def finish(self):
        for idx in range(len(self.outs)):
            for slot in range(2):
                self.copy(idx, slot, 0).wait()


def project_kernel(layer, with_hidden, u_hbm, w_qkv_hbm, w_gate_hbm, w_up_hbm, cos_ref, sin_ref, *rest):
    n_out = 4 if with_hidden else 3
    outs, rest = rest[:n_out], rest[n_out:]
    stages, rest = rest[:n_out], rest[n_out:]
    w_qkv, w_gate, w_up, full, send_sems, recv_sems, local_sem, w_sems, out_sems = rest
    rows = full.shape[1]
    loads = [
        pltpu.make_async_copy(src.at[layer], dst, w_sems.at[idx])
        for idx, (src, dst) in enumerate(((w_qkv_hbm, w_qkv), (w_gate_hbm, w_gate), (w_up_hbm, w_up)))
    ]
    for load in loads:
        load.start()
    writer = RowWriter(stages, outs, out_sems, rows)

    def before():
        for load in loads:
            load.wait()

    def compute(step, shard):
        slot = step % 2
        writer.reuse(step, shard)
        u_rows = full[shard]
        table = pl.ds(pl.multiple_of(shard * rows, rows), rows)
        cos_tab, sin_tab = cos_ref[table], sin_ref[table]
        qkv = dot(u_rows, w_qkv[...]).astype(BF16)
        for head in range(w_qkv.shape[1] // HEAD_DIM):
            cols = slice(head * HEAD_DIM, (head + 1) * HEAD_DIM)
            part = qkv[:, cols]
            if head % 3 != 2:
                part = rotate(part.astype(F32), cos_tab, sin_tab).astype(BF16)
            stages[0][slot, :, cols] = part
        gate = dot(u_rows, w_gate[...]).astype(BF16)
        up = dot(u_rows, w_up[...]).astype(BF16)
        stages[1][slot] = gate
        stages[2][slot] = up
        if with_hidden:
            stages[3][slot] = (jax.nn.silu(gate.astype(F32)) * up.astype(F32)).astype(BF16)
        writer.start(step, shard)

    gather_shards(u_hbm, full, send_sems, recv_sems, local_sem, before, compute)
    writer.finish()


def project(u_loc, w_qkv, w_gate, w_up, tables, layer, tp_size, with_hidden):
    rows, width = u_loc.shape
    seq_len = rows * tp_size
    qkv_cols, ff_cols = w_qkv.shape[2], w_gate.shape[2]
    out_cols = [qkv_cols, ff_cols, ff_cols] + ([ff_cols] if with_hidden else [])
    outs = [jax.ShapeDtypeStruct((seq_len, cols), BF16) for cols in out_cols]
    scratch = [pltpu.VMEM((2, rows, cols), BF16) for cols in out_cols]
    scratch += [pltpu.VMEM((width, cols), BF16) for cols in (qkv_cols, ff_cols, ff_cols)]
    scratch += gather_scratch(tp_size, rows, width)
    scratch += [pltpu.SemaphoreType.DMA((3,)), pltpu.SemaphoreType.DMA((len(outs), 2))]
    total = qkv_cols + 2 * ff_cols
    return pl.pallas_call(
        functools.partial(project_kernel, layer, with_hidden),
        out_shape=outs,
        in_specs=[ANY] * 4 + [VMEM] * 2,
        out_specs=[ANY] * len(outs),
        scratch_shapes=scratch,
        compiler_params=params(collective_id=1 + layer),
        cost_estimate=cost(2 * seq_len * width * total, 2 * (width * total + seq_len * total)),
        name=f'project_{layer}',
    )(u_loc, w_qkv, w_gate, w_up, *tables)


def down_kernel(layer, dy_hbm, w_out_hbm, w_down_hbm, gate_hbm, up_hbm, *rest):
    outs, rest = rest[:5], rest[5:]
    stages, rest = rest[:4], rest[4:]
    gate_in, up_in, w_out, w_down, full, send_sems, recv_sems, local_sem, w_sems, out_sems, in_sems, full_sems = rest
    rows = full.shape[1]
    loads = [
        pltpu.make_async_copy(src.at[layer], dst, w_sems.at[idx])
        for idx, (src, dst) in enumerate(((w_out_hbm, w_out), (w_down_hbm, w_down)))
    ]
    for load in loads:
        load.start()
    writer = RowWriter(stages, outs[:4], out_sems, rows)
    dy_full = outs[4]

    def before():
        for load in loads:
            load.wait()

    def keep(shard):
        return pltpu.make_async_copy(full.at[shard], dy_full.at[pl.ds(pl.multiple_of(shard * rows, rows), rows)], full_sems.at[shard])

    def compute(step, shard):
        slot = step % 2
        here = pl.ds(pl.multiple_of(shard * rows, rows), rows)
        fetch = [pltpu.make_async_copy(src.at[here], dst, in_sems.at[idx]) for idx, (src, dst) in enumerate(((gate_hbm, gate_in), (up_hbm, up_in)))]
        for item in fetch:
            item.start()
        keep(shard).start()
        writer.reuse(step, shard)
        dy_rows = full[shard]
        stages[0][slot] = dot_nt(dy_rows, w_out[...]).astype(BF16)
        d_hidden = dot_nt(dy_rows, w_down[...]).astype(BF16).astype(F32)
        for item in fetch:
            item.wait()
        gate, up = gate_in[...].astype(F32), up_in[...].astype(F32)
        sig = jax.nn.sigmoid(gate)
        act = gate * sig
        stages[1][slot] = (act * up).astype(BF16)
        stages[2][slot] = (d_hidden * up * (sig + act * (1.0 - sig))).astype(BF16)
        stages[3][slot] = (d_hidden * act).astype(BF16)
        writer.start(step, shard)

    gather_shards(dy_hbm, full, send_sems, recv_sems, local_sem, before, compute)
    writer.finish()
    for shard in range(full.shape[0]):
        keep(shard).wait()


def down_backward(dy_loc, w_out, w_down, gate_act, up_act, layer, tp_size):
    rows, width = dy_loc.shape
    seq_len = rows * tp_size
    head_cols, ff_cols = w_out.shape[1], w_down.shape[1]
    out_cols = [head_cols, ff_cols, ff_cols, ff_cols]
    outs = [jax.ShapeDtypeStruct((seq_len, cols), BF16) for cols in out_cols + [width]]
    scratch = [pltpu.VMEM((2, rows, cols), BF16) for cols in out_cols]
    scratch += [pltpu.VMEM((rows, ff_cols), BF16)] * 2
    scratch += [pltpu.VMEM((cols, width), BF16) for cols in (head_cols, ff_cols)]
    scratch += gather_scratch(tp_size, rows, width)
    scratch += [pltpu.SemaphoreType.DMA((2,)), pltpu.SemaphoreType.DMA((4, 2)), pltpu.SemaphoreType.DMA((2,)), pltpu.SemaphoreType.DMA((tp_size,))]
    total = head_cols + ff_cols
    return pl.pallas_call(
        functools.partial(down_kernel, layer),
        out_shape=outs,
        in_specs=[ANY] * 5,
        out_specs=[ANY] * 5,
        scratch_shapes=scratch,
        compiler_params=params(collective_id=3 + layer),
        cost_estimate=cost(2 * seq_len * width * total, 2 * (width * total + 3 * seq_len * total)),
        name=f'down_backward_{layer}',
    )(dy_loc, w_out, w_down, gate_act, up_act)


def scatter_blocks(blocks_each, load_block, product, tmp, acc, ring, pair_send, pair_recv, ring_send, ring_recv):
    me, chip, core = ring_place()
    partner = device_at(chip, 1 - core)
    right, left = device_at(chip + 1, core), device_at(chip - 1, core)
    per_step = 2 * blocks_each
    n_blocks = N_CHIPS * per_step
    slots = tmp.shape[0]
    meet((partner, right, left))

    def place(block):
        step = block // per_step
        way = block % 2
        dest = (chip + (1 + step) * (2 * way - 1) + 2 * N_CHIPS) % N_CHIPS
        cols = way * blocks_each + (block % per_step) // 2
        return step, way, dest, cols

    def to_partner(block):
        return remote_copy(tmp.at[block % slots, 1 - core], acc.at[block], pair_send.at[block % slots], pair_recv.at[block], partner)

    def to_next(block):
        way = block % 2
        peer = device_at(chip + 1 - 2 * way, core)
        return remote_copy(acc.at[block], ring.at[block], ring_send.at[block], ring_recv.at[block], peer)

    def body(block, carry):
        @pl.when(block < n_blocks)
        def _():
            step, way, dest, cols = place(block)
            load_block(block)

            @pl.when(block >= slots)
            def _():
                to_partner(block - slots).wait_send()

            product(dest, cols, tmp.at[block % slots])
            to_partner(block).start()

        @pl.when(block >= 1)
        def _():
            last = block - 1
            to_partner(last).wait_recv()

            @pl.when(last < per_step)
            def _():
                acc[last] = acc[last] + tmp[last % slots, core]

            @pl.when(last >= per_step)
            def _():
                to_next(last - per_step).wait_recv()
                acc[last] = (acc[last] + tmp[last % slots, core]) + ring[last - per_step]

            @pl.when(last < n_blocks - per_step)
            def _():
                to_next(last).start()

        return carry

    lax.fori_loop(0, n_blocks + 1, body, 0)
    for block in range(n_blocks - slots, n_blocks):
        to_partner(block).wait_send()
    for block in range(n_blocks - per_step):
        to_next(block).wait_send()
    return lambda cols: acc.at[n_blocks - per_step + 2 * (cols % blocks_each) + cols // blocks_each]


def scatter_scratch(blocks_each, rows, width):
    per_step = 2 * blocks_each
    n_blocks = N_CHIPS * per_step
    cols = width // per_step
    return [
        pltpu.VMEM((3, 2, rows, cols), F32),
        pltpu.VMEM((n_blocks, rows, cols), F32),
        pltpu.VMEM((n_blocks - per_step, rows, cols), F32),
        pltpu.SemaphoreType.DMA((3,)),
        pltpu.SemaphoreType.DMA((n_blocks,)),
        pltpu.SemaphoreType.DMA((n_blocks - per_step,)),
        pltpu.SemaphoreType.DMA((n_blocks - per_step,)),
    ]


BLOCKS_EACH = 2
ROWS_AT_ONCE = 32


def row_loads(pairs, sems, rows, chip):
    def load(order, hop):
        span = pl.ds(pl.multiple_of(((chip + hop) % N_CHIPS) * rows, rows), rows)
        return [pltpu.make_async_copy(src.at[span], dst.at[span], sems.at[idx, order]) for idx, (src, dst) in enumerate(pairs)]

    return [load(order, hop) for order, hop in enumerate((3, 1, 2, 0))]


def forward_kernel(layer, next_gain, o_hbm, m_hbm, w_out_hbm, w_down_hbm, x_ref, gain_ref, y_ref, u_ref, o_all, m_all, w_out, w_down, row_sems, w_sems, *scatter):
    me, chip, core = ring_place()
    per_step = 2 * BLOCKS_EACH
    rows = x_ref.shape[0]
    width = x_ref.shape[1]
    block_cols = width // per_step
    loads = row_loads(((o_hbm, o_all), (m_hbm, m_all)), row_sems, 2 * rows, chip)

    def w_load(cols):
        span = pl.ds(cols * block_cols, block_cols)
        return [
            pltpu.make_async_copy(src.at[layer, :, span], dst.at[cols], w_sems.at[idx, cols])
            for idx, (src, dst) in enumerate(((w_out_hbm, w_out), (w_down_hbm, w_down)))
        ]

    order = [way * BLOCKS_EACH + j for j in range(BLOCKS_EACH) for way in range(2)]
    for block, cols in enumerate(order):
        for item in w_load(cols):
            item.start()
        if block < 2:
            for item in loads[block]:
                item.start()
    for block in range(2, 4):
        for item in loads[block]:
            item.start()

    def load_block(block):
        for idx, cols in enumerate(order):
            @pl.when(block == idx)
            def _():
                for item in w_load(cols):
                    item.wait()

        for idx, at in enumerate((0, 1, per_step, 3 * per_step)):
            @pl.when(block == at)
            def _():
                for item in loads[idx]:
                    item.wait()

    def product(dest, cols, out):
        span = pl.ds(pl.multiple_of(dest * 2 * rows, 2 * rows), 2 * rows)
        total = dot(o_all[span], w_out[cols]) + dot(m_all[span], w_down[cols])
        out[0] = total[:rows]
        out[1] = total[rows:]

    result = scatter_blocks(BLOCKS_EACH, load_block, product, *scatter)

    def finish(idx, carry):
        span = pl.ds(pl.multiple_of(idx * ROWS_AT_ONCE, ROWS_AT_ONCE), ROWS_AT_ONCE)
        summed = jnp.concatenate([result(cols)[span] for cols in range(per_step)], axis=1)
        y = (x_ref[span].astype(F32) + summed).astype(BF16)
        y_ref[span] = y
        u_ref[span] = rms_scale(y.astype(F32), gain_ref[next_gain:next_gain + 1]).astype(BF16)
        return carry

    lax.fori_loop(0, rows // ROWS_AT_ONCE, finish, 0)


def block_output(attn_out, hidden, w_out, w_down, x_loc, norm_gain, layer):
    rows, width = x_loc.shape
    seq_len = attn_out.shape[0]
    head_cols, ff_cols = w_out.shape[1], w_down.shape[1]
    per_step = 2 * BLOCKS_EACH
    cols = width // per_step
    shard = jax.ShapeDtypeStruct((rows, width), BF16)
    return pl.pallas_call(
        functools.partial(forward_kernel, layer, layer + 1),
        out_shape=[shard, shard],
        in_specs=[ANY] * 4 + [VMEM] * 2,
        out_specs=[VMEM] * 2,
        scratch_shapes=[
            pltpu.VMEM((seq_len, head_cols), BF16),
            pltpu.VMEM((seq_len, ff_cols), BF16),
            pltpu.VMEM((per_step, head_cols, cols), BF16),
            pltpu.VMEM((per_step, ff_cols, cols), BF16),
            pltpu.SemaphoreType.DMA((2, 4)),
            pltpu.SemaphoreType.DMA((2, per_step)),
        ] + scatter_scratch(BLOCKS_EACH, rows, width),
        compiler_params=params(collective_id=5 + layer),
        cost_estimate=cost(2 * seq_len * width * (head_cols + ff_cols), 4 * seq_len * (head_cols + ff_cols)),
        name=f'block_output_{layer}',
    )(attn_out, hidden, w_out, w_down, x_loc, norm_gain)


def backward_kernel(layer, dqkv_hbm, dgate_hbm, dup_hbm, w_qkv_hbm, w_gate_hbm, w_up_hbm, x_ref, dy_ref, gain_ref, dx_ref, dgain_ref, *rest):
    acts, rest = rest[:3], rest[3:]
    weights, rest = rest[:3], rest[3:]
    row_sems, w_sems, *scatter = rest
    me, chip, core = ring_place()
    per_step = 2 * BLOCKS_EACH
    rows, width = x_ref.shape
    block_cols = width // per_step
    loads = row_loads(list(zip((dqkv_hbm, dgate_hbm, dup_hbm), acts)), row_sems, 2 * rows, chip)

    def w_load(cols):
        span = pl.ds(cols * block_cols, block_cols)
        return [
            pltpu.make_async_copy(src.at[layer, span], dst.at[span], w_sems.at[idx, cols])
            for idx, (src, dst) in enumerate(zip((w_qkv_hbm, w_gate_hbm, w_up_hbm), weights))
        ]

    order = [way * BLOCKS_EACH + j for j in range(BLOCKS_EACH) for way in range(2)]
    for block, cols in enumerate(order):
        for item in w_load(cols):
            item.start()
        if block < 2:
            for item in loads[block]:
                item.start()
    for block in range(2, 4):
        for item in loads[block]:
            item.start()

    def load_block(block):
        for idx, cols in enumerate(order):
            @pl.when(block == idx)
            def _():
                for item in w_load(cols):
                    item.wait()

        for idx, at in enumerate((0, 1, per_step, 3 * per_step)):
            @pl.when(block == at)
            def _():
                for item in loads[idx]:
                    item.wait()

    def product(dest, cols, out):
        span = pl.ds(pl.multiple_of(dest * 2 * rows, 2 * rows), 2 * rows)
        w_span = pl.ds(pl.multiple_of(cols * block_cols, block_cols), block_cols)
        total = dot_nt(acts[0][span], weights[0][w_span]) + dot_nt(acts[1][span], weights[1][w_span]) + dot_nt(acts[2][span], weights[2][w_span])
        out[0] = total[:rows]
        out[1] = total[rows:]

    result = scatter_blocks(BLOCKS_EACH, load_block, product, *scatter)
    gain_row = gain_ref[layer:layer + 1]
    dgain_ref[...] = jnp.zeros_like(dgain_ref)

    def finish(idx, carry):
        span = pl.ds(pl.multiple_of(idx * ROWS_AT_ONCE, ROWS_AT_ONCE), ROWS_AT_ONCE)
        summed = jnp.concatenate([result(cols)[span] for cols in range(per_step)], axis=1)
        d_normed = summed.astype(BF16).astype(F32)
        x_f32 = x_ref[span].astype(F32)
        inv_rms = lax.rsqrt(jnp.mean(x_f32 * x_f32, axis=-1, keepdims=True) + NORM_EPS)
        scaled = d_normed * gain_row
        dgain_ref[...] += jnp.sum(d_normed * (x_f32 * inv_rms), axis=0, keepdims=True)
        mix = jnp.mean(scaled * x_f32, axis=-1, keepdims=True) * (inv_rms * inv_rms * inv_rms)
        dx_ref[span] = (dy_ref[span].astype(F32) + (scaled * inv_rms - x_f32 * mix)).astype(BF16)
        return carry

    lax.fori_loop(0, rows // ROWS_AT_ONCE, finish, 0)


def block_input_backward(d_qkv, d_gate, d_up, w_qkv, w_gate, w_up, x_loc, dy_loc, norm_gain, layer):
    rows, width = x_loc.shape
    seq_len = d_qkv.shape[0]
    all_cols = (w_qkv.shape[2], w_gate.shape[2], w_up.shape[2])
    per_step = 2 * BLOCKS_EACH
    return pl.pallas_call(
        functools.partial(backward_kernel, layer),
        out_shape=[jax.ShapeDtypeStruct((rows, width), BF16), jax.ShapeDtypeStruct((1, width), F32)],
        in_specs=[ANY] * 6 + [VMEM] * 3,
        out_specs=[VMEM] * 2,
        scratch_shapes=[pltpu.VMEM((seq_len, cols), BF16) for cols in all_cols]
        + [pltpu.VMEM((width, cols), BF16) for cols in all_cols]
        + [pltpu.SemaphoreType.DMA((3, 4)), pltpu.SemaphoreType.DMA((3, per_step))]
        + scatter_scratch(BLOCKS_EACH, rows, width),
        compiler_params=params(collective_id=7 + layer),
        cost_estimate=cost(2 * seq_len * width * sum(all_cols), 4 * seq_len * sum(all_cols)),
        name=f'block_input_backward_{layer}',
    )(d_qkv, d_gate, d_up, w_qkv, w_gate, w_up, x_loc, dy_loc, norm_gain)


Q_ROWS = 256


def causal_tile(size):
    return lax.broadcasted_iota(jnp.int32, (size, size), 0) >= lax.broadcasted_iota(jnp.int32, (size, size), 1)


def masked_scores(query, keys, q_start):
    size = query.shape[0]
    scores = dot_nt(query, keys[:q_start + size])
    diagonal = jnp.where(causal_tile(size), scores[:, q_start:], -1e30)
    return diagonal if q_start == 0 else jnp.concatenate([scores[:, :q_start], diagonal], axis=1)


def attention_kernel(qkv_ref, o_ref, lse_ref):
    seq_len = qkv_ref.shape[0]
    keys = qkv_ref[:, HEAD_DIM:2 * HEAD_DIM]
    values = qkv_ref[:, 2 * HEAD_DIM:]
    for q_start in range(0, seq_len, Q_ROWS):
        span = slice(q_start, q_start + Q_ROWS)
        scores = masked_scores(qkv_ref[span, :HEAD_DIM], keys, q_start) * (SCALE * LOG2E)
        row_max = jnp.max(scores, axis=-1, keepdims=True)
        prob = jnp.exp2(scores - row_max)
        norm = jnp.sum(prob, axis=-1, keepdims=True)
        prob = (prob * (1.0 / norm)).astype(BF16)
        o_ref[span] = dot(prob, values[:q_start + Q_ROWS]).astype(BF16)
        lse_ref[span] = jnp.broadcast_to(row_max + jnp.log2(norm), (Q_ROWS, HEAD_DIM))


def attention(qkv):
    seq_len, cols = qkv.shape
    heads = cols // (3 * HEAD_DIM)
    work = heads * seq_len * seq_len
    return pl.pallas_call(
        attention_kernel,
        grid=(heads,),
        out_shape=[jax.ShapeDtypeStruct((seq_len, heads * HEAD_DIM), BF16), jax.ShapeDtypeStruct((seq_len, heads * HEAD_DIM), F32)],
        in_specs=[pl.BlockSpec((seq_len, 3 * HEAD_DIM), lambda h: (0, h))],
        out_specs=[pl.BlockSpec((seq_len, HEAD_DIM), lambda h: (0, h))] * 2,
        compiler_params=params(semantics=('arbitrary',)),
        cost_estimate=cost(8 * work * HEAD_DIM // 2, 2 * seq_len * cols, work // 2),
        name='attention',
    )(qkv)


def attention_backward_kernel(qkv_ref, lse_ref, do_ref, cos_ref, sin_ref, dqkv_ref, dk_acc, dv_acc):
    seq_len = qkv_ref.shape[0]
    keys = qkv_ref[:, HEAD_DIM:2 * HEAD_DIM]
    values = qkv_ref[:, 2 * HEAD_DIM:]
    dk_acc[...] = jnp.zeros_like(dk_acc)
    dv_acc[...] = jnp.zeros_like(dv_acc)

    def unrotate(cotangent, span):
        return rotate(cotangent.astype(BF16).astype(F32), cos_ref[span], -sin_ref[span]).astype(BF16)

    for q_start in range(0, seq_len, Q_ROWS):
        span = slice(q_start, q_start + Q_ROWS)
        seen = slice(0, q_start + Q_ROWS)
        query = qkv_ref[span, :HEAD_DIM]
        d_out = do_ref[span]
        scores = masked_scores(query, keys, q_start) * (SCALE * LOG2E)
        prob = jnp.exp2(scores - lse_ref[span, :1])
        d_prob = dot_nt(d_out, values[seen]).astype(BF16).astype(F32)
        dv_acc[seen] += dot_tn(prob.astype(BF16), d_out)
        inner = jnp.sum(prob * d_prob, axis=-1, keepdims=True)
        d_scores = (prob * (d_prob - inner) * SCALE).astype(BF16)
        dqkv_ref[span, :HEAD_DIM] = unrotate(dot(d_scores, keys[seen]), span)
        dk_acc[seen] += dot_tn(d_scores, query)
    everything = slice(0, seq_len)
    dqkv_ref[:, HEAD_DIM:2 * HEAD_DIM] = unrotate(dk_acc[...], everything)
    dqkv_ref[:, 2 * HEAD_DIM:] = dv_acc[...].astype(BF16)


def attention_backward(qkv, lse, d_attn, tables):
    seq_len, cols = qkv.shape
    heads = cols // (3 * HEAD_DIM)
    work = heads * seq_len * seq_len
    head_block = pl.BlockSpec((seq_len, HEAD_DIM), lambda h: (0, h))
    table_block = pl.BlockSpec((seq_len, HEAD_DIM), lambda h: (0, 0))
    qkv_block = pl.BlockSpec((seq_len, 3 * HEAD_DIM), lambda h: (0, h))
    return pl.pallas_call(
        attention_backward_kernel,
        grid=(heads,),
        out_shape=jax.ShapeDtypeStruct((seq_len, cols), BF16),
        in_specs=[qkv_block, head_block, head_block, table_block, table_block],
        out_specs=qkv_block,
        scratch_shapes=[pltpu.VMEM((seq_len, HEAD_DIM), F32)] * 2,
        compiler_params=params(semantics=('arbitrary',)),
        cost_estimate=cost(20 * work * HEAD_DIM // 2, 6 * seq_len * cols, work // 2),
        name='attention_backward',
    )(qkv, lse, d_attn, *tables)


def weight_grad_kernel(n_pairs, n_held, lhs_refs_first, *refs):
    ins, outs = refs[:n_pairs + 1 + n_held], refs[n_pairs + 1 + n_held:]
    shared, others = ins[0], ins[1:1 + n_pairs]
    for other, out in zip(others, outs):
        lhs, rhs = (shared, other) if lhs_refs_first else (other, shared)
        out[0] = dot_tn(lhs[...], rhs[...]).astype(BF16)


def weight_grads(shared, others, held, layer, n_layers, shared_is_lhs, block):
    seq_len, width = shared.shape
    n_pairs = len(others)
    n_held = len(held)
    shapes = [(width, item.shape[1]) if shared_is_lhs else (item.shape[1], width) for item in others]
    if shared_is_lhs:
        out_specs = [pl.BlockSpec((1, block, item.shape[1]), lambda i: (layer, i, 0)) for item in others]
    else:
        out_specs = [pl.BlockSpec((1, item.shape[1], block), lambda i: (layer, 0, i)) for item in others]
    total = sum(item.shape[1] for item in others)
    return pl.pallas_call(
        functools.partial(weight_grad_kernel, n_pairs, n_held, shared_is_lhs),
        grid=(width // block,),
        out_shape=[jax.ShapeDtypeStruct((n_layers,) + shape, BF16) for shape in shapes],
        in_specs=[pl.BlockSpec((seq_len, block), lambda i: (0, i))]
        + [pl.BlockSpec(item.shape, lambda i: (0, 0), pipeline_mode=pl.Buffered(1)) for item in others]
        + [ANY] * n_held,
        out_specs=out_specs,
        input_output_aliases={1 + n_pairs + idx: idx for idx in range(n_held)},
        compiler_params=params(semantics=('arbitrary',)),
        cost_estimate=cost(2 * seq_len * width * total, 2 * (seq_len * (width + total) + width * total)),
        name=f'weight_grads_{layer}',
    )(shared, *others, *held)


def solution(mesh):
    tp_size = mesh.shape['tp']
    assert tp_size == 2 * N_CHIPS
    row_spec = P(('dp', 'tp'), None)
    col_spec = P(None, None, 'tp')
    inner_spec = P(None, 'tp', None)

    def device_program(x_loc, dy_loc, norm_gain, w_qkv, w_out, w_gate, w_up, w_down):
        n_layers = w_qkv.shape[0]
        seq_len = x_loc.shape[0] * tp_size
        tables = tuple(jnp.asarray(table) for table in rope_tables(seq_len))
        x_cur = x_loc
        u_loc = rms_scale(x_loc.astype(F32), norm_gain[0]).astype(BF16)
        saved = []
        for layer in range(n_layers):
            last = layer == n_layers - 1
            projected = project(u_loc, w_qkv, w_gate, w_up, tables, layer, tp_size, not last)
            qkv, gate_act, up_act = projected[:3]
            attn_out, lse = attention(qkv)
            saved.append((x_cur, u_loc, qkv, gate_act, up_act, attn_out, lse))
            if not last:
                x_cur, u_loc = block_output(attn_out, projected[3], w_out, w_down, x_cur, norm_gain, layer)
        grad_cur = dy_loc
        grads_in, grads_out, gains = (), (), [None] * n_layers
        for layer in reversed(range(n_layers)):
            x_cur, u_loc, qkv, gate_act, up_act, attn_out, lse = saved[layer]
            d_attn, hidden, d_gate, d_up, dy_full = down_backward(grad_cur, w_out, w_down, gate_act, up_act, layer, tp_size)
            u_loc, d_attn = lax.optimization_barrier((u_loc, d_attn))
            u_full = lax.all_gather(u_loc, 'tp', axis=0, tiled=True)
            d_qkv = attention_backward(qkv, lse, d_attn, tables)
            grad_cur, gains[layer] = block_input_backward(d_qkv, d_gate, d_up, w_qkv, w_gate, w_up, x_cur, grad_cur, norm_gain, layer)
            grads_out = weight_grads(dy_full, (attn_out, hidden), grads_out, layer, n_layers, False, 512)
            grads_in = weight_grads(u_full, (d_qkv, d_gate, d_up), grads_in, layer, n_layers, True, 512)
        grad_gain = lax.psum(jnp.concatenate(gains, axis=0), 'tp')
        return (grad_cur, grad_gain, grads_in[0], grads_out[0], grads_in[1], grads_in[2], grads_out[1])

    return jax.shard_map(
        device_program,
        mesh=mesh,
        in_specs=(row_spec, row_spec, P(None, None), col_spec, inner_spec, col_spec, col_spec, inner_spec),
        out_specs=(row_spec, P('dp', None), P('dp', None, 'tp'), P('dp', 'tp', None), P('dp', None, 'tp'), P('dp', None, 'tp'), P('dp', 'tp', None)),
        check_vma=False,
    )
```

```python
import functools

import jax
import jax.numpy as jnp
import numpy as np
from jax import lax
from jax.experimental import pallas as pl
from jax.experimental.pallas import tpu as pltpu
from jax.sharding import PartitionSpec as P

HEAD_DIM = 128
NORM_EPS = 1e-5
ROPE_BASE = 10000.0
SCALE = HEAD_DIM ** -0.5
LOG2E = 1.4426950408889634
VMEM_LIMIT = 64000 * 1024
N_CHIPS = 4
SUBS = 4
Q_ROWS = 256
ROWS_AT_ONCE = 32
BF16 = jnp.bfloat16
F32 = jnp.float32
ANY = pl.BlockSpec(memory_space=pl.ANY)
VMEM = pl.BlockSpec(memory_space=pltpu.VMEM)
NT = (((1,), (1,)), ((), ()))
TN = (((0,), (0,)), ((), ()))


def dot(lhs, rhs):
    return jnp.dot(lhs, rhs, preferred_element_type=F32)


def dot_nt(lhs, rhs):
    return lax.dot_general(lhs, rhs, NT, preferred_element_type=F32)


def dot_tn(lhs, rhs):
    return lax.dot_general(lhs, rhs, TN, preferred_element_type=F32)


def params(collective_id=None, semantics=None):
    if collective_id is None:
        return pltpu.CompilerParams(vmem_limit_bytes=VMEM_LIMIT, dimension_semantics=semantics)
    return pltpu.CompilerParams(vmem_limit_bytes=VMEM_LIMIT, collective_id=collective_id, has_side_effects=True)


def cost(flops, bytes_accessed, transcendentals=0):
    return pl.CostEstimate(flops=flops, bytes_accessed=bytes_accessed, transcendentals=transcendentals)


def rope_tables(seq_len):
    half_dim = HEAD_DIM // 2
    freqs = np.float32(ROPE_BASE) ** (np.float32(-2.0) * np.arange(half_dim, dtype=np.float32) / np.float32(HEAD_DIM))
    angles = np.arange(seq_len, dtype=np.float32)[:, None] * freqs[None, :].astype(np.float32)
    cos_half, sin_half = np.cos(angles).astype(np.float32), np.sin(angles).astype(np.float32)
    return np.concatenate([cos_half, cos_half], axis=1), np.concatenate([-sin_half, sin_half], axis=1)


def rotate(values, cos_tab, sin_tab):
    return values * cos_tab + pltpu.roll(values, HEAD_DIM // 2, 1) * sin_tab


def rms_scale(x_f32, gain_row):
    inv_rms = lax.rsqrt(jnp.mean(x_f32 * x_f32, axis=-1, keepdims=True) + NORM_EPS)
    return x_f32 * inv_rms * gain_row


def ring_place():
    me = lax.axis_index('tp')
    chip = me // 2
    core = me % 2
    return me, chip, core


def device_at(chip, core):
    return ((chip + N_CHIPS) % N_CHIPS) * 2 + core


def remote_copy(src, dst, send_sem, recv_sem, peer):
    return pltpu.make_async_remote_copy(
        src_ref=src, dst_ref=dst, send_sem=send_sem, recv_sem=recv_sem, device_id={'tp': peer}, device_id_type=pl.DeviceIdType.MESH
    )


def meet(peers):
    barrier = pltpu.get_barrier_semaphore()
    for peer in peers:
        pl.semaphore_signal(barrier, inc=1, device_id={'tp': peer}, device_id_type=pl.DeviceIdType.MESH)
    pl.semaphore_wait(barrier, len(peers))


class Gather:
    EVERY, EARLY, LATE = range(SUBS), range(SUBS // 2), range(SUBS // 2, SUBS)

    def __init__(self, full, send_sems, recv_sems):
        self.full, self.send_sems, self.recv_sems = full, send_sems, recv_sems
        self.me, chip, core = ring_place()
        turn = 1 - 2 * core
        self.chip, self.core, self.turn = chip, core, turn
        self.partner = device_at(chip, 1 - core)
        self.ahead = device_at(chip + turn, core)
        self.behind = device_at(chip - turn, core)
        self.first = device_at(chip - turn, core)
        self.first_other = device_at(chip + turn, 1 - core)
        self.second = device_at(chip + turn, core)
        self.second_other = device_at(chip - turn, 1 - core)
        self.third = device_at(chip + 2, core)
        self.third_other = device_at(chip + 2, 1 - core)

    def peers(self):
        return self.partner, self.ahead, self.behind

    def piece(self, kind, shard, sub, peer):
        rows = self.full.shape[1] // SUBS
        part = self.full.at[shard, pl.ds(sub * rows, rows)]
        return remote_copy(part, part, self.send_sems.at[kind, sub], self.recv_sems.at[shard, sub], peer)

    def send(self, kind, shard, peer):
        for sub in self.EVERY:
            self.piece(kind, shard, sub, peer).start()

    def sent(self, kind, shard, peer, subs=EVERY):
        for sub in subs:
            self.piece(kind, shard, sub, peer).wait_send()

    def arrived(self, shard, subs=EVERY, pass_on=None):
        for sub in subs:
            self.piece(0, shard, sub, self.partner).wait_recv()
            if pass_on is not None:
                self.piece(pass_on, shard, sub, self.partner).start()

    def launch(self):
        self.send(1, self.me, self.ahead)
        self.send(0, self.me, self.partner)

    def turn_back(self):
        self.sent(1, self.me, self.ahead, range(SUBS - 1))
        self.send(2, self.me, self.behind)

    def pass_ahead(self):
        self.sent(2, self.me, self.behind, range(SUBS - 1))
        self.send(4, self.first, self.ahead)

    def events(self):
        return (
            lambda: None,
            lambda: (self.turn_back(), self.arrived(self.partner)),
            lambda: self.arrived(self.first, pass_on=3),
            lambda: self.arrived(self.first_other),
            lambda: (self.pass_ahead(), self.arrived(self.second, pass_on=5)),
            lambda: self.arrived(self.second_other),
            lambda: (self.arrived(self.third, self.EARLY, 6), self.arrived(self.third_other, self.EARLY)),
            lambda: (self.arrived(self.third, self.LATE, 6), self.arrived(self.third_other, self.LATE)),
        )

    def places(self, step):
        half = self.full.shape[1] // 2
        pair = step // 2
        odd = step % 2
        side = self.turn * (1 - 2 * odd)
        hop = (3 * pair + (pair // 2) * (2 * pair - 5)) % N_CHIPS
        shard = device_at((self.chip + side * hop + 2 * N_CHIPS) % N_CHIPS, (self.core + odd) % 2)
        last = step // (2 * N_CHIPS - 2)
        upper = (1 - last) * shard + last * self.third
        lower = (1 - last) * shard + last * self.third_other
        return (upper, last * odd * half), (lower, (1 - last) * half + last * odd * half)

    def finish(self):
        self.sent(0, self.me, self.partner)
        self.sent(1, self.me, self.ahead, (SUBS - 1,))
        self.sent(2, self.me, self.behind, (SUBS - 1,))
        self.sent(3, self.first, self.partner)
        self.sent(4, self.first, self.ahead)
        self.sent(5, self.second, self.partner)
        self.sent(6, self.third, self.partner)


def run_at(step, actions):
    for idx, action in enumerate(actions):
        @pl.when(step == idx)
        def _():
            action()


def gather_scratch(tp_size, rows, width):
    return [
        pltpu.VMEM((tp_size, rows, width), BF16),
        pltpu.SemaphoreType.DMA((7, SUBS)),
        pltpu.SemaphoreType.DMA((tp_size, SUBS)),
    ]


def half_rows(ref, place, half):
    return ref[place[0], pl.ds(pl.multiple_of(place[1], half), half)]


def both_halves(ref, places, half):
    return jnp.concatenate([half_rows(ref, place, half) for place in places], axis=0)


def table_rows(ref, places, half, rows):
    parts = [ref[pl.ds(pl.multiple_of(shard * rows + row, half), half)] for shard, row in places]
    return jnp.concatenate(parts, axis=0)


class RowWriter:
    def __init__(self, stages, outs, sems, rows):
        self.stages, self.outs, self.sems, self.rows = stages, outs, sems, rows

    def copies(self, slot, places):
        half = self.rows // 2
        items = []
        for idx in range(len(self.outs)):
            for part, (shard, row) in enumerate(places):
                start = pl.multiple_of(shard * self.rows + row, half)
                src = self.stages[idx].at[slot, pl.ds(part * half, half)]
                items.append(pltpu.make_async_copy(src, self.outs[idx].at[pl.ds(start, half)], self.sems.at[idx, slot, part]))
        return items

    def reuse(self, step):
        @pl.when(step >= 2)
        def _():
            for item in self.copies(step % 2, ((0, 0), (0, 0))):
                item.wait()

    def start(self, step, places):
        for item in self.copies(step % 2, places):
            item.start()

    def finish(self):
        for slot in range(2):
            for item in self.copies(slot, ((0, 0), (0, 0))):
                item.wait()


def project_kernel(layer, first, x_ref, gain_ref, w_qkv_hbm, w_gate_hbm, w_up_hbm, cos_hbm, sin_hbm, *rest):
    n_out = 4 if first else 3
    outs, rest = rest[:n_out], rest[n_out:]
    if first:
        u_ref, *rest = rest
    stages, rest = rest[:n_out], rest[n_out:]
    cos_ref, sin_ref, weights, full, send_sems, recv_sems, w_sems, out_sems = rest
    rows = full.shape[1]
    half = rows // 2
    gather = Gather(full, send_sems, recv_sems)
    loads, spans, start = [], [], 0
    for idx, src in enumerate((w_qkv_hbm, w_gate_hbm, w_up_hbm)):
        spans.append(slice(start, start + src.shape[2]))
        start += src.shape[2]
        loads.append(pltpu.make_async_copy(src.at[layer], weights.at[:, spans[-1]], w_sems.at[idx]))
    loads += [pltpu.make_async_copy(cos_hbm, cos_ref, w_sems.at[3]), pltpu.make_async_copy(sin_hbm, sin_ref, w_sems.at[4])]
    writer = RowWriter(stages, outs, out_sems, rows)
    if first:
        def norm(idx, carry):
            span = pl.ds(pl.multiple_of(idx * ROWS_AT_ONCE, ROWS_AT_ONCE), ROWS_AT_ONCE)
            normed = rms_scale(x_ref[span].astype(F32), gain_ref[layer:layer + 1]).astype(BF16)
            full[gather.me, span] = normed
            u_ref[span] = normed
            return carry

        lax.fori_loop(0, rows // ROWS_AT_ONCE, norm, 0)
        meet(gather.peers())
    else:
        own = pltpu.make_async_copy(x_ref, full.at[gather.me], w_sems.at[5])
        own.start()
        meet(gather.peers())
        own.wait()
    gather.launch()
    for load in loads:
        load.start()
    for load in loads:
        load.wait()

    def step_body(step, carry):
        run_at(step, gather.events())
        places = gather.places(step)
        slot = step % 2
        writer.reuse(step)
        cos_tab, sin_tab = table_rows(cos_ref, places, half, rows), table_rows(sin_ref, places, half, rows)
        product = dot(both_halves(full, places, half), weights[...]).astype(BF16)
        qkv, gate, up = (product[:, span] for span in spans)
        for head in range(qkv.shape[1] // HEAD_DIM):
            cols = slice(head * HEAD_DIM, (head + 1) * HEAD_DIM)
            part = qkv[:, cols]
            if head % 3 != 2:
                part = rotate(part.astype(F32), cos_tab, sin_tab).astype(BF16)
            stages[0][slot, :, cols] = part
        stages[1][slot] = gate
        stages[2][slot] = up
        if first:
            stages[3][slot] = (jax.nn.silu(gate.astype(F32)) * up.astype(F32)).astype(BF16)
        writer.start(step, places)
        return carry

    lax.fori_loop(0, 2 * N_CHIPS, step_body, 0)
    gather.finish()
    writer.finish()


def project(source, norm_gain, w_qkv, w_gate, w_up, tables, layer, tp_size, first):
    rows, width = source.shape
    seq_len = rows * tp_size
    qkv_cols, ff_cols = w_qkv.shape[2], w_gate.shape[2]
    out_cols = [qkv_cols, ff_cols, ff_cols] + ([ff_cols] if first else [])
    total = qkv_cols + 2 * ff_cols
    outs = [jax.ShapeDtypeStruct((seq_len, cols), BF16) for cols in out_cols]
    out_specs = [ANY] * len(outs)
    if first:
        outs.append(jax.ShapeDtypeStruct((rows, width), BF16))
        out_specs.append(VMEM)
    scratch = [pltpu.VMEM((2, rows, cols), BF16) for cols in out_cols]
    scratch += [pltpu.VMEM(table.shape, F32) for table in tables]
    scratch += [pltpu.VMEM((width, total), BF16)]
    scratch += gather_scratch(tp_size, rows, width)
    scratch += [pltpu.SemaphoreType.DMA((6,)), pltpu.SemaphoreType.DMA((len(out_cols), 2, 2))]
    return pl.pallas_call(
        functools.partial(project_kernel, layer, first),
        out_shape=outs,
        in_specs=[VMEM if first else ANY, VMEM] + [ANY] * 5,
        out_specs=out_specs,
        scratch_shapes=scratch,
        compiler_params=params(collective_id=1 + layer),
        cost_estimate=cost(2 * seq_len * width * total, 2 * (width * total + seq_len * total)),
        name=f'project_{layer}',
    )(source, norm_gain, w_qkv, w_gate, w_up, *tables)


def scatter_blocks(blocks_each, peers, load_block, product, beside, tmp, acc, ring, pair_send, pair_recv, ring_send, ring_recv):
    me, chip, core = ring_place()
    partner = device_at(chip, 1 - core)
    right, left = device_at(chip + 1, core), device_at(chip - 1, core)
    per_step = 2 * blocks_each
    n_blocks = N_CHIPS * per_step
    slots = tmp.shape[0]
    meet(peers or (partner, right, left))

    def place(block):
        step = block // per_step
        way = block % 2
        dest = (chip + (1 + step) * (2 * way - 1) + 2 * N_CHIPS) % N_CHIPS
        cols = way * blocks_each + (block % per_step) // 2
        return step, way, dest, cols

    def to_partner(block):
        return remote_copy(tmp.at[block % slots, 1 - core], acc.at[block], pair_send.at[block % slots], pair_recv.at[block], partner)

    def to_next(block):
        way = block % 2
        peer = device_at(chip + 1 - 2 * way, core)
        return remote_copy(acc.at[block], ring.at[block], ring_send.at[block], ring_recv.at[block], peer)

    def body(block, carry):
        @pl.when(block < n_blocks)
        def _():
            step, way, dest, cols = place(block)
            load_block(block)

            @pl.when(block >= slots)
            def _():
                to_partner(block - slots).wait_send()

            product(dest, cols, tmp.at[block % slots])
            to_partner(block).start()
            beside(block)

        @pl.when(block >= 1)
        def _():
            last = block - 1
            to_partner(last).wait_recv()

            @pl.when(last < per_step)
            def _():
                acc[last] = acc[last] + tmp[last % slots, core]

            @pl.when(last >= per_step)
            def _():
                to_next(last - per_step).wait_recv()
                acc[last] = (acc[last] + tmp[last % slots, core]) + ring[last - per_step]

            @pl.when(last < n_blocks - per_step)
            def _():
                to_next(last).start()

        return carry

    lax.fori_loop(0, n_blocks + 1, body, 0)
    for block in range(n_blocks - slots, n_blocks):
        to_partner(block).wait_send()
    for block in range(n_blocks - per_step):
        to_next(block).wait_send()
    return lambda cols: acc.at[n_blocks - per_step + 2 * (cols % blocks_each) + cols // blocks_each]


def scatter_scratch(blocks_each, rows, width):
    per_step = 2 * blocks_each
    n_blocks = N_CHIPS * per_step
    cols = width // per_step
    return [
        pltpu.VMEM((3, 2, rows, cols), F32),
        pltpu.VMEM((n_blocks, rows, cols), F32),
        pltpu.VMEM((n_blocks - per_step, rows, cols), F32),
        pltpu.SemaphoreType.DMA((3,)),
        pltpu.SemaphoreType.DMA((n_blocks,)),
        pltpu.SemaphoreType.DMA((n_blocks - per_step,)),
        pltpu.SemaphoreType.DMA((n_blocks - per_step,)),
    ]


BLOCKS_EACH = 2


def row_loads(pairs, sems, rows, chip):
    def load(order, hop):
        span = pl.ds(pl.multiple_of(((chip + hop) % N_CHIPS) * rows, rows), rows)
        return [pltpu.make_async_copy(src.at[span], dst.at[span], sems.at[idx, order]) for idx, (src, dst) in enumerate(pairs)]

    return [load(order, hop) for order, hop in enumerate((3, 1, 2, 0))]


def forward_kernel(layer, next_gain, o_hbm, m_hbm, w_out_hbm, w_down_hbm, x_ref, gain_ref, y_ref, u_ref, o_all, m_all, w_out, w_down, row_sems, w_sems, *scatter):
    me, chip, core = ring_place()
    per_step = 2 * BLOCKS_EACH
    rows = x_ref.shape[0]
    width = x_ref.shape[1]
    block_cols = width // per_step
    loads = row_loads(((o_hbm, o_all), (m_hbm, m_all)), row_sems, 2 * rows, chip)

    def w_load(cols):
        span = pl.ds(cols * block_cols, block_cols)
        return [
            pltpu.make_async_copy(src.at[layer, :, span], dst.at[cols], w_sems.at[idx, cols])
            for idx, (src, dst) in enumerate(((w_out_hbm, w_out), (w_down_hbm, w_down)))
        ]

    order = [way * BLOCKS_EACH + j for j in range(BLOCKS_EACH) for way in range(2)]
    for block, cols in enumerate(order):
        for item in w_load(cols):
            item.start()
        if block < 2:
            for item in loads[block]:
                item.start()
    for block in range(2, 4):
        for item in loads[block]:
            item.start()

    def load_block(block):
        for idx, cols in enumerate(order):
            @pl.when(block == idx)
            def _():
                for item in w_load(cols):
                    item.wait()

        for idx, at in enumerate((0, 1, per_step, 3 * per_step)):
            @pl.when(block == at)
            def _():
                for item in loads[idx]:
                    item.wait()

    def product(dest, cols, out):
        span = pl.ds(pl.multiple_of(dest * 2 * rows, 2 * rows), 2 * rows)
        total = dot(o_all[span], w_out[cols]) + dot(m_all[span], w_down[cols])
        out[0] = total[:rows]
        out[1] = total[rows:]

    result = scatter_blocks(BLOCKS_EACH, None, load_block, product, lambda block: None, *scatter)

    def finish(idx, carry):
        span = pl.ds(pl.multiple_of(idx * ROWS_AT_ONCE, ROWS_AT_ONCE), ROWS_AT_ONCE)
        summed = jnp.concatenate([result(cols)[span] for cols in range(per_step)], axis=1)
        y = (x_ref[span].astype(F32) + summed).astype(BF16)
        y_ref[span] = y
        u_ref[span] = rms_scale(y.astype(F32), gain_ref[next_gain:next_gain + 1]).astype(BF16)
        return carry

    lax.fori_loop(0, rows // ROWS_AT_ONCE, finish, 0)


def block_output(attn_out, hidden, w_out, w_down, x_loc, norm_gain, layer):
    rows, width = x_loc.shape
    seq_len = attn_out.shape[0]
    head_cols, ff_cols = w_out.shape[1], w_down.shape[1]
    per_step = 2 * BLOCKS_EACH
    cols = width // per_step
    shard = jax.ShapeDtypeStruct((rows, width), BF16)
    return pl.pallas_call(
        functools.partial(forward_kernel, layer, layer + 1),
        out_shape=[shard, shard],
        in_specs=[ANY] * 4 + [VMEM] * 2,
        out_specs=[VMEM] * 2,
        scratch_shapes=[
            pltpu.VMEM((seq_len, head_cols), BF16),
            pltpu.VMEM((seq_len, ff_cols), BF16),
            pltpu.VMEM((per_step, head_cols, cols), BF16),
            pltpu.VMEM((per_step, ff_cols, cols), BF16),
            pltpu.SemaphoreType.DMA((2, 4)),
            pltpu.SemaphoreType.DMA((2, per_step)),
        ] + scatter_scratch(BLOCKS_EACH, rows, width),
        compiler_params=params(collective_id=5 + layer),
        cost_estimate=cost(2 * seq_len * width * (head_cols + ff_cols), 4 * seq_len * (head_cols + ff_cols)),
        name=f'block_output_{layer}',
    )(attn_out, hidden, w_out, w_down, x_loc, norm_gain)


GRAD_ROWS = 4


def backward_kernel(layer, dqkv_hbm, dgate_hbm, dup_hbm, w_qkv_hbm, w_gate_hbm, w_up_hbm, u_hbm, x_ref, dy_ref, gain_ref, *rest):
    first_layer = layer == 0
    if first_layer:
        later_gains_ref, *rest = rest
    dx_ref, dgain_ref, *rest = rest
    grads, rest = rest[:3], rest[3:]
    acts, rest = rest[:3], rest[3:]
    weights, rest = rest[:3], rest[3:]
    u_all, stage, row_sems, w_sems, u_sem, stage_sems, *rest = rest
    if first_layer:
        gain_parts, gain_send, gain_recv, *rest = rest
    scatter = rest
    me, chip, core = ring_place()
    per_step = 2 * BLOCKS_EACH
    rows, width = x_ref.shape
    block_cols = width // per_step
    loads = row_loads(list(zip((dqkv_hbm, dgate_hbm, dup_hbm), acts)), row_sems, 2 * rows, chip)
    u_load = pltpu.make_async_copy(u_hbm, u_all, u_sem)

    def w_load(cols):
        span = pl.ds(cols * block_cols, block_cols)
        return [
            pltpu.make_async_copy(src.at[layer, span], dst.at[span], w_sems.at[idx, cols])
            for idx, (src, dst) in enumerate(zip((w_qkv_hbm, w_gate_hbm, w_up_hbm), weights))
        ]

    order = [way * BLOCKS_EACH + j for j in range(BLOCKS_EACH) for way in range(2)]
    for block, cols in enumerate(order):
        for item in w_load(cols):
            item.start()
        if block < 2:
            for item in loads[block]:
                item.start()
    for block in range(2, 4):
        for item in loads[block]:
            item.start()
    u_load.start()

    def load_block(block):
        for idx, cols in enumerate(order):
            @pl.when(block == idx)
            def _():
                for item in w_load(cols):
                    item.wait()

        for idx, at in enumerate((0, 1, per_step)):
            @pl.when(block == at)
            def _():
                for item in loads[idx]:
                    item.wait()

        @pl.when(block == per_step)
        def _():
            for item in loads[3]:
                item.wait()
            u_load.wait()

    def product(dest, cols, out):
        span = pl.ds(pl.multiple_of(dest * 2 * rows, 2 * rows), 2 * rows)
        w_span = pl.ds(pl.multiple_of(cols * block_cols, block_cols), block_cols)
        total = dot_nt(acts[0][span], weights[0][w_span]) + dot_nt(acts[1][span], weights[1][w_span]) + dot_nt(acts[2][span], weights[2][w_span])
        out[0] = total[:rows]
        out[1] = total[rows:]

    grad_rows = width // GRAD_ROWS

    def grad_out(which, part):
        slot = which % 2
        src = stage.at[slot, :, :grads[which].shape[1]]
        return pltpu.make_async_copy(src, grads[which].at[pl.ds(pl.multiple_of(part * grad_rows, grad_rows), grad_rows)], stage_sems.at[slot])

    def beside(block):
        task = block - per_step
        part = task // 3
        cols = pl.ds(pl.multiple_of(part * grad_rows, grad_rows), grad_rows)
        for turn, which in enumerate((2, 1, 0)):
            @pl.when((task >= 0) & (task % 3 == turn))
            def _():
                if which == 2:
                    @pl.when(part > 0)
                    def _():
                        grad_out(0, part - 1).wait()
                elif which == 0:
                    grad_out(2, part).wait()
                else:
                    @pl.when(part > 0)
                    def _():
                        grad_out(1, part - 1).wait()
                stage[which % 2, :, :grads[which].shape[1]] = dot_tn(u_all[:, cols], acts[which][...]).astype(BF16)
                grad_out(which, part).start()

    peers = [(me + 1 + idx) % (2 * N_CHIPS) for idx in range(2 * N_CHIPS - 1)] if first_layer else None
    result = scatter_blocks(BLOCKS_EACH, peers, load_block, product, beside, *scatter)
    gain_row = gain_ref[layer:layer + 1]
    dgain = gain_parts.at[me, layer:layer + 1] if first_layer else dgain_ref
    dgain[...] = jnp.zeros_like(dgain)

    def finish(idx, carry):
        span = pl.ds(pl.multiple_of(idx * ROWS_AT_ONCE, ROWS_AT_ONCE), ROWS_AT_ONCE)
        summed = jnp.concatenate([result(cols)[span] for cols in range(per_step)], axis=1)
        d_normed = summed.astype(BF16).astype(F32)
        x_f32 = x_ref[span].astype(F32)
        inv_rms = lax.rsqrt(jnp.mean(x_f32 * x_f32, axis=-1, keepdims=True) + NORM_EPS)
        scaled = d_normed * gain_row
        dgain[...] += jnp.sum(d_normed * (x_f32 * inv_rms), axis=0, keepdims=True)
        mix = jnp.mean(scaled * x_f32, axis=-1, keepdims=True) * (inv_rms * inv_rms * inv_rms)
        dx_ref[span] = (dy_ref[span].astype(F32) + (scaled * inv_rms - x_f32 * mix)).astype(BF16)
        return carry

    lax.fori_loop(0, rows // ROWS_AT_ONCE, finish, 0)
    if first_layer:
        gain_parts[me, 1:] = later_gains_ref[...]
        copies = [remote_copy(gain_parts.at[me], gain_parts.at[me], gain_send.at[idx], gain_recv.at[me], peer) for idx, peer in enumerate(peers)]
        for item in copies:
            item.start()
        for idx, peer in enumerate(peers):
            remote_copy(gain_parts.at[peer], gain_parts.at[peer], gain_send.at[idx], gain_recv.at[peer], peer).wait_recv()
        total = gain_parts[0]
        for idx in range(1, 2 * N_CHIPS):
            total = total + gain_parts[idx]
        dgain_ref[...] = total
        for item in copies:
            item.wait_send()
    grad_out(0, GRAD_ROWS - 1).wait()
    grad_out(1, GRAD_ROWS - 1).wait()


def block_input_backward(d_qkv, d_gate, d_up, w_qkv, w_gate, w_up, u_full, x_loc, dy_loc, norm_gain, later_gains, layer):
    rows, width = x_loc.shape
    seq_len = d_qkv.shape[0]
    n_layers = norm_gain.shape[0]
    all_cols = (w_qkv.shape[2], w_gate.shape[2], w_up.shape[2])
    per_step = 2 * BLOCKS_EACH
    first_layer = layer == 0
    out_shape = [jax.ShapeDtypeStruct((rows, width), BF16), jax.ShapeDtypeStruct((n_layers if first_layer else 1, width), F32)]
    out_shape += [jax.ShapeDtypeStruct((width, cols), BF16) for cols in all_cols]
    scratch = [pltpu.VMEM((seq_len, cols), BF16) for cols in all_cols]
    scratch += [pltpu.VMEM((width, cols), BF16) for cols in all_cols]
    scratch += [pltpu.VMEM((seq_len, width), BF16), pltpu.VMEM((2, width // GRAD_ROWS, max(all_cols)), BF16)]
    scratch += [pltpu.SemaphoreType.DMA((3, 4)), pltpu.SemaphoreType.DMA((3, per_step)), pltpu.SemaphoreType.DMA, pltpu.SemaphoreType.DMA((2,))]
    if first_layer:
        scratch += [pltpu.VMEM((2 * N_CHIPS, n_layers, width), F32), pltpu.SemaphoreType.DMA((2 * N_CHIPS - 1,)), pltpu.SemaphoreType.DMA((2 * N_CHIPS,))]
    flops = 2 * seq_len * width * sum(all_cols)
    return pl.pallas_call(
        functools.partial(backward_kernel, layer),
        out_shape=out_shape,
        in_specs=[ANY] * 7 + [VMEM] * (4 if first_layer else 3),
        out_specs=[VMEM] * 2 + [ANY] * 3,
        scratch_shapes=scratch + scatter_scratch(BLOCKS_EACH, rows, width),
        compiler_params=params(collective_id=7 + layer),
        cost_estimate=cost(2 * flops, 4 * seq_len * sum(all_cols)),
        name=f'block_input_backward_{layer}',
    )(d_qkv, d_gate, d_up, w_qkv, w_gate, w_up, u_full, x_loc, dy_loc, norm_gain, *((later_gains,) if first_layer else ()))


def stack_kernel(n_arrays, *refs):
    ins, outs = refs[:-n_arrays], refs[-n_arrays:]
    per_array = len(ins) // n_arrays
    for idx, out in enumerate(outs):
        for layer in range(per_array):
            out[layer] = ins[idx * per_array + layer][...]


def stack_layers(arrays, steps):
    flat = [item for layers in arrays for item in layers]
    n_layers = len(arrays[0])
    return pl.pallas_call(
        functools.partial(stack_kernel, len(arrays)),
        grid=(steps,),
        out_shape=[jax.ShapeDtypeStruct((n_layers,) + layers[0].shape, BF16) for layers in arrays],
        in_specs=[pl.BlockSpec((item.shape[0] // steps, item.shape[1]), lambda i: (i, 0)) for item in flat],
        out_specs=[pl.BlockSpec((n_layers, layers[0].shape[0] // steps, layers[0].shape[1]), lambda i: (0, i, 0)) for layers in arrays],
        compiler_params=params(semantics=('arbitrary',)),
        cost_estimate=cost(0, 4 * sum(item.size for item in flat)),
        name='stack_layers',
    )(*flat)


def causal_tile(size):
    return lax.broadcasted_iota(jnp.int32, (size, size), 0) >= lax.broadcasted_iota(jnp.int32, (size, size), 1)


def masked_scores(query, keys):
    size = query.shape[0]
    q_start = keys.shape[0] - size
    scores = dot_nt(query, keys)
    diagonal = jnp.where(causal_tile(size), scores[:, q_start:], -1e30)
    scores = diagonal if q_start == 0 else jnp.concatenate([scores[:, :q_start], diagonal], axis=1)
    return scores * (SCALE * LOG2E)


def head_cols(head, part, parts):
    return pl.ds(pl.multiple_of((head * parts + part) * HEAD_DIM, HEAD_DIM), HEAD_DIM)


def attend_rows(q_start, head, qkv_ref, o_ref, lse_ref):
    span, seen = slice(q_start, q_start + Q_ROWS), slice(0, q_start + Q_ROWS)
    scores = masked_scores(qkv_ref[span, head_cols(head, 0, 3)], qkv_ref[seen, head_cols(head, 1, 3)])
    row_max = jnp.max(scores, axis=-1, keepdims=True)
    prob = jnp.exp2(scores - row_max)
    norm = jnp.sum(prob, axis=-1, keepdims=True)
    prob = (prob * (1.0 / norm)).astype(BF16)
    o_ref[span, head_cols(head, 0, 1)] = dot(prob, qkv_ref[seen, head_cols(head, 2, 3)]).astype(BF16)
    lse_ref[span, head_cols(head, 0, 1)] = jnp.broadcast_to(row_max + jnp.log2(norm), (Q_ROWS, HEAD_DIM))


def attend_rows_backward(q_start, head, qkv_ref, lse_ref, do_ref, dq_ref, dk_acc, dv_acc):
    span, seen = slice(q_start, q_start + Q_ROWS), slice(0, q_start + Q_ROWS)
    query = qkv_ref[span, head_cols(head, 0, 3)]
    keys = qkv_ref[seen, head_cols(head, 1, 3)]
    d_out = do_ref[span, head_cols(head, 0, 1)]
    scores = masked_scores(query, keys)
    prob = jnp.exp2(scores - lse_ref[span, head_cols(head, 0, 1)][:, :1])
    d_prob = dot_nt(d_out, qkv_ref[seen, head_cols(head, 2, 3)]).astype(BF16).astype(F32)
    dv_acc[head, seen] += dot_tn(prob.astype(BF16), d_out)
    inner = jnp.sum(prob * d_prob, axis=-1, keepdims=True)
    d_scores = (prob * (d_prob - inner) * SCALE).astype(BF16)
    dq_ref[span, head_cols(head, 0, 3)] = dot(d_scores, keys).astype(BF16)
    dk_acc[head, seen] += dot_tn(d_scores, query)


def attention_kernel(qkv_ref, o_ref, lse_ref):
    for q_start in range(0, qkv_ref.shape[0], Q_ROWS):
        attend_rows(q_start, 0, qkv_ref, o_ref, lse_ref)


def attention(qkv):
    seq_len, cols = qkv.shape
    heads = cols // (3 * HEAD_DIM)
    work = heads * seq_len * seq_len
    return pl.pallas_call(
        attention_kernel,
        grid=(heads,),
        out_shape=[jax.ShapeDtypeStruct((seq_len, heads * HEAD_DIM), BF16), jax.ShapeDtypeStruct((seq_len, heads * HEAD_DIM), F32)],
        in_specs=[pl.BlockSpec((seq_len, 3 * HEAD_DIM), lambda h: (0, h))],
        out_specs=[pl.BlockSpec((seq_len, HEAD_DIM), lambda h: (0, h))] * 2,
        compiler_params=params(semantics=('arbitrary',)),
        cost_estimate=cost(8 * work * HEAD_DIM // 2, 2 * seq_len * cols, work // 2),
        name='attention',
    )(qkv)


def middle_kernel(layer, with_forward, dy_hbm, u_hbm, w_out_hbm, w_down_hbm, gate_hbm, up_hbm, cos_hbm, sin_hbm, qkv_hbm, *rest):
    if not with_forward:
        (o_hbm, lse_hbm), rest = rest[:2], rest[2:]
    (dgate_hbm, dup_hbm, dqkv_hbm, u_full_hbm, g_out_hbm, g_down_hbm), rest = rest[:6], rest[6:]
    (dgate_stage, dup_stage, gate_in, up_in, weights, qkv, o_all, lse, hidden, d_attn, dqkv, dk_acc, dv_acc, grad_stage, cos_ref, sin_ref), rest = rest[:16], rest[16:]
    dy_full, dy_send, dy_recv, u_full, u_send, u_recv, load_sems, out_sems, in_sems, u_sems, grad_sems = rest
    rows = dy_full.shape[1]
    half = rows // 2
    seq_len = qkv.shape[0]
    n_heads = o_all.shape[1] // HEAD_DIM
    o_cols = o_all.shape[1]
    gather = Gather(dy_full, dy_send, dy_recv)
    u_gather = Gather(u_full, u_send, u_recv)
    me = gather.me
    own_dy = pltpu.make_async_copy(dy_hbm, dy_full.at[me], load_sems.at[0])
    own_u = pltpu.make_async_copy(u_hbm, u_full.at[me], load_sems.at[1])
    w_loads = [
        pltpu.make_async_copy(w_out_hbm.at[layer], weights.at[:o_cols], load_sems.at[2]),
        pltpu.make_async_copy(w_down_hbm.at[layer], weights.at[o_cols:], load_sems.at[3]),
    ]
    loads = [
        pltpu.make_async_copy(src, dst, load_sems.at[4 + idx])
        for idx, (src, dst) in enumerate([(qkv_hbm, qkv), (cos_hbm, cos_ref), (sin_hbm, sin_ref)] + ([] if with_forward else [(o_hbm, o_all), (lse_hbm, lse)]))
    ]
    writer = RowWriter((dgate_stage, dup_stage), (dgate_hbm, dup_hbm), out_sems, rows)
    own_dy.start()
    meet(gather.peers())
    own_dy.wait()
    gather.launch()
    for item in w_loads + loads + [own_u]:
        item.start()
    dk_acc[...] = jnp.zeros_like(dk_acc)
    dv_acc[...] = jnp.zeros_like(dv_acc)
    for item in w_loads + loads + [own_u]:
        item.wait()

    def both_heads(function, *args):
        def body(head, carry):
            function(*args[:1], head, *args[1:])
            return carry

        lax.fori_loop(0, n_heads, body, 0)

    def dy_step(step, carry):
        run_at(step, gather.events())

        @pl.when(step == 2 * N_CHIPS - 2)
        def _():
            u_gather.launch()

        places = gather.places(step)
        slot = step % 2
        fetch = []
        for idx, (src, dst) in enumerate(((gate_hbm, gate_in), (up_hbm, up_in))):
            for part, (shard, row) in enumerate(places):
                here = pl.ds(pl.multiple_of(shard * rows + row, half), half)
                fetch.append(pltpu.make_async_copy(src.at[here], dst.at[pl.ds(part * half, half)], in_sems.at[idx, part]))
        for item in fetch:
            item.start()
        writer.reuse(step)
        product = dot_nt(both_halves(dy_full, places, half), weights[...]).astype(BF16)
        d_hidden = product[:, o_cols:].astype(F32)
        for item in fetch:
            item.wait()
        gate, up = gate_in[...].astype(F32), up_in[...].astype(F32)
        sig = jax.nn.sigmoid(gate)
        act = gate * sig
        hidden_rows = (act * up).astype(BF16)
        for part, (shard, row) in enumerate(places):
            here = pl.ds(pl.multiple_of(shard * rows + row, half), half)
            d_attn[here] = product[part * half:(part + 1) * half, :o_cols]
            hidden[here] = hidden_rows[part * half:(part + 1) * half]
        dgate_stage[slot] = (d_hidden * up * (sig + act * (1.0 - sig))).astype(BF16)
        dup_stage[slot] = (d_hidden * act).astype(BF16)
        writer.start(step, places)
        if with_forward:
            run_at(step, [functools.partial(both_heads, attend_rows, q_start, qkv, o_all, lse) for q_start in range(0, seq_len, Q_ROWS)])
        return carry

    lax.fori_loop(0, 2 * N_CHIPS, dy_step, 0)

    def grad_copies(step):
        slot = step % 2
        cols = pl.ds(pl.multiple_of(step * grad_cols, grad_cols), grad_cols)
        return (
            pltpu.make_async_copy(grad_stage.at[slot, :o_cols], g_out_hbm.at[:, cols], grad_sems.at[slot, 0]),
            pltpu.make_async_copy(grad_stage.at[slot, o_cols:], g_down_hbm.at[:, cols], grad_sems.at[slot, 1]),
        )

    grad_cols = dy_full.shape[2] // (2 * N_CHIPS)
    u_events = (
        lambda: u_gather.turn_back(),
        lambda: u_gather.arrived(u_gather.partner),
        lambda: u_gather.arrived(u_gather.first, pass_on=3),
        lambda: u_gather.arrived(u_gather.first_other),
        lambda: (u_gather.pass_ahead(), u_gather.arrived(u_gather.second, pass_on=5)),
        lambda: u_gather.arrived(u_gather.second_other),
        lambda: u_gather.arrived(u_gather.third, u_gather.EARLY, 6),
        lambda: None,
    )

    def u_step(step, carry):
        run_at(step, u_events)

        @pl.when(step >= 2)
        def _():
            for item in grad_copies(step - 2):
                item.wait()

        cols = pl.ds(pl.multiple_of(step * grad_cols, grad_cols), grad_cols)
        dy_cols = dy_full[:, :, cols].reshape(seq_len, grad_cols)
        slot = step % 2
        grad_stage[slot, :o_cols] = dot_tn(o_all[...], dy_cols).astype(BF16)
        grad_stage[slot, o_cols:] = dot_tn(hidden[...], dy_cols).astype(BF16)
        for item in grad_copies(step):
            item.start()
        run_at(step, [functools.partial(both_heads, attend_rows_backward, q_start, qkv, lse, d_attn, dqkv, dk_acc, dv_acc) for q_start in range(0, seq_len, Q_ROWS)])
        return carry

    lax.fori_loop(0, 2 * N_CHIPS, u_step, 0)
    u_gather.arrived(u_gather.third, u_gather.LATE, 6)
    u_gather.arrived(u_gather.third_other)
    keep_u = pltpu.make_async_copy(u_full, u_full_hbm, u_sems.at[0])
    keep_u.start()

    def finish(idx, carry):
        span = pl.ds(pl.multiple_of(idx * Q_ROWS, Q_ROWS), Q_ROWS)
        cos_tab, sin_tab = cos_ref[span], -sin_ref[span]
        for head in range(n_heads):
            for part, value in enumerate((dqkv[span, head_cols(head, 0, 3)], dk_acc[head, span].astype(BF16))):
                dqkv[span, head_cols(head, part, 3)] = rotate(value.astype(F32), cos_tab, sin_tab).astype(BF16)
            dqkv[span, head_cols(head, 2, 3)] = dv_acc[head, span].astype(BF16)
        return carry

    lax.fori_loop(0, seq_len // Q_ROWS, finish, 0)
    keep_dqkv = pltpu.make_async_copy(dqkv, dqkv_hbm, u_sems.at[1])
    keep_dqkv.start()
    for step in (2 * N_CHIPS - 2, 2 * N_CHIPS - 1):
        for item in grad_copies(step):
            item.wait()
    gather.finish()
    u_gather.finish()
    writer.finish()
    keep_u.wait()
    keep_dqkv.wait()


def middle(dy_loc, u_loc, w_out, w_down, gate_act, up_act, tables, qkv, attended, layer, tp_size):
    rows, width = dy_loc.shape
    seq_len = rows * tp_size
    o_cols, ff_cols, qkv_cols = w_out.shape[1], w_down.shape[1], qkv.shape[1]
    n_heads = o_cols // HEAD_DIM
    total = o_cols + ff_cols
    outs = [(seq_len, ff_cols), (seq_len, ff_cols), (seq_len, qkv_cols), (tp_size, rows, width), (o_cols, width), (ff_cols, width)]
    scratch = [pltpu.VMEM((2, rows, ff_cols), BF16)] * 2
    scratch += [pltpu.VMEM((rows, ff_cols), BF16)] * 2
    scratch += [
        pltpu.VMEM((total, width), BF16),
        pltpu.VMEM((seq_len, qkv_cols), BF16),
        pltpu.VMEM((seq_len, o_cols), BF16),
        pltpu.VMEM((seq_len, o_cols), F32),
        pltpu.VMEM((seq_len, ff_cols), BF16),
        pltpu.VMEM((seq_len, o_cols), BF16),
        pltpu.VMEM((seq_len, qkv_cols), BF16),
        pltpu.VMEM((n_heads, seq_len, HEAD_DIM), F32),
        pltpu.VMEM((n_heads, seq_len, HEAD_DIM), F32),
        pltpu.VMEM((2, total, width // (2 * N_CHIPS)), BF16),
    ]
    scratch += [pltpu.VMEM(table.shape, F32) for table in tables]
    scratch += gather_scratch(tp_size, rows, width) + gather_scratch(tp_size, rows, width)
    scratch += [
        pltpu.SemaphoreType.DMA((9,)),
        pltpu.SemaphoreType.DMA((2, 2, 2)),
        pltpu.SemaphoreType.DMA((2, 2)),
        pltpu.SemaphoreType.DMA((2,)),
        pltpu.SemaphoreType.DMA((2, 2)),
    ]
    work = n_heads * seq_len * seq_len * HEAD_DIM
    return pl.pallas_call(
        functools.partial(middle_kernel, layer, not attended),
        out_shape=[jax.ShapeDtypeStruct(shape, BF16) for shape in outs],
        in_specs=[ANY] * (9 + len(attended)),
        out_specs=[ANY] * len(outs),
        scratch_shapes=scratch,
        compiler_params=params(collective_id=3 + layer),
        cost_estimate=cost(4 * seq_len * width * total + 10 * work, 2 * (width * total + 3 * seq_len * total)),
        name=f'middle_{layer}',
    )(dy_loc, u_loc, w_out, w_down, gate_act, up_act, *tables, qkv, *attended)


def solution(mesh):
    tp_size = mesh.shape['tp']
    assert tp_size == 2 * N_CHIPS
    row_spec = P(('dp', 'tp'), None)
    col_spec = P(None, None, 'tp')
    inner_spec = P(None, 'tp', None)

    def device_program(x_loc, dy_loc, norm_gain, w_qkv, w_out, w_gate, w_up, w_down):
        n_layers = w_qkv.shape[0]
        seq_len = x_loc.shape[0] * tp_size
        tables = tuple(jnp.asarray(table) for table in rope_tables(seq_len))
        x_cur, source = x_loc, x_loc
        saved = []
        for layer in range(n_layers):
            first, last = layer == 0, layer == n_layers - 1
            qkv, gate_act, up_act, *more = project(source, norm_gain, w_qkv, w_gate, w_up, tables, layer, tp_size, first)
            u_loc = more[1] if first else source
            if last:
                saved.append((x_cur, u_loc, qkv, gate_act, up_act, ()))
            else:
                attended = attention(qkv)
                saved.append((x_cur, u_loc, qkv, gate_act, up_act, tuple(attended)))
                x_cur, source = block_output(attended[0], more[0], w_out, w_down, x_cur, norm_gain, layer)
        grad_cur = dy_loc
        grads, gains = [None] * n_layers, ()
        for layer in reversed(range(n_layers)):
            x_cur, u_loc, qkv, gate_act, up_act, attended = saved[layer]
            d_gate, d_up, d_qkv, u_full, g_out, g_down = middle(grad_cur, u_loc, w_out, w_down, gate_act, up_act, tables, qkv, attended, layer, tp_size)
            u_full = u_full.reshape(seq_len, u_full.shape[2])
            later_gains = jnp.concatenate(gains, axis=0) if gains else None
            grad_cur, gain_grad, g_qkv, g_gate, g_up = block_input_backward(
                d_qkv, d_gate, d_up, w_qkv, w_gate, w_up, u_full, x_cur, grad_cur, norm_gain, later_gains, layer
            )
            grads[layer] = (g_qkv, g_gate, g_up, g_out, g_down)
            gains = (gain_grad,) + gains
        g_qkv, g_gate, g_up, g_out, g_down = stack_layers(list(zip(*grads)), 8)
        return (grad_cur, gains[0], g_qkv, g_out, g_gate, g_up, g_down)

    return jax.shard_map(
        device_program,
        mesh=mesh,
        in_specs=(row_spec, row_spec, P(None, None), col_spec, inner_spec, col_spec, col_spec, inner_spec),
        out_specs=(row_spec, P('dp', None), P('dp', None, 'tp'), P('dp', 'tp', None), P('dp', None, 'tp'), P('dp', None, 'tp'), P('dp', 'tp', None)),
        check_vma=False,
    )
```

```python
import functools

import jax
import jax.numpy as jnp
import numpy as np
from jax import lax
from jax.experimental import pallas as pl
from jax.experimental.pallas import tpu as pltpu
from jax.sharding import PartitionSpec as P

HEAD_DIM = 128
NORM_EPS = 1e-5
ROPE_BASE = 10000.0
SCALE = HEAD_DIM ** -0.5
LOG2E = 1.4426950408889634
VMEM_LIMIT = 64000 * 1024
CORES = 2
N_CHIPS = 4
N_DEVICES = CORES * N_CHIPS
WAYS = 2
BUFFERS = 2
SUBS = 4
Q_ROWS = 256
ROWS_AT_ONCE = 32
FINE = 128
BF16 = jnp.bfloat16
F32 = jnp.float32
ANY = pl.BlockSpec(memory_space=pl.ANY)
VMEM = pl.BlockSpec(memory_space=pltpu.VMEM)
NT = (((1,), (1,)), ((), ()))
TN = (((0,), (0,)), ((), ()))


def height(array):
    return array.shape[0]


def width_of(array):
    return array.shape[1]


def piece_at(idx, size):
    return pl.ds(pl.multiple_of(idx * size, size), size)


def dma_sems(*shape):
    return pltpu.SemaphoreType.DMA(shape)


def dot(lhs, rhs):
    return jnp.dot(lhs, rhs, preferred_element_type=F32)


def dot_nt(lhs, rhs):
    return lax.dot_general(lhs, rhs, NT, preferred_element_type=F32)


def dot_tn(lhs, rhs):
    return lax.dot_general(lhs, rhs, TN, preferred_element_type=F32)


def params(collective_id=None, semantics=None):
    if collective_id is None:
        return pltpu.CompilerParams(vmem_limit_bytes=VMEM_LIMIT, dimension_semantics=semantics)
    return pltpu.CompilerParams(vmem_limit_bytes=VMEM_LIMIT, collective_id=collective_id, has_side_effects=True)


def row_mean(values):
    return jnp.mean(values, axis=-1, keepdims=True)


def row_sum(values):
    return jnp.sum(values, axis=-1, keepdims=True)


def rope_tables(seq_len, fine):
    half_dim = HEAD_DIM // 2
    freqs = np.float32(ROPE_BASE) ** (np.float32(-2.0) * np.arange(half_dim, dtype=np.float32) / np.float32(HEAD_DIM))
    tables = []
    for positions in (np.arange(fine), np.arange(0, seq_len, fine)):
        angles = positions.astype(np.float32)[:, None] * freqs[None, :]
        tables += [np.tile(np.cos(angles), 2).astype(np.float32), np.tile(np.sin(angles), 2).astype(np.float32)]
    return tables


def fill_rope(fine_cos, fine_sin, coarse_cos, coarse_sin, cos_ref, sin_ref):
    fine = height(fine_cos)
    sign = jnp.where(lax.broadcasted_iota(jnp.int32, (1, HEAD_DIM), 1) < HEAD_DIM // 2, -1.0, 1.0)

    def body(idx, carry):
        span = piece_at(idx, fine)
        big_cos, big_sin = coarse_cos[pl.ds(idx, 1)], coarse_sin[pl.ds(idx, 1)]
        cos_ref[span] = big_cos * fine_cos[...] - big_sin * fine_sin[...]
        sin_ref[span] = (big_sin * fine_cos[...] + big_cos * fine_sin[...]) * sign
        return carry

    lax.fori_loop(0, height(cos_ref) // fine, body, 0)


def rotate(values, cos_tab, sin_tab):
    return values * cos_tab + pltpu.roll(values, HEAD_DIM // 2, 1) * sin_tab


def rms_scale(x_f32, gain_row):
    inv_rms = lax.rsqrt(row_mean(x_f32 * x_f32) + NORM_EPS)
    return x_f32 * inv_rms * gain_row


def ring_place():
    me = lax.axis_index('tp')
    chip = me // 2
    core = me % 2
    return me, chip, core


def device_at(chip, core):
    return ((chip + N_CHIPS) % N_CHIPS) * 2 + core


def remote_copy(src, dst, send_sem, recv_sem, peer):
    return pltpu.make_async_remote_copy(
        src_ref=src, dst_ref=dst, send_sem=send_sem, recv_sem=recv_sem, device_id={'tp': peer}, device_id_type=pl.DeviceIdType.MESH
    )


def meet(peers):
    barrier = pltpu.get_barrier_semaphore()
    for peer in peers:
        pl.semaphore_signal(barrier, inc=1, device_id={'tp': peer}, device_id_type=pl.DeviceIdType.MESH)
    pl.semaphore_wait(barrier, len(peers))


OWN_PARTNER, OWN_AHEAD, OWN_BEHIND, FIRST_PARTNER, FIRST_AHEAD, SECOND_PARTNER, THIRD_PARTNER = KINDS = range(7)


class Gather:
    EVERY, EARLY, LATE = range(SUBS), range(SUBS // 2), range(SUBS // 2, SUBS)

    def __init__(self, full, send_sems, recv_sems):
        self.full, self.send_sems, self.recv_sems = full, send_sems, recv_sems
        self.me, chip, core = ring_place()
        turn = 1 - 2 * core
        self.chip, self.core, self.turn = chip, core, turn
        self.partner = device_at(chip, 1 - core)
        self.ahead = device_at(chip + turn, core)
        self.behind = device_at(chip - turn, core)
        self.first = device_at(chip - turn, core)
        self.first_other = device_at(chip + turn, 1 - core)
        self.second = device_at(chip + turn, core)
        self.second_other = device_at(chip - turn, 1 - core)
        self.third = device_at(chip + 2, core)
        self.third_other = device_at(chip + 2, 1 - core)

    def peers(self):
        return self.partner, self.ahead, self.behind

    def piece(self, kind, shard, sub, peer):
        rows = width_of(self.full) // SUBS
        part = self.full.at[shard, pl.ds(sub * rows, rows)]
        return remote_copy(part, part, self.send_sems.at[kind, sub], self.recv_sems.at[shard, sub], peer)

    def send(self, kind, shard, peer, subs=EVERY):
        for sub in subs:
            self.piece(kind, shard, sub, peer).start()

    def sent(self, kind, shard, peer, subs=EVERY):
        for sub in subs:
            self.piece(kind, shard, sub, peer).wait_send()

    def arrived(self, shard, subs=EVERY, pass_on=None):
        for sub in subs:
            self.piece(OWN_PARTNER, shard, sub, self.partner).wait_recv()
            if pass_on is not None:
                self.piece(pass_on, shard, sub, self.partner).start()

    def launch(self, subs=EVERY):
        self.send(OWN_AHEAD, self.me, self.ahead, subs)
        self.send(OWN_PARTNER, self.me, self.partner, subs)

    def turn_back(self):
        self.sent(OWN_AHEAD, self.me, self.ahead, range(SUBS - 1))
        self.send(OWN_BEHIND, self.me, self.behind)

    def pass_ahead(self):
        self.sent(OWN_BEHIND, self.me, self.behind, range(SUBS - 1))
        self.send(FIRST_AHEAD, self.first, self.ahead)

    def launch_both(self):
        self.launch()
        self.send(OWN_BEHIND, self.me, self.behind)

    def pass_piece(self, sub):
        self.piece(OWN_PARTNER, self.first, sub, self.partner).wait_recv()
        self.piece(FIRST_AHEAD, self.first, sub, self.ahead).start()
        self.piece(FIRST_PARTNER, self.first, sub, self.partner).start()
        self.arrived(self.second, (sub,), SECOND_PARTNER)

    def end_piece(self, sub):
        self.arrived(self.third, (sub,), THIRD_PARTNER)

    def events(self, early=False):
        return (
            lambda: None,
            lambda: (self.turn_back(), self.arrived(self.partner)),
            lambda: self.arrived(self.first, pass_on=FIRST_PARTNER),
            lambda: (self.pass_ahead() if early else None, self.arrived(self.first_other)),
            lambda: (None if early else self.pass_ahead(), self.arrived(self.second, pass_on=SECOND_PARTNER)),
            lambda: self.arrived(self.second_other),
            lambda: (self.arrived(self.third, self.EARLY, THIRD_PARTNER), self.arrived(self.third_other, self.EARLY)),
            lambda: (self.arrived(self.third, self.LATE, THIRD_PARTNER), self.arrived(self.third_other, self.LATE)),
        )

    def places(self, step):
        half = width_of(self.full) // 2
        pair = step // 2
        odd = step % BUFFERS
        side = self.turn * (1 - 2 * odd)
        hop = (3 * pair + (pair // 2) * (2 * pair - 5)) % N_CHIPS
        shard = device_at((self.chip + side * hop + N_DEVICES) % N_CHIPS, (self.core + odd) % 2)
        last = step // (N_DEVICES - 2)
        upper = (1 - last) * shard + last * self.third
        lower = (1 - last) * shard + last * self.third_other
        return (upper, last * odd * half), (lower, (1 - last) * half + last * odd * half)

    def finish(self, waited=SUBS - 1):
        self.sent(OWN_PARTNER, self.me, self.partner)
        self.sent(OWN_AHEAD, self.me, self.ahead, range(waited, SUBS))
        self.sent(OWN_BEHIND, self.me, self.behind, range(waited, SUBS))
        self.sent(FIRST_PARTNER, self.first, self.partner)
        self.sent(FIRST_AHEAD, self.first, self.ahead)
        self.sent(SECOND_PARTNER, self.second, self.partner)
        self.sent(THIRD_PARTNER, self.third, self.partner)


def run_at(step, actions):
    for idx, action in enumerate(actions):
        @pl.when(step == idx)
        def _():
            action()


def gather_scratch(tp_size, rows, width):
    return [
        pltpu.VMEM((tp_size, rows, width), BF16),
        dma_sems(len(KINDS), SUBS),
        dma_sems(tp_size, SUBS),
    ]


def half_rows(ref, place, half):
    return ref[place[0], pl.ds(pl.multiple_of(place[1], half), half)]


def both_halves(ref, places, half):
    return jnp.concatenate([half_rows(ref, place, half) for place in places], axis=0)


def table_rows(ref, places, half, rows):
    parts = [ref[pl.ds(pl.multiple_of(shard * rows + row, half), half)] for shard, row in places]
    return jnp.concatenate(parts, axis=0)


class RowWriter:
    def __init__(self, stages, outs, sems, rows):
        self.stages, self.outs, self.sems, self.rows = stages, outs, sems, rows

    def copies(self, slot, places):
        half = self.rows // 2
        items = []
        for idx in range(len(self.outs)):
            for part, (shard, row) in enumerate(places):
                start = pl.multiple_of(shard * self.rows + row, half)
                src = self.stages[idx].at[slot, pl.ds(part * half, half)]
                items.append(pltpu.make_async_copy(src, self.outs[idx].at[pl.ds(start, half)], self.sems.at[idx, slot, part]))
        return items

    def reuse(self, step):
        @pl.when(step >= 2)
        def _():
            for item in self.copies(step % BUFFERS, ((0, 0), (0, 0))):
                item.wait()

    def start(self, step, places):
        for item in self.copies(step % BUFFERS, places):
            item.start()

    def finish(self):
        for slot in range(BUFFERS):
            for item in self.copies(slot, ((0, 0), (0, 0))):
                item.wait()


def project_kernel(layer, first, x_ref, gain_ref, w_qkv_hbm, w_gate_hbm, w_up_hbm, *rest):
    n_out = 4 if first else 3
    n_tables = 4 if first else 2
    tables, rest = rest[:n_tables], rest[n_tables:]
    outs, rest = rest[:n_out], rest[n_out:]
    if first:
        u_ref, cos_out, sin_out, *rest = rest
    stages, rest = rest[:n_out], rest[n_out:]
    cos_ref, sin_ref, weights, full, send_sems, recv_sems, w_sems, out_sems = rest
    rows = width_of(full)
    half = rows // 2
    gather = Gather(full, send_sems, recv_sems)
    loads, spans, start = [], [], 0
    for idx, src in enumerate((w_qkv_hbm, w_gate_hbm, w_up_hbm)):
        spans.append(slice(start, start + src.shape[2]))
        start += src.shape[2]
        loads.append(pltpu.make_async_copy(src.at[layer], weights.at[:, spans[-1]], w_sems.at[idx]))
    if first:
        keep_tables = [pltpu.make_async_copy(cos_ref, cos_out, w_sems.at[3]), pltpu.make_async_copy(sin_ref, sin_out, w_sems.at[4])]
    else:
        loads += [pltpu.make_async_copy(src, dst, w_sems.at[3 + idx]) for idx, (src, dst) in enumerate(zip(tables, (cos_ref, sin_ref)))]
    writer = RowWriter(stages, outs, out_sems, rows)
    if first:
        norm_rows = min(ROWS_AT_ONCE, rows // SUBS)

        def norm(idx, carry):
            span = piece_at(idx, norm_rows)
            normed = rms_scale(x_ref[span].astype(F32), gain_ref[layer:layer + 1]).astype(BF16)
            full[gather.me, span] = normed
            u_ref[span] = normed
            return carry

        for load in loads:
            load.start()
        meet(gather.peers())
        per_piece = rows // SUBS // norm_rows
        for sub in range(SUBS):
            lax.fori_loop(sub * per_piece, (sub + 1) * per_piece, norm, 0)
            gather.launch((sub,))
        fill_rope(*tables, cos_ref, sin_ref)
        for item in keep_tables:
            item.start()
    else:
        own = pltpu.make_async_copy(x_ref, full.at[gather.me], w_sems.at[5])
        own.start()
        meet(gather.peers())
        own.wait()
        gather.launch()
        for load in loads:
            load.start()
    for load in loads:
        load.wait()

    def step_body(step, carry):
        run_at(step, gather.events())
        places = gather.places(step)
        slot = step % BUFFERS
        writer.reuse(step)
        cos_tab, sin_tab = table_rows(cos_ref, places, half, rows), table_rows(sin_ref, places, half, rows)
        product = dot(both_halves(full, places, half), weights[...]).astype(BF16)
        qkv, gate, up = (product[:, span] for span in spans)
        for head in range(width_of(qkv) // HEAD_DIM):
            cols = slice(head * HEAD_DIM, (head + 1) * HEAD_DIM)
            part = qkv[:, cols]
            if head % 3 != 2:
                part = rotate(part.astype(F32), cos_tab, sin_tab).astype(BF16)
            stages[0][slot, :, cols] = part
        stages[1][slot] = gate
        stages[2][slot] = up
        if first:
            stages[3][slot] = (jax.nn.silu(gate.astype(F32)) * up.astype(F32)).astype(BF16)
        writer.start(step, places)
        return carry

    lax.fori_loop(0, N_DEVICES, step_body, 0)
    gather.finish()
    writer.finish()
    if first:
        for item in keep_tables:
            item.wait()


def project(source, norm_gain, w_qkv, w_gate, w_up, tables, layer, tp_size, first):
    rows, width = source.shape
    seq_len = rows * tp_size
    qkv_cols, ff_cols = w_qkv.shape[2], w_gate.shape[2]
    out_cols = [qkv_cols, ff_cols, ff_cols] + ([ff_cols] if first else [])
    total = qkv_cols + 2 * ff_cols
    outs = [jax.ShapeDtypeStruct((seq_len, cols), BF16) for cols in out_cols]
    out_specs = [ANY] * len(outs)
    table = (seq_len, HEAD_DIM)
    if first:
        outs += [jax.ShapeDtypeStruct((rows, width), BF16)] + [jax.ShapeDtypeStruct(table, F32)] * 2
        out_specs += [VMEM, ANY, ANY]
    scratch = [pltpu.VMEM((BUFFERS, rows, cols), BF16) for cols in out_cols]
    scratch += [pltpu.VMEM(table, F32)] * 2
    scratch += [pltpu.VMEM((width, total), BF16)]
    scratch += gather_scratch(tp_size, rows, width)
    scratch += [dma_sems(6), pltpu.SemaphoreType.DMA((len(out_cols), 2, 2))]
    return pl.pallas_call(
        functools.partial(project_kernel, layer, first),
        out_shape=outs,
        in_specs=[VMEM if first else ANY, VMEM] + [ANY] * 3 + [VMEM if first else ANY] * len(tables),
        out_specs=out_specs,
        scratch_shapes=scratch,
        compiler_params=params(collective_id=1 + layer),
        name=f'project_{layer}',
    )(source, norm_gain, w_qkv, w_gate, w_up, *tables)


EACH = 4
PER_STEP = WAYS * EACH
N_BLOCKS = N_CHIPS * PER_STEP
N_PAIRS = (N_BLOCKS - PER_STEP) // 2
SLOTS = 6


def scatter_blocks(peers, load, product, beside, tmp, acc, ring, pair_send, pair_recv, ring_send, ring_recv):
    me, chip, core = ring_place()
    partner = device_at(chip, 1 - core)
    meet(peers or (partner, device_at(chip + 1, core), device_at(chip - 1, core)))

    def dest(step, way):
        return (chip + (step + 1) * (WAYS * way - 1) + N_DEVICES) % N_CHIPS

    def to_partner(block, slot):
        return remote_copy(tmp.at[slot, 1 - core], acc.at[block], pair_send.at[slot], pair_recv.at[block], partner)

    def to_next(block):
        peer = device_at(chip + 1 - 2 * (block % WAYS), core)
        return remote_copy(acc.at[block], ring.at[block], ring_send.at[block], ring_recv.at[block], peer)

    def serve_first(block):
        to_partner(block, block % SLOTS).wait_recv()
        acc[block] = acc[block] + tmp[block % SLOTS, core]
        to_next(block).start()

    def first_body(block, carry):
        load(block)

        @pl.when(block >= SLOTS)
        def _():
            to_partner(block - SLOTS, block % SLOTS).wait_send()

        way = block % WAYS
        product(dest(0, way), way * EACH + block // WAYS, 1, tmp.at[pl.ds(block % SLOTS, 1)])
        to_partner(block, block % SLOTS).start()

        @pl.when(block >= 1)
        def _():
            serve_first(block - 1)

        return carry

    lax.fori_loop(0, PER_STEP, first_body, 0)

    def pair_blocks(pair):
        step, rest = 1 + pair // EACH, pair % EACH
        way, col = rest % WAYS, 2 * (rest // 2)
        block = step * PER_STEP + 2 * col + way
        slot = (PER_STEP + 2 * pair) % SLOTS
        return step, way, col, ((block, slot), (block + 2, slot + 1))

    def body(pair, carry):
        @pl.when(pair < N_PAIRS)
        def _():
            step, way, col, blocks = pair_blocks(pair)
            load(PER_STEP + pair)
            for block, slot in blocks:
                to_partner(block, slot).wait_send()
            product(dest(step, way), way * EACH + col, 2, tmp.at[pl.ds(blocks[0][1], 2)])
            for block, slot in blocks:
                to_partner(block, slot).start()
            beside(pair)

        @pl.when(pair == 0)
        def _():
            serve_first(PER_STEP - 1)

        @pl.when(pair >= 1)
        def _():
            step, way, col, blocks = pair_blocks(pair - 1)
            for block, slot in blocks:
                to_partner(block, slot).wait_recv()
                to_next(block - PER_STEP).wait_recv()
                acc[block] = (acc[block] + tmp[slot, core]) + ring[block - PER_STEP]

                @pl.when(step < N_CHIPS - 1)
                def _():
                    to_next(block).start()

        return carry

    lax.fori_loop(0, N_PAIRS + 1, body, 0)
    for slot in range(SLOTS):
        to_partner(0, slot).wait_send()
    for block in range(N_BLOCKS - PER_STEP):
        to_next(block).wait_send()
    return lambda cols: acc.at[N_BLOCKS - PER_STEP + 2 * (cols % EACH) + cols // EACH]


def scatter_scratch(rows, width):
    cols = width // PER_STEP
    return [
        pltpu.VMEM((SLOTS, 2, rows, cols), F32),
        pltpu.VMEM((N_BLOCKS, rows, cols), F32),
        pltpu.VMEM((N_BLOCKS - PER_STEP, rows, cols), F32),
        dma_sems(SLOTS),
        dma_sems(N_BLOCKS),
        dma_sems(N_BLOCKS - PER_STEP),
        dma_sems(N_BLOCKS - PER_STEP),
    ]


def start_loads(w_load, row_loads_of):
    order = [(block % WAYS) * EACH + block // WAYS for block in range(PER_STEP)]
    for block, cols in enumerate(order):
        for item in w_load(cols):
            item.start()
        if block < 2:
            for item in row_loads_of[block]:
                item.start()
    for items in row_loads_of[2:]:
        for item in items:
            item.start()

    def load(product):
        for idx, cols in enumerate(order):
            @pl.when(product == idx)
            def _():
                for item in w_load(cols) + (row_loads_of[idx] if idx < 2 else []):
                    item.wait()

    return load


def row_loads(pairs, sems, rows, chip):
    def load(order, hop):
        span = pl.ds(pl.multiple_of(((chip + hop) % N_CHIPS) * rows, rows), rows)
        return [pltpu.make_async_copy(src.at[span], dst.at[span], sems.at[idx, order]) for idx, (src, dst) in enumerate(pairs)]

    return [load(order, hop) for order, hop in enumerate((3, 1, 2, 0))]


def forward_kernel(layer, next_gain, o_hbm, m_hbm, w_out_hbm, w_down_hbm, x_ref, gain_ref, y_ref, u_ref, o_all, m_all, w_out, w_down, row_sems, w_sems, *scatter):
    me, chip, core = ring_place()
    rows, width = x_ref.shape
    block_cols = width // PER_STEP
    loads = row_loads(((o_hbm, o_all), (m_hbm, m_all)), row_sems, CORES * rows, chip)

    def w_load(cols):
        span = pl.ds(cols * block_cols, block_cols)
        return [
            pltpu.make_async_copy(src.at[layer, :, span], dst.at[:, span], w_sems.at[idx, cols])
            for idx, (src, dst) in enumerate(((w_out_hbm, w_out), (w_down_hbm, w_down)))
        ]

    load_first = start_loads(w_load, loads)

    def load(product):
        load_first(product)
        for items, at in ((loads[2], PER_STEP), (loads[3], PER_STEP + 2 * EACH)):
            @pl.when(product == at)
            def _():
                for item in items:
                    item.wait()

    def product(dest, cols, n_cols, out):
        span = piece_at(dest, CORES * rows)
        w_span = pl.ds(pl.multiple_of(cols * block_cols, block_cols), n_cols * block_cols)
        total = dot(o_all[span], w_out[:, w_span]) + dot(m_all[span], w_down[:, w_span])
        for idx in range(n_cols):
            for kind in range(CORES):
                out[idx, kind] = total[kind * rows:(kind + 1) * rows, idx * block_cols:(idx + 1) * block_cols]

    result = scatter_blocks(None, load, product, lambda pair: None, *scatter)

    def finish(idx, carry):
        span = piece_at(idx, ROWS_AT_ONCE)
        summed = jnp.concatenate([result(cols)[span] for cols in range(PER_STEP)], axis=1)
        y = (x_ref[span].astype(F32) + summed).astype(BF16)
        y_ref[span] = y
        u_ref[span] = rms_scale(y.astype(F32), gain_ref[next_gain:next_gain + 1]).astype(BF16)
        return carry

    lax.fori_loop(0, rows // ROWS_AT_ONCE, finish, 0)


def block_output(attn_out, hidden, w_out, w_down, x_loc, norm_gain, layer):
    rows, width = x_loc.shape
    seq_len = height(attn_out)
    o_cols, ff_cols = width_of(w_out), width_of(w_down)
    shard = jax.ShapeDtypeStruct((rows, width), BF16)
    return pl.pallas_call(
        functools.partial(forward_kernel, layer, layer + 1),
        out_shape=[shard, shard],
        in_specs=[ANY] * 4 + [VMEM] * 2,
        out_specs=[VMEM] * 2,
        scratch_shapes=[
            pltpu.VMEM((seq_len, o_cols), BF16),
            pltpu.VMEM((seq_len, ff_cols), BF16),
            pltpu.VMEM((o_cols, width), BF16),
            pltpu.VMEM((ff_cols, width), BF16),
            dma_sems(2, N_CHIPS),
            dma_sems(2, PER_STEP),
        ] + scatter_scratch(rows, width),
        compiler_params=params(collective_id=5 + layer),
        name=f'block_output_{layer}',
    )(attn_out, hidden, w_out, w_down, x_loc, norm_gain)


GRAD_ROWS = N_PAIRS // 3


def backward_kernel(layer, dqkv_hbm, dgate_hbm, dup_hbm, w_qkv_hbm, w_gate_hbm, w_up_hbm, u_hbm, x_ref, dy_ref, gain_ref, *rest):
    first_layer = layer == 0
    if first_layer:
        later_gains_ref, *rest = rest
    dx_ref, dgain_ref, *rest = rest
    grads, rest = rest[:3], rest[3:]
    acts, rest = rest[:3], rest[3:]
    weights, rest = rest[:3], rest[3:]
    u_all, stage, row_sems, w_sems, u_sem, stage_sems, *rest = rest
    if first_layer:
        gain_parts, gain_send, gain_recv, *rest = rest
    scatter = rest
    me, chip, core = ring_place()
    rows, width = x_ref.shape
    block_cols = width // PER_STEP
    loads = row_loads(list(zip((dqkv_hbm, dgate_hbm, dup_hbm), acts)), row_sems, CORES * rows, chip)
    u_load = pltpu.make_async_copy(u_hbm, u_all, u_sem)

    def w_load(cols):
        span = pl.ds(cols * block_cols, block_cols)
        return [
            pltpu.make_async_copy(src.at[layer, span], dst.at[span], w_sems.at[idx, cols])
            for idx, (src, dst) in enumerate(zip((w_qkv_hbm, w_gate_hbm, w_up_hbm), weights))
        ]

    load_first = start_loads(w_load, loads)
    u_load.start()

    def load(product):
        load_first(product)

        @pl.when(product == PER_STEP)
        def _():
            for item in loads[2] + loads[3] + [u_load]:
                item.wait()

    def product(dest, cols, n_cols, out):
        span = piece_at(dest, CORES * rows)
        w_span = pl.ds(pl.multiple_of(cols * block_cols, block_cols), n_cols * block_cols)
        total = dot_nt(acts[0][span], weights[0][w_span]) + dot_nt(acts[1][span], weights[1][w_span]) + dot_nt(acts[2][span], weights[2][w_span])
        for idx in range(n_cols):
            for kind in range(CORES):
                out[idx, kind] = total[kind * rows:(kind + 1) * rows, idx * block_cols:(idx + 1) * block_cols]

    grad_rows = width // GRAD_ROWS

    def grad_out(which, part):
        slot = which % BUFFERS
        src = stage.at[slot, :, :width_of(grads[which])]
        return pltpu.make_async_copy(src, grads[which].at[piece_at(part, grad_rows)], stage_sems.at[slot])

    def beside(task):
        part = task // 3
        cols = piece_at(part, grad_rows)
        for turn, which in enumerate((2, 1, 0)):
            @pl.when(task % 3 == turn)
            def _():
                if which == 2:
                    @pl.when(part > 0)
                    def _():
                        grad_out(0, part - 1).wait()
                elif which == 0:
                    grad_out(2, part).wait()
                else:
                    @pl.when(part > 0)
                    def _():
                        grad_out(1, part - 1).wait()
                stage[which % BUFFERS, :, :width_of(grads[which])] = dot_tn(u_all[:, cols], acts[which][...]).astype(BF16)
                grad_out(which, part).start()

    peers = [(me + 1 + idx) % (N_DEVICES) for idx in range(N_DEVICES - 1)] if first_layer else None
    result = scatter_blocks(peers, load, product, beside, *scatter)
    gain_row = gain_ref[layer:layer + 1]
    dgain = gain_parts.at[me, layer:layer + 1] if first_layer else dgain_ref
    dgain[...] = jnp.zeros_like(dgain)

    def row_values(idx):
        span = piece_at(idx, ROWS_AT_ONCE)
        summed = jnp.concatenate([result(cols)[span] for cols in range(PER_STEP)], axis=1)
        x_f32 = x_ref[span].astype(F32)
        inv_rms = lax.rsqrt(row_mean(x_f32 * x_f32) + NORM_EPS)
        return span, summed.astype(BF16).astype(F32), x_f32, inv_rms

    def gain_rows(idx, carry):
        _, d_normed, x_f32, inv_rms = row_values(idx)
        dgain[...] += jnp.sum(d_normed * (x_f32 * inv_rms), axis=0, keepdims=True)
        return carry

    def input_rows(idx, carry):
        span, d_normed, x_f32, inv_rms = row_values(idx)
        scaled = d_normed * gain_row
        mix = row_mean(scaled * x_f32) * (inv_rms * inv_rms * inv_rms)
        dx_ref[span] = (dy_ref[span].astype(F32) + (scaled * inv_rms - x_f32 * mix)).astype(BF16)
        return carry

    lax.fori_loop(0, rows // ROWS_AT_ONCE, gain_rows, 0)
    if first_layer:
        gain_parts[me, 1:] = later_gains_ref[...]
        copies = [remote_copy(gain_parts.at[me], gain_parts.at[me], gain_send.at[idx], gain_recv.at[me], peer) for idx, peer in enumerate(peers)]
        for item in copies:
            item.start()
    lax.fori_loop(0, rows // ROWS_AT_ONCE, input_rows, 0)
    if first_layer:
        for idx, peer in enumerate(peers):
            remote_copy(gain_parts.at[peer], gain_parts.at[peer], gain_send.at[idx], gain_recv.at[peer], peer).wait_recv()
        total = gain_parts[0]
        for idx in range(1, N_DEVICES):
            total = total + gain_parts[idx]
        dgain_ref[...] = total
        for item in copies:
            item.wait_send()
    grad_out(0, GRAD_ROWS - 1).wait()
    grad_out(1, GRAD_ROWS - 1).wait()


def block_input_backward(d_qkv, d_gate, d_up, w_qkv, w_gate, w_up, u_full, x_loc, dy_loc, norm_gain, later_gains, layer):
    rows, width = x_loc.shape
    seq_len = height(d_qkv)
    n_layers = height(norm_gain)
    all_cols = (w_qkv.shape[2], w_gate.shape[2], w_up.shape[2])
    first_layer = layer == 0
    out_shape = [jax.ShapeDtypeStruct((rows, width), BF16), jax.ShapeDtypeStruct((n_layers if first_layer else 1, width), F32)]
    out_shape += [jax.ShapeDtypeStruct((width, cols), BF16) for cols in all_cols]
    scratch = [pltpu.VMEM((seq_len, cols), BF16) for cols in all_cols]
    scratch += [pltpu.VMEM((width, cols), BF16) for cols in all_cols]
    scratch += [pltpu.VMEM((seq_len, width), BF16), pltpu.VMEM((2, width // GRAD_ROWS, max(all_cols)), BF16)]
    scratch += [dma_sems(3, N_CHIPS), dma_sems(3, PER_STEP), pltpu.SemaphoreType.DMA, dma_sems(2)]
    if first_layer:
        scratch += [pltpu.VMEM((N_DEVICES, n_layers, width), F32), dma_sems(N_DEVICES - 1), dma_sems(N_DEVICES)]
    return pl.pallas_call(
        functools.partial(backward_kernel, layer),
        out_shape=out_shape,
        in_specs=[ANY] * 7 + [VMEM] * (4 if first_layer else 3),
        out_specs=[VMEM] * 2 + [ANY] * 3,
        scratch_shapes=scratch + scatter_scratch(rows, width),
        compiler_params=params(collective_id=7 + layer),
        name=f'block_input_backward_{layer}',
    )(d_qkv, d_gate, d_up, w_qkv, w_gate, w_up, u_full, x_loc, dy_loc, norm_gain, *((later_gains,) if first_layer else ()))


COLLECT_SLOTS = 3


def collect_kernel(moves, steps, dy_hbm, attn_hbm, hidden_hbm, *refs):
    ins, refs = refs[:len(moves)], refs[len(moves):]
    n_outs = 1 + max(out for out, _ in moves)
    outs, refs = refs[:n_outs], refs[n_outs:]
    buffers, refs = refs[:len(moves)], refs[len(moves):]
    dy_full, attn_out, hidden, stage, in_sems, out_sems, whole_sems, dy_sems, grad_sems = refs
    o_cols, cols = width_of(attn_out), width_of(dy_full) // steps

    def move(idx, step, back):
        rows = width_of(buffers[idx])
        span = piece_at(step, rows)
        slot = step % COLLECT_SLOTS
        out, layer = moves[idx]
        dst = outs[out].at[span] if layer is None else outs[out].at[layer, span]
        if back:
            return pltpu.make_async_copy(buffers[idx].at[slot], dst, out_sems.at[idx, slot])
        return pltpu.make_async_copy(ins[idx].at[span], buffers[idx].at[slot], in_sems.at[idx, slot])

    def moves_of(step, back):
        return [move(idx, step, back) for idx in range(len(moves))]

    def dy_load(step):
        span = piece_at(step, cols)
        return pltpu.make_async_copy(dy_hbm.at[:, span], dy_full.at[:, span], dy_sems.at[step])

    def grads(step):
        span = piece_at(step, cols)
        slot = step % BUFFERS
        return (
            pltpu.make_async_copy(stage.at[slot, :o_cols], outs[1].at[1, :, span], grad_sems.at[slot, 0]),
            pltpu.make_async_copy(stage.at[slot, o_cols:], outs[2].at[1, :, span], grad_sems.at[slot, 1]),
        )

    whole = [pltpu.make_async_copy(attn_hbm, attn_out, whole_sems.at[0]), pltpu.make_async_copy(hidden_hbm, hidden, whole_sems.at[1])]
    for item in moves_of(0, False) + whole + [dy_load(0)] + moves_of(1, False):
        item.start()
    for step in range(1, steps):
        dy_load(step).start()
    for item in whole:
        item.wait()

    def body(step, carry):
        @pl.when((step >= 1) & (step + 2 <= steps))
        def _():
            @pl.when(step >= COLLECT_SLOTS - 1)
            def _():
                for item in moves_of(step + 1 - COLLECT_SLOTS, True):
                    item.wait()

            for item in moves_of(step + 1, False):
                item.start()

        for item in moves_of(step, False):
            item.wait()
        for item in moves_of(step, True):
            item.start()

        @pl.when(step >= 2)
        def _():
            for item in grads(step - 2):
                item.wait()

        dy_load(step).wait()
        dy_cols = dy_full[:, piece_at(step, cols)]
        slot = step % BUFFERS
        stage[slot, :o_cols] = dot_tn(attn_out[...], dy_cols).astype(BF16)
        stage[slot, o_cols:] = dot_tn(hidden[...], dy_cols).astype(BF16)
        for item in grads(step):
            item.start()
        return carry

    lax.fori_loop(0, steps, body, 0)
    for step in range(steps - COLLECT_SLOTS, steps):
        for item in moves_of(step, True):
            item.wait()
    for item in grads(steps - 2) + grads(steps - 1):
        item.wait()


def collect(grad_x, dy_full, attn_out, hidden, g_out_first, g_down_first, made, steps):
    n_layers = len(made[0])
    assert n_layers == 2
    seq_len, width, o_cols, ff_cols = height(dy_full), width_of(dy_full), width_of(attn_out), width_of(hidden)
    sources = [(grad_x, 0, None), (g_out_first, 1, 0), (g_down_first, 2, 0)]
    sources += [(item, 3 + idx, layer) for idx, layers in enumerate(made) for layer, item in enumerate(layers)]
    moves = [(out, layer) for _, out, layer in sources]
    out_shape = [jax.ShapeDtypeStruct(grad_x.shape, BF16), jax.ShapeDtypeStruct((n_layers, o_cols, width), BF16), jax.ShapeDtypeStruct((n_layers, ff_cols, width), BF16)]
    out_shape += [jax.ShapeDtypeStruct((n_layers,) + layers[0].shape, BF16) for layers in made]
    scratch = [pltpu.VMEM((COLLECT_SLOTS, height(item) // steps, width_of(item)), BF16) for item, _, _ in sources]
    scratch += [pltpu.VMEM(item.shape, BF16) for item in (dy_full, attn_out, hidden)]
    scratch += [
        pltpu.VMEM((2, o_cols + ff_cols, width // steps), BF16),
        pltpu.SemaphoreType.DMA((len(moves), COLLECT_SLOTS)),
        pltpu.SemaphoreType.DMA((len(moves), COLLECT_SLOTS)),
        dma_sems(2),
        dma_sems(steps),
        dma_sems(2, 2),
    ]
    return pl.pallas_call(
        functools.partial(collect_kernel, moves, steps),
        out_shape=out_shape,
        in_specs=[ANY] * (3 + len(moves)),
        out_specs=[ANY] * len(out_shape),
        scratch_shapes=scratch,
        compiler_params=params(),
        name='collect',
    )(dy_full, attn_out, hidden, *[item for item, _, _ in sources])


def causal_tile(size):
    return lax.broadcasted_iota(jnp.int32, (size, size), 0) >= lax.broadcasted_iota(jnp.int32, (size, size), 1)


def masked_scores(query, keys):
    size = height(query)
    q_start = height(keys) - size
    scores = dot_nt(query, keys)
    diagonal = jnp.where(causal_tile(size), scores[:, q_start:], -1e30)
    scores = diagonal if q_start == 0 else jnp.concatenate([scores[:, :q_start], diagonal], axis=1)
    return scores * (SCALE * LOG2E)


def head_cols(head, part, parts):
    return pl.ds(pl.multiple_of((head * parts + part) * HEAD_DIM, HEAD_DIM), HEAD_DIM)


def attend_rows(q_start, head, qkv_ref, o_ref, lse_ref):
    span, seen = slice(q_start, q_start + Q_ROWS), slice(0, q_start + Q_ROWS)
    scores = masked_scores(qkv_ref[span, head_cols(head, 0, 3)], qkv_ref[seen, head_cols(head, 1, 3)])
    row_max = jnp.max(scores, axis=-1, keepdims=True)
    prob = jnp.exp2(scores - row_max)
    norm = row_sum(prob)
    prob = (prob * (1.0 / norm)).astype(BF16)
    o_ref[span, head_cols(head, 0, 1)] = dot(prob, qkv_ref[seen, head_cols(head, 2, 3)]).astype(BF16)
    lse_ref[span, head_cols(head, 0, 1)] = jnp.broadcast_to(row_max + jnp.log2(norm), (Q_ROWS, HEAD_DIM))


def attend_rows_backward(q_start, head, qkv_ref, lse_ref, do_ref, o_ref, cos_ref, sin_ref, dq_ref, dkt_acc, dvt_acc, prob_tmp, ds_tmp):
    span, seen = slice(q_start, q_start + Q_ROWS), slice(0, q_start + Q_ROWS)
    query = qkv_ref[span, head_cols(head, 0, 3)]
    d_out = do_ref[span, head_cols(head, 0, 1)]
    inner = row_sum(d_out.astype(F32) * o_ref[span, head_cols(head, 0, 1)].astype(F32))
    lse = lse_ref[span, head_cols(head, 0, 1)][:, :1]
    for k_start in range(0, q_start + Q_ROWS, Q_ROWS):
        keys = slice(k_start, k_start + Q_ROWS)
        scores = dot_nt(query, qkv_ref[keys, head_cols(head, 1, 3)]) * (SCALE * LOG2E)
        if k_start == q_start:
            scores = jnp.where(causal_tile(Q_ROWS), scores, -1e30)
        prob = jnp.exp2(scores - lse)
        d_prob = dot_nt(d_out, qkv_ref[keys, head_cols(head, 2, 3)]).astype(BF16).astype(F32)
        ds_tmp[:, keys] = (prob * (d_prob - inner) * SCALE).astype(BF16)
        prob_tmp[:, keys] = prob.astype(BF16)
    dvt_acc[head, :, seen] += dot_tn(d_out, prob_tmp[:, seen])
    dkt_acc[head, :, seen] += dot_tn(query, ds_tmp[:, seen])
    d_query = dot(ds_tmp[:, seen], qkv_ref[seen, head_cols(head, 1, 3)]).astype(BF16)
    dq_ref[span, head_cols(head, 0, 3)] = rotate(d_query.astype(F32), cos_ref[span], -sin_ref[span]).astype(BF16)


def attention_kernel(qkv_ref, o_ref, lse_ref):
    for q_start in range(0, height(qkv_ref), Q_ROWS):
        attend_rows(q_start, 0, qkv_ref, o_ref, lse_ref)


def attention(qkv):
    seq_len, cols = qkv.shape
    heads = cols // (3 * HEAD_DIM)
    return pl.pallas_call(
        attention_kernel,
        grid=(heads,),
        out_shape=[jax.ShapeDtypeStruct((seq_len, heads * HEAD_DIM), BF16), jax.ShapeDtypeStruct((seq_len, heads * HEAD_DIM), F32)],
        in_specs=[pl.BlockSpec((seq_len, 3 * HEAD_DIM), lambda h: (0, h))],
        out_specs=[pl.BlockSpec((seq_len, HEAD_DIM), lambda h: (0, h))] * 2,
        compiler_params=params(semantics=('arbitrary',)),
        name='attention',
    )(qkv)


def middle_kernel(layer, with_forward, dy_hbm, u_hbm, w_out_hbm, w_down_hbm, gate_hbm, up_hbm, cos_hbm, sin_hbm, qkv_hbm, *rest):
    if not with_forward:
        (o_hbm, lse_hbm), rest = rest[:2], rest[2:]
    (dgate_hbm, dup_hbm, dqkv_hbm, u_full_hbm), rest = rest[:4], rest[4:]
    if with_forward:
        (dy_full_hbm, o_hbm, hidden_hbm), rest = rest[:3], rest[3:]
    else:
        (g_out_hbm, g_down_hbm), rest = rest[:2], rest[2:]
    (dgate_stage, dup_stage, gate_in, up_in, weights, qkv, o_all, lse, hidden, d_attn, dqkv, dk_acc, dv_acc, prob_tmp, ds_tmp, grad_stage, cos_ref, sin_ref), rest = rest[:18], rest[18:]
    dy_full, dy_send, dy_recv, u_full, u_send, u_recv, load_sems, out_sems, in_sems, u_sems, dqkv_sem, grad_sems = rest
    rows = width_of(dy_full)
    half = rows // 2
    seq_len = height(qkv)
    n_heads = width_of(o_all) // HEAD_DIM
    o_cols = width_of(o_all)
    gather = Gather(dy_full, dy_send, dy_recv)
    u_gather = Gather(u_full, u_send, u_recv)
    me = gather.me
    own_dy = pltpu.make_async_copy(dy_hbm, dy_full.at[me], load_sems.at[0])
    own_u = pltpu.make_async_copy(u_hbm, u_full.at[me], load_sems.at[1])
    w_loads = [
        pltpu.make_async_copy(w_out_hbm.at[layer], weights.at[:o_cols], load_sems.at[2]),
        pltpu.make_async_copy(w_down_hbm.at[layer], weights.at[o_cols:], load_sems.at[3]),
    ]
    loads = [
        pltpu.make_async_copy(src, dst, load_sems.at[4 + idx])
        for idx, (src, dst) in enumerate([(qkv_hbm, qkv), (cos_hbm, cos_ref), (sin_hbm, sin_ref)] + ([] if with_forward else [(o_hbm, o_all), (lse_hbm, lse)]))
    ]
    writer = RowWriter((dgate_stage, dup_stage), (dgate_hbm, dup_hbm), out_sems, rows)
    own_dy.start()
    meet(gather.peers())
    own_dy.wait()
    gather.launch()
    for item in w_loads + loads + [own_u]:
        item.start()
    dk_acc[...] = jnp.zeros_like(dk_acc)
    dv_acc[...] = jnp.zeros_like(dv_acc)
    for item in w_loads:
        item.wait()

    def both_heads(function, q_start, *args):
        def body(head, carry):
            function(q_start, head, *args)
            return carry

        lax.fori_loop(0, n_heads, body, 0)

    def attend(index):
        run_at(index, [functools.partial(both_heads, attend_rows, q_start, qkv, o_all, lse) for q_start in range(0, seq_len, Q_ROWS)])

    def attend_backward(index):
        refs = (qkv, lse, d_attn, o_all, cos_ref, sin_ref, dqkv, dk_acc, dv_acc, prob_tmp, ds_tmp)
        run_at(index, [functools.partial(both_heads, attend_rows_backward, q_start, *refs) for q_start in range(0, seq_len, Q_ROWS)])

    def finish_keys_values():
        def body(idx, carry):
            span = piece_at(idx, Q_ROWS)
            for head in range(n_heads):
                d_keys = dk_acc[head, :, span].T.astype(BF16).astype(F32)
                dqkv[span, head_cols(head, 1, 3)] = rotate(d_keys, cos_ref[span], -sin_ref[span]).astype(BF16)
                dqkv[span, head_cols(head, 2, 3)] = dv_acc[head, :, span].T.astype(BF16)
            return carry

        lax.fori_loop(0, seq_len // Q_ROWS, body, 0)
        keep_dqkv.start()

    keep_dqkv = pltpu.make_async_copy(dqkv, dqkv_hbm, dqkv_sem)

    def dy_rows(step):
        run_at(step, gather.events(early=True))

        @pl.when(step == N_DEVICES - 2)
        def _():
            own_u.wait()
            u_gather.launch_both()
            keep_u(me)

        places = gather.places(step)
        slot = step % BUFFERS
        fetch = []
        for idx, (src, dst) in enumerate(((gate_hbm, gate_in), (up_hbm, up_in))):
            for part, (shard, row) in enumerate(places):
                here = pl.ds(pl.multiple_of(shard * rows + row, half), half)
                fetch.append(pltpu.make_async_copy(src.at[here], dst.at[pl.ds(part * half, half)], in_sems.at[idx, part]))
        for item in fetch:
            item.start()
        writer.reuse(step)
        product = dot_nt(both_halves(dy_full, places, half), weights[...]).astype(BF16)
        d_hidden = product[:, o_cols:].astype(F32)
        for item in fetch:
            item.wait()
        gate, up = gate_in[...].astype(F32), up_in[...].astype(F32)
        sig = jax.nn.sigmoid(gate)
        act = gate * sig
        hidden_rows = (act * up).astype(BF16)
        for part, (shard, row) in enumerate(places):
            here = pl.ds(pl.multiple_of(shard * rows + row, half), half)
            d_attn[here] = product[part * half:(part + 1) * half, :o_cols]
            hidden[here] = hidden_rows[part * half:(part + 1) * half]
        dgate_stage[slot] = (d_hidden * up * (sig + act * (1.0 - sig))).astype(BF16)
        dup_stage[slot] = (d_hidden * act).astype(BF16)
        writer.start(step, places)

    def wait_loads(step):
        @pl.when(step == 0)
        def _():
            for item in loads:
                item.wait()

    def dy_step_forward(step, carry):
        dy_rows(step)
        wait_loads(step)
        attend(seq_len // Q_ROWS - 1 - step)
        return carry

    def dy_step_backward(step, carry):
        @pl.when(step < N_DEVICES)
        def _():
            dy_rows(step)

        wait_loads(step)
        after = step // (N_DEVICES)
        turn = (1 - after) * (step // 2) + after * (step - 5)
        upper, lower = gather.places(turn)
        shard = upper[0] + (turn // 7) * (lower[0] - upper[0])

        @pl.when(step == 10)
        def _():
            u_gather.pass_piece(0)

        @pl.when(step == 12)
        def _():
            u_gather.pass_piece(1)

        @pl.when((step == 0) | (step == 3) | (step == 5) | (step >= N_DEVICES))
        def _():
            attend_backward(shard * rows // Q_ROWS)

        return carry

    def keep_u(shard):
        pltpu.make_async_copy(u_full.at[shard], u_full_hbm.at[shard], u_sems.at[shard]).start()

    if with_forward:
        lax.fori_loop(0, N_DEVICES, dy_step_forward, 0)
    else:
        lax.fori_loop(0, N_DEVICES + 5, dy_step_backward, 0)

    def grad_copies(step):
        slot = step % BUFFERS
        cols = piece_at(step, grad_cols)
        return (
            pltpu.make_async_copy(grad_stage.at[slot, :o_cols], g_out_hbm.at[:, cols], grad_sems.at[slot, 0]),
            pltpu.make_async_copy(grad_stage.at[slot, o_cols:], g_down_hbm.at[:, cols], grad_sems.at[slot, 1]),
        )

    grad_cols = dy_full.shape[2] // (N_DEVICES)
    first_parts, last_parts = u_gather.pass_piece, u_gather.end_piece
    if with_forward:
        u_at = {1: [0], 2: [1], 4: [2], 7: [3]}
    else:
        u_at = {1: [2], 4: [3], 6: [4], 7: [5]}

    def u_event(at):
        for part in u_at.get(at, ()):
            first_parts(part) if part < SUBS else last_parts(part - SUBS)
        if at == 2 and not with_forward:
            finish_keys_values()

    u_events = [functools.partial(u_event, at) for at in range(N_DEVICES)]
    last_part = max(part for parts in u_at.values() for part in parts) + 1

    def u_step(step, carry):
        run_at(step, u_events)
        if with_forward:
            attend_backward(seq_len // Q_ROWS - 1 - step)
            return carry

        @pl.when(step >= 2)
        def _():
            for item in grad_copies(step - 2):
                item.wait()

        cols = piece_at(step, grad_cols)
        dy_cols = dy_full[:, :, cols].reshape(seq_len, grad_cols)
        slot = step % BUFFERS
        grad_stage[slot, :o_cols] = dot_tn(o_all[...], dy_cols).astype(BF16)
        grad_stage[slot, o_cols:] = dot_tn(hidden[...], dy_cols).astype(BF16)
        for item in grad_copies(step):
            item.start()
        return carry

    if with_forward:
        keeps = [pltpu.make_async_copy(src, dst, grad_sems.at[0, idx]) for idx, (src, dst) in enumerate(((o_all, o_hbm), (hidden, hidden_hbm)))]
        keeps += [pltpu.make_async_copy(dy_full, dy_full_hbm, grad_sems.at[1, 0])]
        for item in keeps:
            item.start()
    lax.fori_loop(0, N_DEVICES, u_step, 0)
    if with_forward:
        finish_keys_values()
    for shard in (u_gather.partner, u_gather.first_other, u_gather.second_other):
        u_gather.arrived(shard)
        keep_u(shard)
    for shard in (u_gather.first, u_gather.second):
        keep_u(shard)
    for part in range(last_part, 2 * SUBS):
        last_parts(part - SUBS)
    keep_u(u_gather.third)
    u_gather.arrived(u_gather.third_other)
    keep_u(u_gather.third_other)
    for item in keeps if with_forward else grad_copies(N_DEVICES - 2) + grad_copies(N_DEVICES - 1):
        item.wait()
    gather.finish()
    u_gather.finish(0)
    writer.finish()
    keep_dqkv.wait()
    for shard in range(N_DEVICES):
        pltpu.make_async_copy(u_full.at[shard], u_full_hbm.at[shard], u_sems.at[shard]).wait()


def middle(dy_loc, u_loc, w_out, w_down, gate_act, up_act, tables, qkv, attended, layer, tp_size):
    rows, width = dy_loc.shape
    seq_len = rows * tp_size
    o_cols, ff_cols, qkv_cols = width_of(w_out), width_of(w_down), width_of(qkv)
    n_heads = o_cols // HEAD_DIM
    total = o_cols + ff_cols
    outs = [(seq_len, ff_cols), (seq_len, ff_cols), (seq_len, qkv_cols), (tp_size, rows, width)]
    outs += [(o_cols, width), (ff_cols, width)] if attended else [(tp_size, rows, width), (seq_len, o_cols), (seq_len, ff_cols)]
    scratch = [pltpu.VMEM((2, rows, ff_cols), BF16)] * 2
    scratch += [pltpu.VMEM((rows, ff_cols), BF16)] * 2
    scratch += [
        pltpu.VMEM((total, width), BF16),
        pltpu.VMEM((seq_len, qkv_cols), BF16),
        pltpu.VMEM((seq_len, o_cols), BF16),
        pltpu.VMEM((seq_len, o_cols), F32),
        pltpu.VMEM((seq_len, ff_cols), BF16),
        pltpu.VMEM((seq_len, o_cols), BF16),
        pltpu.VMEM((seq_len, qkv_cols), BF16),
        pltpu.VMEM((n_heads, HEAD_DIM, seq_len), F32),
        pltpu.VMEM((n_heads, HEAD_DIM, seq_len), F32),
        pltpu.VMEM((Q_ROWS, seq_len), BF16),
        pltpu.VMEM((Q_ROWS, seq_len), BF16),
        pltpu.VMEM((2, total, width // (N_DEVICES)), BF16),
    ]
    scratch += [pltpu.VMEM(table.shape, F32) for table in tables]
    scratch += gather_scratch(tp_size, rows, width) + gather_scratch(tp_size, rows, width)
    scratch += [
        dma_sems(9),
        dma_sems(2, 2, 2),
        dma_sems(2, 2),
        dma_sems(tp_size),
        pltpu.SemaphoreType.DMA,
        dma_sems(2, 2),
    ]
    return pl.pallas_call(
        functools.partial(middle_kernel, layer, not attended),
        out_shape=[jax.ShapeDtypeStruct(shape, BF16) for shape in outs],
        in_specs=[ANY] * (9 + len(attended)),
        out_specs=[ANY] * len(outs),
        scratch_shapes=scratch,
        compiler_params=params(collective_id=3 + layer),
        name=f'middle_{layer}',
    )(dy_loc, u_loc, w_out, w_down, gate_act, up_act, *tables, qkv, *attended)


def solution(mesh):
    tp_size = mesh.shape['tp']
    assert tp_size == N_DEVICES
    row_spec = P(('dp', 'tp'), None)
    col_spec = P(None, None, 'tp')
    inner_spec = P(None, 'tp', None)

    def device_program(x_loc, dy_loc, norm_gain, w_qkv, w_out, w_gate, w_up, w_down):
        n_layers = height(w_qkv)
        seq_len = height(x_loc) * tp_size
        tables = tuple(jnp.asarray(table) for table in rope_tables(seq_len, FINE))
        x_cur, source = x_loc, x_loc
        saved = []
        for layer in range(n_layers):
            first, last = layer == 0, layer == n_layers - 1
            qkv, gate_act, up_act, *more = project(source, norm_gain, w_qkv, w_gate, w_up, tables, layer, tp_size, first)
            u_loc = more[1] if first else source
            tables = more[2:] if first else tables
            if last:
                saved.append((x_cur, u_loc, qkv, gate_act, up_act, ()))
            else:
                attended = attention(qkv)
                saved.append((x_cur, u_loc, qkv, gate_act, up_act, tuple(attended)))
                x_cur, source = block_output(attended[0], more[0], w_out, w_down, x_cur, norm_gain, layer)
        grad_cur = dy_loc
        grads, gains = [None] * n_layers, ()
        for layer in reversed(range(n_layers)):
            x_cur, u_loc, qkv, gate_act, up_act, attended = saved[layer]
            d_gate, d_up, d_qkv, u_full, *more = middle(grad_cur, u_loc, w_out, w_down, gate_act, up_act, tables, qkv, attended, layer, tp_size)
            u_full = u_full.reshape(seq_len, u_full.shape[2])
            later_gains = jnp.concatenate(gains, axis=0) if gains else None
            grad_cur, gain_grad, g_qkv, g_gate, g_up = block_input_backward(
                d_qkv, d_gate, d_up, w_qkv, w_gate, w_up, u_full, x_cur, grad_cur, norm_gain, later_gains, layer
            )
            grads[layer] = (g_qkv, g_gate, g_up)
            if layer == n_layers - 1:
                dy_full, attn_out, hidden = more
            gains = (gain_grad,) + gains
        grad_x, g_out, g_down, g_qkv, g_gate, g_up = collect(grad_cur, dy_full.reshape(seq_len, -1), attn_out, hidden, *more, list(zip(*grads)), 8)
        return (grad_x, gains[0], g_qkv, g_out, g_gate, g_up, g_down)

    return jax.shard_map(
        device_program,
        mesh=mesh,
        in_specs=(row_spec, row_spec, P(None, None), col_spec, inner_spec, col_spec, col_spec, inner_spec),
        out_specs=(row_spec, P('dp', None), P('dp', None, 'tp'), P('dp', 'tp', None), P('dp', None, 'tp'), P('dp', None, 'tp'), P('dp', 'tp', None)),
        check_vma=False,
    )
```

```python
import functools

import jax
import jax.numpy as jnp
import numpy as np
from jax import lax
from jax.experimental import pallas as pl
from jax.experimental.pallas import tpu as pltpu
from jax.sharding import PartitionSpec as P

HEAD_DIM = 128
NORM_EPS = 1e-5
ROPE_BASE = 10000.0
SCALE = HEAD_DIM ** -0.5
LOG2E = 1.4426950408889634
VMEM_LIMIT = 64000 * 1024
CORES = 2
N_CHIPS = 4
N_DEVICES = CORES * N_CHIPS
WAYS = 2
BUFFERS = 2
SUBS = 4
Q_ROWS = 256
ROWS_AT_ONCE = 32
FINE = 128
BF16 = jnp.bfloat16
F32 = jnp.float32
ANY = pl.BlockSpec(memory_space=pl.ANY)
VMEM = pl.BlockSpec(memory_space=pltpu.VMEM)
NT = (((1,), (1,)), ((), ()))
TN = (((0,), (0,)), ((), ()))


def height(array):
    return array.shape[0]


def width_of(array):
    return array.shape[1]


def piece_at(idx, size):
    return pl.ds(pl.multiple_of(idx * size, size), size)


def loop(count, body):
    lax.fori_loop(0, count, body, 0)


def dma_sems(*shape):
    return pltpu.SemaphoreType.DMA(shape)


def dot(lhs, rhs):
    return jnp.dot(lhs, rhs, preferred_element_type=F32)


def dot_nt(lhs, rhs):
    return lax.dot_general(lhs, rhs, NT, preferred_element_type=F32)


def dot_tn(lhs, rhs):
    return lax.dot_general(lhs, rhs, TN, preferred_element_type=F32)


def params(collective_id=None, semantics=None):
    if collective_id is None:
        return pltpu.CompilerParams(vmem_limit_bytes=VMEM_LIMIT, dimension_semantics=semantics)
    return pltpu.CompilerParams(vmem_limit_bytes=VMEM_LIMIT, collective_id=collective_id, has_side_effects=True)


def row_mean(values):
    return jnp.mean(values, axis=-1, keepdims=True)


def row_sum(values):
    return jnp.sum(values, axis=-1, keepdims=True)


def rope_tables(seq_len, fine):
    half_dim = HEAD_DIM // 2
    freqs = np.float32(ROPE_BASE) ** (np.float32(-2.0) * np.arange(half_dim, dtype=np.float32) / np.float32(HEAD_DIM))
    tables = []
    for positions in (np.arange(fine), np.arange(0, seq_len, fine)):
        angles = positions.astype(np.float32)[:, None] * freqs[None, :]
        tables += [np.tile(np.cos(angles), 2).astype(np.float32), np.tile(np.sin(angles), 2).astype(np.float32)]
    return tables


def fill_rope(fine_cos, fine_sin, coarse_cos, coarse_sin, cos_ref, sin_ref):
    fine = height(fine_cos)
    sign = jnp.where(lax.broadcasted_iota(jnp.int32, (1, HEAD_DIM), 1) < HEAD_DIM // 2, -1.0, 1.0)

    def body(idx, carry):
        span = piece_at(idx, fine)
        big_cos, big_sin = coarse_cos[pl.ds(idx, 1)], coarse_sin[pl.ds(idx, 1)]
        cos_ref[span] = big_cos * fine_cos[...] - big_sin * fine_sin[...]
        sin_ref[span] = (big_sin * fine_cos[...] + big_cos * fine_sin[...]) * sign
        return carry

    loop(height(cos_ref) // fine, body)


def rotate(values, cos_tab, sin_tab):
    return values * cos_tab + pltpu.roll(values, HEAD_DIM // 2, 1) * sin_tab


def rms_scale(x_f32, gain_row):
    inv_rms = lax.rsqrt(row_mean(x_f32 * x_f32) + NORM_EPS)
    return x_f32 * inv_rms * gain_row


def ring_place():
    me = lax.axis_index('tp')
    chip = me // 2
    core = me % 2
    return me, chip, core


def device_at(chip, core):
    return ((chip + N_CHIPS) % N_CHIPS) * 2 + core


def remote_copy(src, dst, send_sem, recv_sem, peer):
    return pltpu.make_async_remote_copy(
        src_ref=src, dst_ref=dst, send_sem=send_sem, recv_sem=recv_sem, device_id={'tp': peer}, device_id_type=pl.DeviceIdType.MESH
    )


def meet(peers):
    barrier = pltpu.get_barrier_semaphore()
    for peer in peers:
        pl.semaphore_signal(barrier, inc=1, device_id={'tp': peer}, device_id_type=pl.DeviceIdType.MESH)
    pl.semaphore_wait(barrier, len(peers))


OWN_PARTNER, OWN_AHEAD, OWN_BEHIND, FIRST_PARTNER, FIRST_AHEAD, SECOND_PARTNER, THIRD_PARTNER = KINDS = range(7)


class Gather:
    EVERY, EARLY, LATE = range(SUBS), range(SUBS // 2), range(SUBS // 2, SUBS)

    def __init__(self, full, send_sems, recv_sems):
        self.full, self.send_sems, self.recv_sems = full, send_sems, recv_sems
        self.me, chip, core = ring_place()
        turn = 1 - 2 * core
        self.chip, self.core, self.turn = chip, core, turn
        self.partner = device_at(chip, 1 - core)
        self.ahead = device_at(chip + turn, core)
        self.behind = device_at(chip - turn, core)
        self.first = device_at(chip - turn, core)
        self.first_other = device_at(chip + turn, 1 - core)
        self.second = device_at(chip + turn, core)
        self.second_other = device_at(chip - turn, 1 - core)
        self.third = device_at(chip + 2, core)
        self.third_other = device_at(chip + 2, 1 - core)

    def peers(self):
        return self.partner, self.ahead, self.behind

    def piece(self, kind, shard, sub, peer):
        rows = width_of(self.full) // SUBS
        part = self.full.at[shard, pl.ds(sub * rows, rows)]
        return remote_copy(part, part, self.send_sems.at[kind, sub], self.recv_sems.at[shard, sub], peer)

    def send(self, kind, shard, peer, subs=EVERY):
        for sub in subs:
            self.piece(kind, shard, sub, peer).start()

    def sent(self, kind, shard, peer, subs=EVERY):
        for sub in subs:
            self.piece(kind, shard, sub, peer).wait_send()

    def arrived(self, shard, subs=EVERY, pass_on=None):
        for sub in subs:
            self.piece(OWN_PARTNER, shard, sub, self.partner).wait_recv()
            if pass_on is not None:
                self.piece(pass_on, shard, sub, self.partner).start()

    def launch(self, subs=EVERY):
        self.send(OWN_AHEAD, self.me, self.ahead, subs)
        self.send(OWN_PARTNER, self.me, self.partner, subs)

    def turn_back(self):
        self.sent(OWN_AHEAD, self.me, self.ahead, range(SUBS - 1))
        self.send(OWN_BEHIND, self.me, self.behind)

    def pass_ahead(self):
        self.sent(OWN_BEHIND, self.me, self.behind, range(SUBS - 1))
        self.send(FIRST_AHEAD, self.first, self.ahead)

    def launch_both(self):
        self.launch()
        self.send(OWN_BEHIND, self.me, self.behind)

    def pass_piece(self, sub):
        self.piece(OWN_PARTNER, self.first, sub, self.partner).wait_recv()
        self.piece(FIRST_AHEAD, self.first, sub, self.ahead).start()
        self.piece(FIRST_PARTNER, self.first, sub, self.partner).start()
        self.arrived(self.second, (sub,), SECOND_PARTNER)

    def end_piece(self, sub):
        self.arrived(self.third, (sub,), THIRD_PARTNER)

    def events(self, early=False):
        return (
            lambda: None,
            lambda: (self.turn_back(), self.arrived(self.partner)),
            lambda: self.arrived(self.first, pass_on=FIRST_PARTNER),
            lambda: (self.pass_ahead() if early else None, self.arrived(self.first_other)),
            lambda: (None if early else self.pass_ahead(), self.arrived(self.second, pass_on=SECOND_PARTNER)),
            lambda: self.arrived(self.second_other),
            lambda: (self.arrived(self.third, self.EARLY, THIRD_PARTNER), self.arrived(self.third_other, self.EARLY)),
            lambda: (self.arrived(self.third, self.LATE, THIRD_PARTNER), self.arrived(self.third_other, self.LATE)),
        )

    def places(self, step):
        half = width_of(self.full) // 2
        pair = step // 2
        odd = step % BUFFERS
        side = self.turn * (1 - 2 * odd)
        hop = (3 * pair + (pair // 2) * (2 * pair - 5)) % N_CHIPS
        shard = device_at((self.chip + side * hop + N_DEVICES) % N_CHIPS, (self.core + odd) % 2)
        last = step // (N_DEVICES - 2)
        upper = (1 - last) * shard + last * self.third
        lower = (1 - last) * shard + last * self.third_other
        return (upper, last * odd * half), (lower, (1 - last) * half + last * odd * half)

    def finish(self, waited=SUBS - 1):
        self.sent(OWN_PARTNER, self.me, self.partner)
        self.sent(OWN_AHEAD, self.me, self.ahead, range(waited, SUBS))
        self.sent(OWN_BEHIND, self.me, self.behind, range(waited, SUBS))
        self.sent(FIRST_PARTNER, self.first, self.partner)
        self.sent(FIRST_AHEAD, self.first, self.ahead)
        self.sent(SECOND_PARTNER, self.second, self.partner)
        self.sent(THIRD_PARTNER, self.third, self.partner)


def run_at(step, actions):
    for idx, action in enumerate(actions):
        @pl.when(step == idx)
        def _():
            action()


def gather_scratch(tp_size, rows, width):
    return [
        pltpu.VMEM((tp_size, rows, width), BF16),
        dma_sems(len(KINDS), SUBS),
        dma_sems(tp_size, SUBS),
    ]


def half_rows(ref, place, half):
    return ref[place[0], pl.ds(pl.multiple_of(place[1], half), half)]


def both_halves(ref, places, half):
    return jnp.concatenate([half_rows(ref, place, half) for place in places], axis=0)


def table_rows(ref, places, half, rows):
    parts = [ref[pl.ds(pl.multiple_of(shard * rows + row, half), half)] for shard, row in places]
    return jnp.concatenate(parts, axis=0)


class RowWriter:
    def __init__(self, stages, outs, sems, rows):
        self.stages, self.outs, self.sems, self.rows = stages, outs, sems, rows

    def copies(self, slot, places):
        half = self.rows // 2
        items = []
        for idx in range(len(self.outs)):
            for part, (shard, row) in enumerate(places):
                start = pl.multiple_of(shard * self.rows + row, half)
                src = self.stages[idx].at[slot, pl.ds(part * half, half)]
                items.append(pltpu.make_async_copy(src, self.outs[idx].at[pl.ds(start, half)], self.sems.at[idx, slot, part]))
        return items

    def reuse(self, step):
        @pl.when(step >= 2)
        def _():
            for item in self.copies(step % BUFFERS, ((0, 0), (0, 0))):
                item.wait()

    def start(self, step, places):
        for item in self.copies(step % BUFFERS, places):
            item.start()

    def finish(self):
        for slot in range(BUFFERS):
            for item in self.copies(slot, ((0, 0), (0, 0))):
                item.wait()


def project_loads(layer, sources, weights, sems):
    loads, spans, start = [], [], 0
    for idx, src in enumerate(sources):
        spans.append(slice(start, start + src.shape[-1]))
        start += src.shape[-1]
        loads.append(pltpu.make_async_copy(src.at[layer], weights.at[:, spans[-1]], sems.at[idx]))
    return loads, spans


def project_steps(gather, weights, spans, stages, writer, cos_ref, sin_ref, with_hidden):
    rows = width_of(gather.full)
    half = rows // CORES

    def step_body(step, carry):
        run_at(step, gather.events())
        places = gather.places(step)
        slot = step % BUFFERS
        writer.reuse(step)
        cos_tab, sin_tab = table_rows(cos_ref, places, half, rows), table_rows(sin_ref, places, half, rows)
        product = dot(both_halves(gather.full, places, half), weights[...]).astype(BF16)
        qkv, gate, up = (product[:, span] for span in spans)
        for head in range(width_of(qkv) // HEAD_DIM):
            cols = slice(head * HEAD_DIM, (head + 1) * HEAD_DIM)
            part = qkv[:, cols]
            if head % 3 != 2:
                part = rotate(part.astype(F32), cos_tab, sin_tab).astype(BF16)
            stages[0][slot, :, cols] = part
        stages[1][slot] = gate
        stages[2][slot] = up
        if with_hidden:
            stages[3][slot] = (jax.nn.silu(gate.astype(F32)) * up.astype(F32)).astype(BF16)
        writer.start(step, places)
        return carry

    loop(N_DEVICES, step_body)
    gather.finish()
    writer.finish()


def project_kernel(layer, x_ref, gain_ref, w_qkv_hbm, w_gate_hbm, w_up_hbm, *rest):
    tables, rest = rest[:4], rest[4:]
    outs, rest = rest[:4], rest[4:]
    u_ref, cos_out, sin_out, *rest = rest
    stages, rest = rest[:4], rest[4:]
    cos_ref, sin_ref, weights, full, send_sems, recv_sems, w_sems, table_sems, out_sems = rest
    rows = width_of(full)
    gather = Gather(full, send_sems, recv_sems)
    loads, spans = project_loads(layer, (w_qkv_hbm, w_gate_hbm, w_up_hbm), weights, w_sems)
    keep_tables = [pltpu.make_async_copy(cos_ref, cos_out, table_sems.at[0]), pltpu.make_async_copy(sin_ref, sin_out, table_sems.at[1])]
    norm_rows = min(ROWS_AT_ONCE, rows // SUBS)

    def norm(idx, carry):
        span = piece_at(idx, norm_rows)
        normed = rms_scale(x_ref[span].astype(F32), gain_ref[layer:layer + 1]).astype(BF16)
        full[gather.me, span] = normed
        u_ref[span] = normed
        return carry

    for load in loads:
        load.start()
    meet(gather.peers())
    per_piece = rows // SUBS // norm_rows
    for sub in range(SUBS):
        lax.fori_loop(sub * per_piece, (sub + 1) * per_piece, norm, 0)
        gather.launch((sub,))
    fill_rope(*tables, cos_ref, sin_ref)
    for item in keep_tables:
        item.start()
    for load in loads:
        load.wait()
    project_steps(gather, weights, spans, stages, RowWriter(stages, outs, out_sems, rows), cos_ref, sin_ref, True)
    for item in keep_tables:
        item.wait()


def project(x_loc, norm_gain, w_qkv, w_gate, w_up, tables, layer, tp_size):
    rows, width = x_loc.shape
    seq_len = rows * tp_size
    out_cols = [item.shape[-1] for item in (w_qkv, w_gate, w_up, w_up)]
    table = (seq_len, HEAD_DIM)
    outs = [jax.ShapeDtypeStruct((seq_len, cols), BF16) for cols in out_cols]
    outs += [jax.ShapeDtypeStruct((rows, width), BF16)] + [jax.ShapeDtypeStruct(table, F32)] * 2
    scratch = [pltpu.VMEM((BUFFERS, rows, cols), BF16) for cols in out_cols]
    scratch += [pltpu.VMEM(table, F32)] * 2
    scratch += [pltpu.VMEM((width, sum(out_cols[:3])), BF16)]
    scratch += gather_scratch(tp_size, rows, width)
    scratch += [dma_sems(3), dma_sems(2), dma_sems(len(out_cols), BUFFERS, CORES)]
    return pl.pallas_call(
        functools.partial(project_kernel, layer),
        out_shape=outs,
        in_specs=[VMEM] * 2 + [ANY] * 3 + [VMEM] * len(tables),
        out_specs=[ANY] * len(out_cols) + [VMEM, ANY, ANY],
        scratch_shapes=scratch,
        compiler_params=params(collective_id=1 + layer),
        name=f'project_{layer}',
    )(x_loc, norm_gain, w_qkv, w_gate, w_up, *tables)


EACH = 4
PER_STEP = WAYS * EACH
N_BLOCKS = N_CHIPS * PER_STEP
N_PAIRS = (N_BLOCKS - PER_STEP) // 2
SLOTS = 6


def scatter_blocks(peers, load, early, product, beside, tmp, acc, ring, pair_send, pair_recv, ring_send, ring_recv):
    me, chip, core = ring_place()
    partner = device_at(chip, 1 - core)
    meet(peers or (partner, device_at(chip + 1, core), device_at(chip - 1, core)))

    def dest(step, way):
        return (chip + (step + 1) * (WAYS * way - 1) + N_DEVICES) % N_CHIPS

    def to_partner(block, slot):
        return remote_copy(tmp.at[slot, 1 - core], acc.at[block], pair_send.at[slot], pair_recv.at[block], partner)

    def to_next(block):
        peer = device_at(chip + 1 - 2 * (block % WAYS), core)
        return remote_copy(acc.at[block], ring.at[block], ring_send.at[block], ring_recv.at[block], peer)

    def serve_first(block):
        to_partner(block, block % SLOTS).wait_recv()
        acc[block] = acc[block] + tmp[block % SLOTS, core]
        to_next(block).start()

    def first_body(block, carry):
        load(block)
        early(block)

        @pl.when(block >= SLOTS)
        def _():
            to_partner(block - SLOTS, block % SLOTS).wait_send()

        way = block % WAYS
        product(dest(0, way), way * EACH + block // WAYS, 1, tmp.at[pl.ds(block % SLOTS, 1)])
        to_partner(block, block % SLOTS).start()

        @pl.when(block >= 1)
        def _():
            serve_first(block - 1)

        return carry

    loop(PER_STEP, first_body)

    def pair_blocks(pair):
        step, rest = 1 + pair // EACH, pair % EACH
        way, col = rest % WAYS, 2 * (rest // 2)
        block = step * PER_STEP + 2 * col + way
        slot = (PER_STEP + 2 * pair) % SLOTS
        return step, way, col, ((block, slot), (block + 2, slot + 1))

    def body(pair, carry):
        @pl.when(pair < N_PAIRS)
        def _():
            step, way, col, blocks = pair_blocks(pair)
            load(PER_STEP + pair)
            for block, slot in blocks:
                to_partner(block, slot).wait_send()
            product(dest(step, way), way * EACH + col, 2, tmp.at[pl.ds(blocks[0][1], 2)])
            for block, slot in blocks:
                to_partner(block, slot).start()
            beside(pair)

        @pl.when(pair == 0)
        def _():
            serve_first(PER_STEP - 1)

        @pl.when(pair >= 1)
        def _():
            step, way, col, blocks = pair_blocks(pair - 1)
            for block, slot in blocks:
                to_partner(block, slot).wait_recv()
                to_next(block - PER_STEP).wait_recv()
                acc[block] = (acc[block] + tmp[slot, core]) + ring[block - PER_STEP]

                @pl.when(step < N_CHIPS - 1)
                def _():
                    to_next(block).start()

        return carry

    loop(N_PAIRS + 1, body)
    for slot in range(SLOTS):
        to_partner(0, slot).wait_send()
    for block in range(N_BLOCKS - PER_STEP):
        to_next(block).wait_send()
    return lambda cols: acc.at[N_BLOCKS - PER_STEP + 2 * (cols % EACH) + cols // EACH]


def scatter_scratch(rows, width):
    cols = width // PER_STEP
    return [
        pltpu.VMEM((SLOTS, 2, rows, cols), F32),
        pltpu.VMEM((N_BLOCKS, rows, cols), F32),
        pltpu.VMEM((N_BLOCKS - PER_STEP, rows, cols), F32),
        dma_sems(SLOTS),
        dma_sems(N_BLOCKS),
        dma_sems(N_BLOCKS - PER_STEP),
        dma_sems(N_BLOCKS - PER_STEP),
    ]


def start_loads(w_load, row_loads_of, later):
    order = [(block % WAYS) * EACH + block // WAYS for block in range(PER_STEP)]
    needed = [w_load(cols) + (row_loads_of[idx] if idx < WAYS else []) for idx, cols in enumerate(order)]
    for item in needed[0] + needed[1]:
        item.start()

    def load(product):
        for idx in range(PER_STEP):
            @pl.when(product == idx)
            def _():
                for item in needed[idx]:
                    item.wait()
                for item in (needed[idx + WAYS] if idx + WAYS < PER_STEP else []) + later.get(idx, []):
                    item.start()

    return load


def row_loads(pairs, sems, rows, chip):
    def load(order, hop):
        span = pl.ds(pl.multiple_of(((chip + hop) % N_CHIPS) * rows, rows), rows)
        return [pltpu.make_async_copy(src.at[span], dst.at[span], sems.at[idx, order]) for idx, (src, dst) in enumerate(pairs)]

    return [load(order, hop) for order, hop in enumerate((3, 1, 2, 0))]


def block_kernel(layer, qkv_hbm, m_hbm, w_out_hbm, w_down_hbm, x_ref, gain_ref, w_qkv_hbm, w_gate_hbm, w_up_hbm, cos_hbm, sin_hbm, *rest):
    y_ref, u_ref, o_hbm, lse_hbm, *rest = rest
    outs, rest = rest[:3], rest[3:]
    stages, rest = rest[:3], rest[3:]
    qkv, o_all, lse, m_all, w_out, w_down, weights, cos_ref, sin_ref, row_sems, w_sems, load_sems, out_sems = rest[:13]
    (full, send_sems, recv_sems), scatter = rest[13:16], rest[16:]
    me, chip, core = ring_place()
    rows, width = x_ref.shape
    block_cols = width // PER_STEP
    loads = row_loads(((m_hbm, m_all),), row_sems, CORES * rows, chip)
    gather = Gather(full, send_sems, recv_sems)
    qkv_load = pltpu.make_async_copy(qkv_hbm, qkv, load_sems.at[3])
    keeps = [pltpu.make_async_copy(o_all, o_hbm, load_sems.at[4]), pltpu.make_async_copy(lse, lse_hbm, load_sems.at[5])]
    next_loads, spans = project_loads(layer + 1, (w_qkv_hbm, w_gate_hbm, w_up_hbm), weights, load_sems)
    next_loads += [pltpu.make_async_copy(src, dst, load_sems.at[6 + idx]) for idx, (src, dst) in enumerate(((cos_hbm, cos_ref), (sin_hbm, sin_ref)))]

    def w_load(cols):
        span = pl.ds(cols * block_cols, block_cols)
        return [
            pltpu.make_async_copy(src.at[layer, :, span], dst.at[:, span], w_sems.at[idx, cols])
            for idx, (src, dst) in enumerate(((w_out_hbm, w_out), (w_down_hbm, w_down)))
        ]

    qkv_load.start()
    qkv_load.wait()
    load_first = start_loads(w_load, loads, {4: loads[2], 6: loads[3]})

    def load(product):
        load_first(product)
        for items, at in ((loads[2], PER_STEP), (loads[3], PER_STEP + WAYS * EACH)):
            @pl.when(product == at)
            def _():
                for item in items:
                    item.wait()

        @pl.when(product == PER_STEP)
        def _():
            for item in keeps + next_loads:
                item.start()

    def attend(index):
        def head_rows(q_start):
            def body(head, carry):
                attend_rows(q_start, head, qkv, o_all, lse)
                return carry

            loop(width_of(o_all) // HEAD_DIM, body)

        run_at(index, [functools.partial(head_rows, q_start) for q_start in range(0, height(qkv), Q_ROWS)])

    def early(block):
        turn = block - block // 4 * 2 - block // 6
        dest = (chip + 3 + 2 * turn + turn // 2 * 3) % N_CHIPS
        per_chip = CORES * rows // Q_ROWS

        @pl.when((block == 0) | (block == 1) | (block == 4) | (block == 6))
        def _():
            lax.fori_loop(0, per_chip, lambda idx, carry: (attend(dest * per_chip + idx), carry)[1], 0)

    def product(dest, cols, n_cols, out):
        span = piece_at(dest, CORES * rows)
        w_span = pl.ds(pl.multiple_of(cols * block_cols, block_cols), n_cols * block_cols)
        total = dot(o_all[span], w_out[:, w_span]) + dot(m_all[span], w_down[:, w_span])
        for idx in range(n_cols):
            for kind in range(CORES):
                out[idx, kind] = total[kind * rows:(kind + 1) * rows, idx * block_cols:(idx + 1) * block_cols]

    result = scatter_blocks(gather.peers(), load, early, product, lambda pair: None, *scatter)
    norm_rows = min(ROWS_AT_ONCE, rows // SUBS)

    def finish(idx, carry):
        span = piece_at(idx, norm_rows)
        summed = jnp.concatenate([result(cols)[span] for cols in range(PER_STEP)], axis=1)
        y = (x_ref[span].astype(F32) + summed).astype(BF16)
        normed = rms_scale(y.astype(F32), gain_ref[layer + 1:layer + 2]).astype(BF16)
        y_ref[span] = y
        u_ref[span] = normed
        full[me, span] = normed
        return carry

    per_piece = rows // SUBS // norm_rows
    for sub in range(SUBS):
        lax.fori_loop(sub * per_piece, (sub + 1) * per_piece, finish, 0)
        gather.launch((sub,))
    for item in next_loads:
        item.wait()
    project_steps(gather, weights, spans, stages, RowWriter(stages, outs, out_sems, rows), cos_ref, sin_ref, False)
    for item in keeps:
        item.wait()


def block_rest(qkv, hidden, w_out, w_down, x_loc, norm_gain, w_qkv, w_gate, w_up, tables, layer, tp_size):
    rows, width = x_loc.shape
    seq_len = height(qkv)
    o_cols, ff_cols = width_of(w_out), width_of(w_down)
    out_cols = [item.shape[-1] for item in (w_qkv, w_gate, w_up)]
    outs = [((rows, width), BF16), ((rows, width), BF16), ((seq_len, o_cols), BF16), ((seq_len, o_cols), F32)]
    outs += [((seq_len, cols), BF16) for cols in out_cols]
    scratch = [pltpu.VMEM((BUFFERS, rows, cols), BF16) for cols in out_cols]
    scratch += [
        pltpu.VMEM(qkv.shape, BF16),
        pltpu.VMEM((seq_len, o_cols), BF16),
        pltpu.VMEM((seq_len, o_cols), F32),
        pltpu.VMEM((seq_len, ff_cols), BF16),
        pltpu.VMEM((o_cols, width), BF16),
        pltpu.VMEM((ff_cols, width), BF16),
        pltpu.VMEM((width, sum(out_cols)), BF16),
    ]
    scratch += [pltpu.VMEM(table.shape, F32) for table in tables]
    scratch += [dma_sems(1, N_CHIPS), dma_sems(CORES, PER_STEP), dma_sems(8), dma_sems(len(out_cols), BUFFERS, CORES)]
    return pl.pallas_call(
        functools.partial(block_kernel, layer),
        out_shape=[jax.ShapeDtypeStruct(*item) for item in outs],
        in_specs=[ANY] * 4 + [VMEM] * 2 + [ANY] * 5,
        out_specs=[VMEM] * 2 + [ANY] * 5,
        scratch_shapes=scratch + gather_scratch(tp_size, rows, width) + scatter_scratch(rows, width),
        compiler_params=params(collective_id=5 + layer),
        name=f'block_rest_{layer}',
    )(qkv, hidden, w_out, w_down, x_loc, norm_gain, w_qkv, w_gate, w_up, *tables)


GRAD_ROWS = N_PAIRS // 3


def backward_kernel(layer, dqkv_hbm, dgate_hbm, dup_hbm, w_qkv_hbm, w_gate_hbm, w_up_hbm, u_hbm, x_ref, dy_ref, gain_ref, *rest):
    first_layer = layer == 0
    if first_layer:
        later_gains_ref, *rest = rest
    dx_ref, dgain_ref, *rest = rest
    grads, rest = rest[:3], rest[3:]
    acts, rest = rest[:3], rest[3:]
    weights, rest = rest[:3], rest[3:]
    u_all, stage, row_sems, w_sems, u_sem, stage_sems, *rest = rest
    if first_layer:
        gain_parts, gain_send, gain_recv, *rest = rest
    scatter = rest
    me, chip, core = ring_place()
    rows, width = x_ref.shape
    block_cols = width // PER_STEP
    loads = row_loads(list(zip((dqkv_hbm, dgate_hbm, dup_hbm), acts)), row_sems, CORES * rows, chip)
    u_load = pltpu.make_async_copy(u_hbm, u_all, u_sem)

    def w_load(cols):
        span = pl.ds(cols * block_cols, block_cols)
        return [
            pltpu.make_async_copy(src.at[layer, span], dst.at[span], w_sems.at[idx, cols])
            for idx, (src, dst) in enumerate(zip((w_qkv_hbm, w_gate_hbm, w_up_hbm), weights))
        ]

    load_first = start_loads(w_load, loads, {2: loads[2], 3: loads[3], 4: [u_load]})

    def load(product):
        load_first(product)

        @pl.when(product == PER_STEP)
        def _():
            for item in loads[2] + loads[3] + [u_load]:
                item.wait()

    def product(dest, cols, n_cols, out):
        span = piece_at(dest, CORES * rows)
        w_span = pl.ds(pl.multiple_of(cols * block_cols, block_cols), n_cols * block_cols)
        total = dot_nt(acts[0][span], weights[0][w_span]) + dot_nt(acts[1][span], weights[1][w_span]) + dot_nt(acts[2][span], weights[2][w_span])
        for idx in range(n_cols):
            for kind in range(CORES):
                out[idx, kind] = total[kind * rows:(kind + 1) * rows, idx * block_cols:(idx + 1) * block_cols]

    grad_rows = width // GRAD_ROWS

    def grad_out(which, part):
        slot = which % BUFFERS
        src = stage.at[slot, :, :width_of(grads[which])]
        return pltpu.make_async_copy(src, grads[which].at[piece_at(part, grad_rows)], stage_sems.at[slot])

    def beside(task):
        part = task // 3
        cols = piece_at(part, grad_rows)
        for turn, which in enumerate((2, 1, 0)):
            @pl.when(task % 3 == turn)
            def _():
                if which == 2:
                    @pl.when(part > 0)
                    def _():
                        grad_out(0, part - 1).wait()
                elif which == 0:
                    grad_out(2, part).wait()
                else:
                    @pl.when(part > 0)
                    def _():
                        grad_out(1, part - 1).wait()
                stage[which % BUFFERS, :, :width_of(grads[which])] = dot_tn(u_all[:, cols], acts[which][...]).astype(BF16)
                grad_out(which, part).start()

    peers = [(me + 1 + idx) % (N_DEVICES) for idx in range(N_DEVICES - 1)] if first_layer else None
    result = scatter_blocks(peers, load, lambda block: None, product, beside, *scatter)
    gain_row = gain_ref[layer:layer + 1]
    dgain = gain_parts.at[me, layer:layer + 1] if first_layer else dgain_ref
    dgain[...] = jnp.zeros_like(dgain)

    def row_values(idx):
        span = piece_at(idx, ROWS_AT_ONCE)
        summed = jnp.concatenate([result(cols)[span] for cols in range(PER_STEP)], axis=1)
        x_f32 = x_ref[span].astype(F32)
        inv_rms = lax.rsqrt(row_mean(x_f32 * x_f32) + NORM_EPS)
        return span, summed.astype(BF16).astype(F32), x_f32, inv_rms

    def gain_rows(idx, carry):
        _, d_normed, x_f32, inv_rms = row_values(idx)
        dgain[...] += jnp.sum(d_normed * (x_f32 * inv_rms), axis=0, keepdims=True)
        return carry

    def input_rows(idx, carry):
        span, d_normed, x_f32, inv_rms = row_values(idx)
        scaled = d_normed * gain_row
        mix = row_mean(scaled * x_f32) * (inv_rms * inv_rms * inv_rms)
        dx_ref[span] = (dy_ref[span].astype(F32) + (scaled * inv_rms - x_f32 * mix)).astype(BF16)
        return carry

    def both_rows(idx, carry):
        gain_rows(idx, carry)
        return input_rows(idx, carry)

    if first_layer:
        loop(rows // ROWS_AT_ONCE, gain_rows)
        gain_parts[me, 1:] = later_gains_ref[...]
        copies = [remote_copy(gain_parts.at[me], gain_parts.at[me], gain_send.at[idx], gain_recv.at[me], peer) for idx, peer in enumerate(peers)]
        for item in copies:
            item.start()
    loop(rows // ROWS_AT_ONCE, input_rows if first_layer else both_rows)
    if first_layer:
        for idx, peer in enumerate(peers):
            remote_copy(gain_parts.at[peer], gain_parts.at[peer], gain_send.at[idx], gain_recv.at[peer], peer).wait_recv()
        total = gain_parts[0]
        for idx in range(1, N_DEVICES):
            total = total + gain_parts[idx]
        dgain_ref[...] = total
        for item in copies:
            item.wait_send()
    grad_out(0, GRAD_ROWS - 1).wait()
    grad_out(1, GRAD_ROWS - 1).wait()


def block_input_backward(d_qkv, d_gate, d_up, w_qkv, w_gate, w_up, u_full, x_loc, dy_loc, norm_gain, later_gains, layer):
    rows, width = x_loc.shape
    seq_len = height(d_qkv)
    n_layers = height(norm_gain)
    all_cols = (w_qkv.shape[2], w_gate.shape[2], w_up.shape[2])
    first_layer = layer == 0
    out_shape = [jax.ShapeDtypeStruct((rows, width), BF16), jax.ShapeDtypeStruct((n_layers if first_layer else 1, width), F32)]
    out_shape += [jax.ShapeDtypeStruct((width, cols), BF16) for cols in all_cols]
    scratch = [pltpu.VMEM((seq_len, cols), BF16) for cols in all_cols]
    scratch += [pltpu.VMEM((width, cols), BF16) for cols in all_cols]
    scratch += [pltpu.VMEM((seq_len, width), BF16), pltpu.VMEM((2, width // GRAD_ROWS, max(all_cols)), BF16)]
    scratch += [dma_sems(3, N_CHIPS), dma_sems(3, PER_STEP), pltpu.SemaphoreType.DMA, dma_sems(2)]
    if first_layer:
        scratch += [pltpu.VMEM((N_DEVICES, n_layers, width), F32), dma_sems(N_DEVICES - 1), dma_sems(N_DEVICES)]
    return pl.pallas_call(
        functools.partial(backward_kernel, layer),
        out_shape=out_shape,
        in_specs=[ANY] * 7 + [VMEM] * (4 if first_layer else 3),
        out_specs=[VMEM] * 2 + [ANY] * 3,
        scratch_shapes=scratch + scatter_scratch(rows, width),
        compiler_params=params(collective_id=7 + layer),
        name=f'block_input_backward_{layer}',
    )(d_qkv, d_gate, d_up, w_qkv, w_gate, w_up, u_full, x_loc, dy_loc, norm_gain, *((later_gains,) if first_layer else ()))


COLLECT_SLOTS = 3


def collect_kernel(moves, steps, dy_hbm, attn_hbm, hidden_hbm, *refs):
    ins, refs = refs[:len(moves)], refs[len(moves):]
    n_outs = 1 + max(out for out, _ in moves)
    outs, refs = refs[:n_outs], refs[n_outs:]
    buffers, refs = refs[:len(moves)], refs[len(moves):]
    dy_full, attn_out, hidden, stage, in_sems, out_sems, whole_sems, dy_sems, grad_sems = refs
    o_cols, cols = width_of(attn_out), width_of(dy_full) // steps

    def move(idx, step, back):
        rows = width_of(buffers[idx])
        span = piece_at(step, rows)
        slot = step % COLLECT_SLOTS
        out, layer = moves[idx]
        dst = outs[out].at[span] if layer is None else outs[out].at[layer, span]
        if back:
            return pltpu.make_async_copy(buffers[idx].at[slot], dst, out_sems.at[idx, slot])
        return pltpu.make_async_copy(ins[idx].at[span], buffers[idx].at[slot], in_sems.at[idx, slot])

    def moves_of(step, back):
        return [move(idx, step, back) for idx in range(len(moves))]

    def dy_load(step):
        span = piece_at(step, cols)
        return pltpu.make_async_copy(dy_hbm.at[:, span], dy_full.at[:, span], dy_sems.at[step])

    def grads(step):
        span = piece_at(step, cols)
        slot = step % BUFFERS
        return (
            pltpu.make_async_copy(stage.at[slot, :o_cols], outs[1].at[1, :, span], grad_sems.at[slot, 0]),
            pltpu.make_async_copy(stage.at[slot, o_cols:], outs[2].at[1, :, span], grad_sems.at[slot, 1]),
        )

    whole = [pltpu.make_async_copy(attn_hbm, attn_out, whole_sems.at[0]), pltpu.make_async_copy(hidden_hbm, hidden, whole_sems.at[1])]
    for item in moves_of(0, False) + whole + [dy_load(0)] + moves_of(1, False):
        item.start()
    for step in range(1, steps):
        dy_load(step).start()
    for item in whole:
        item.wait()

    def body(step, carry):
        @pl.when((step >= 1) & (step + 2 <= steps))
        def _():
            @pl.when(step >= COLLECT_SLOTS - 1)
            def _():
                for item in moves_of(step + 1 - COLLECT_SLOTS, True):
                    item.wait()

            for item in moves_of(step + 1, False):
                item.start()

        for item in moves_of(step, False):
            item.wait()
        for item in moves_of(step, True):
            item.start()

        @pl.when(step >= 2)
        def _():
            for item in grads(step - 2):
                item.wait()

        dy_load(step).wait()
        dy_cols = dy_full[:, piece_at(step, cols)]
        slot = step % BUFFERS
        stage[slot, :o_cols] = dot_tn(attn_out[...], dy_cols).astype(BF16)
        stage[slot, o_cols:] = dot_tn(hidden[...], dy_cols).astype(BF16)
        for item in grads(step):
            item.start()
        return carry

    loop(steps, body)
    for step in range(steps - COLLECT_SLOTS, steps):
        for item in moves_of(step, True):
            item.wait()
    for item in grads(steps - 2) + grads(steps - 1):
        item.wait()


def collect(grad_x, dy_full, attn_out, hidden, g_out_first, g_down_first, made, steps):
    n_layers = len(made[0])
    assert n_layers == 2
    seq_len, width, o_cols, ff_cols = height(dy_full), width_of(dy_full), width_of(attn_out), width_of(hidden)
    sources = [(grad_x, 0, None), (g_out_first, 1, 0), (g_down_first, 2, 0)]
    sources += [(item, 3 + idx, layer) for idx, layers in enumerate(made) for layer, item in enumerate(layers)]
    moves = [(out, layer) for _, out, layer in sources]
    out_shape = [jax.ShapeDtypeStruct(grad_x.shape, BF16), jax.ShapeDtypeStruct((n_layers, o_cols, width), BF16), jax.ShapeDtypeStruct((n_layers, ff_cols, width), BF16)]
    out_shape += [jax.ShapeDtypeStruct((n_layers,) + layers[0].shape, BF16) for layers in made]
    scratch = [pltpu.VMEM((COLLECT_SLOTS, height(item) // steps, width_of(item)), BF16) for item, _, _ in sources]
    scratch += [pltpu.VMEM(item.shape, BF16) for item in (dy_full, attn_out, hidden)]
    scratch += [
        pltpu.VMEM((2, o_cols + ff_cols, width // steps), BF16),
        pltpu.SemaphoreType.DMA((len(moves), COLLECT_SLOTS)),
        pltpu.SemaphoreType.DMA((len(moves), COLLECT_SLOTS)),
        dma_sems(2),
        dma_sems(steps),
        dma_sems(2, 2),
    ]
    return pl.pallas_call(
        functools.partial(collect_kernel, moves, steps),
        out_shape=out_shape,
        in_specs=[ANY] * (3 + len(moves)),
        out_specs=[ANY] * len(out_shape),
        scratch_shapes=scratch,
        compiler_params=params(),
        name='collect',
    )(dy_full, attn_out, hidden, *[item for item, _, _ in sources])


def causal_tile(size):
    return lax.broadcasted_iota(jnp.int32, (size, size), 0) >= lax.broadcasted_iota(jnp.int32, (size, size), 1)


def masked_scores(query, keys):
    size = height(query)
    q_start = height(keys) - size
    scores = dot_nt(query, keys)
    diagonal = jnp.where(causal_tile(size), scores[:, q_start:], -1e30)
    scores = diagonal if q_start == 0 else jnp.concatenate([scores[:, :q_start], diagonal], axis=1)
    return scores * (SCALE * LOG2E)


def head_cols(head, part, parts):
    return pl.ds(pl.multiple_of((head * parts + part) * HEAD_DIM, HEAD_DIM), HEAD_DIM)


def attend_rows(q_start, head, qkv_ref, o_ref, lse_ref):
    span, seen = slice(q_start, q_start + Q_ROWS), slice(0, q_start + Q_ROWS)
    scores = masked_scores(qkv_ref[span, head_cols(head, 0, 3)], qkv_ref[seen, head_cols(head, 1, 3)])
    row_max = jnp.max(scores, axis=-1, keepdims=True)
    prob = jnp.exp2(scores - row_max)
    norm = row_sum(prob)
    prob = (prob * (1.0 / norm)).astype(BF16)
    o_ref[span, head_cols(head, 0, 1)] = dot(prob, qkv_ref[seen, head_cols(head, 2, 3)]).astype(BF16)
    lse_ref[span, head_cols(head, 0, 1)] = jnp.broadcast_to(row_max + jnp.log2(norm), (Q_ROWS, HEAD_DIM))


def attend_rows_backward(q_start, head, qkv_ref, lse_ref, do_ref, o_ref, cos_ref, sin_ref, dq_ref, dkt_acc, dvt_acc, prob_tmp, ds_tmp):
    span, seen = slice(q_start, q_start + Q_ROWS), slice(0, q_start + Q_ROWS)
    query = qkv_ref[span, head_cols(head, 0, 3)]
    d_out = do_ref[span, head_cols(head, 0, 1)]
    inner = row_sum(d_out.astype(F32) * o_ref[span, head_cols(head, 0, 1)].astype(F32))
    lse = lse_ref[span, head_cols(head, 0, 1)][:, :1]
    for k_start in range(0, q_start + Q_ROWS, Q_ROWS):
        keys = slice(k_start, k_start + Q_ROWS)
        scores = dot_nt(query, qkv_ref[keys, head_cols(head, 1, 3)]) * (SCALE * LOG2E)
        if k_start == q_start:
            scores = jnp.where(causal_tile(Q_ROWS), scores, -1e30)
        prob = jnp.exp2(scores - lse)
        d_prob = dot_nt(d_out, qkv_ref[keys, head_cols(head, 2, 3)]).astype(BF16).astype(F32)
        ds_tmp[:, keys] = (prob * (d_prob - inner) * SCALE).astype(BF16)
        prob_tmp[:, keys] = prob.astype(BF16)
    dvt_acc[head, :, seen] += dot_tn(d_out, prob_tmp[:, seen])
    dkt_acc[head, :, seen] += dot_tn(query, ds_tmp[:, seen])
    d_query = dot(ds_tmp[:, seen], qkv_ref[seen, head_cols(head, 1, 3)]).astype(BF16)
    dq_ref[span, head_cols(head, 0, 3)] = rotate(d_query.astype(F32), cos_ref[span], -sin_ref[span]).astype(BF16)


def middle_kernel(layer, with_forward, dy_hbm, u_hbm, w_out_hbm, w_down_hbm, gate_hbm, up_hbm, cos_hbm, sin_hbm, qkv_hbm, *rest):
    if not with_forward:
        (o_hbm, lse_hbm), rest = rest[:2], rest[2:]
    (dgate_hbm, dup_hbm, dqkv_hbm, u_full_hbm), rest = rest[:4], rest[4:]
    if with_forward:
        (dy_full_hbm, o_hbm, hidden_hbm), rest = rest[:3], rest[3:]
    else:
        (g_out_hbm, g_down_hbm), rest = rest[:2], rest[2:]
    (dgate_stage, dup_stage, gate_in, up_in, weights, qkv, o_all, lse, hidden, d_attn, dqkv, dk_acc, dv_acc, prob_tmp, ds_tmp, grad_stage, cos_ref, sin_ref), rest = rest[:18], rest[18:]
    dy_full, dy_send, dy_recv, u_full, u_send, u_recv, load_sems, out_sems, in_sems, u_sems, dqkv_sem, grad_sems = rest
    rows = width_of(dy_full)
    half = rows // 2
    seq_len = height(qkv)
    n_heads = width_of(o_all) // HEAD_DIM
    o_cols = width_of(o_all)
    gather = Gather(dy_full, dy_send, dy_recv)
    u_gather = Gather(u_full, u_send, u_recv)
    me = gather.me
    own_dy = pltpu.make_async_copy(dy_hbm, dy_full.at[me], load_sems.at[0])
    own_u = pltpu.make_async_copy(u_hbm, u_full.at[me], load_sems.at[1])
    w_loads = [
        pltpu.make_async_copy(w_out_hbm.at[layer], weights.at[:o_cols], load_sems.at[2]),
        pltpu.make_async_copy(w_down_hbm.at[layer], weights.at[o_cols:], load_sems.at[3]),
    ]
    loads = [
        pltpu.make_async_copy(src, dst, load_sems.at[4 + idx])
        for idx, (src, dst) in enumerate([(qkv_hbm, qkv), (cos_hbm, cos_ref), (sin_hbm, sin_ref)] + ([] if with_forward else [(o_hbm, o_all), (lse_hbm, lse)]))
    ]
    writer = RowWriter((dgate_stage, dup_stage), (dgate_hbm, dup_hbm), out_sems, rows)
    own_dy.start()
    meet(gather.peers())
    own_dy.wait()
    gather.launch()
    for item in w_loads + loads + [own_u]:
        item.start()
    dk_acc[...] = jnp.zeros_like(dk_acc)
    dv_acc[...] = jnp.zeros_like(dv_acc)
    for item in w_loads:
        item.wait()

    def both_heads(function, q_start, *args):
        def body(head, carry):
            function(q_start, head, *args)
            return carry

        loop(n_heads, body)

    def attend(index):
        run_at(index, [functools.partial(both_heads, attend_rows, q_start, qkv, o_all, lse) for q_start in range(0, seq_len, Q_ROWS)])

    def attend_backward(index):
        refs = (qkv, lse, d_attn, o_all, cos_ref, sin_ref, dqkv, dk_acc, dv_acc, prob_tmp, ds_tmp)
        run_at(index, [functools.partial(both_heads, attend_rows_backward, q_start, *refs) for q_start in range(0, seq_len, Q_ROWS)])

    def finish_keys_values():
        def body(idx, carry):
            span = piece_at(idx, Q_ROWS)
            for head in range(n_heads):
                d_keys = dk_acc[head, :, span].T.astype(BF16).astype(F32)
                dqkv[span, head_cols(head, 1, 3)] = rotate(d_keys, cos_ref[span], -sin_ref[span]).astype(BF16)
                dqkv[span, head_cols(head, 2, 3)] = dv_acc[head, :, span].T.astype(BF16)
            return carry

        loop(seq_len // Q_ROWS, body)
        keep_dqkv.start()

    keep_dqkv = pltpu.make_async_copy(dqkv, dqkv_hbm, dqkv_sem)

    def dy_rows(step):
        run_at(step, gather.events(early=True))

        @pl.when(step == N_DEVICES - 2)
        def _():
            own_u.wait()
            u_gather.launch_both()
            keep_u(me)

        places = gather.places(step)
        slot = step % BUFFERS
        fetch = []
        for idx, (src, dst) in enumerate(((gate_hbm, gate_in), (up_hbm, up_in))):
            for part, (shard, row) in enumerate(places):
                here = pl.ds(pl.multiple_of(shard * rows + row, half), half)
                fetch.append(pltpu.make_async_copy(src.at[here], dst.at[pl.ds(part * half, half)], in_sems.at[idx, part]))
        for item in fetch:
            item.start()
        writer.reuse(step)
        product = dot_nt(both_halves(dy_full, places, half), weights[...]).astype(BF16)
        d_hidden = product[:, o_cols:].astype(F32)
        for item in fetch:
            item.wait()
        gate, up = gate_in[...].astype(F32), up_in[...].astype(F32)
        sig = jax.nn.sigmoid(gate)
        act = gate * sig
        hidden_rows = (act * up).astype(BF16)
        for part, (shard, row) in enumerate(places):
            here = pl.ds(pl.multiple_of(shard * rows + row, half), half)
            d_attn[here] = product[part * half:(part + 1) * half, :o_cols]
            hidden[here] = hidden_rows[part * half:(part + 1) * half]
        dgate_stage[slot] = (d_hidden * up * (sig + act * (1.0 - sig))).astype(BF16)
        dup_stage[slot] = (d_hidden * act).astype(BF16)
        writer.start(step, places)

    def wait_loads(step):
        @pl.when(step == 0)
        def _():
            for item in loads:
                item.wait()

    def dy_step_forward(step, carry):
        dy_rows(step)
        wait_loads(step)
        attend(seq_len // Q_ROWS - 1 - step)
        return carry

    def dy_step_backward(step, carry):
        @pl.when(step < N_DEVICES)
        def _():
            dy_rows(step)

        wait_loads(step)
        after = step // (N_DEVICES)
        turn = (1 - after) * (step // 2) + after * (step - 5)
        upper, lower = gather.places(turn)
        shard = upper[0] + (turn // 7) * (lower[0] - upper[0])

        @pl.when(step == 10)
        def _():
            u_gather.pass_piece(0)

        @pl.when(step == 12)
        def _():
            u_gather.pass_piece(1)

        @pl.when((step == 0) | (step == 3) | (step == 5) | (step >= N_DEVICES))
        def _():
            attend_backward(shard * rows // Q_ROWS)

        return carry

    def keep_u(shard):
        pltpu.make_async_copy(u_full.at[shard], u_full_hbm.at[shard], u_sems.at[shard]).start()

    if with_forward:
        loop(N_DEVICES, dy_step_forward)
    else:
        loop(N_DEVICES + 5, dy_step_backward)

    def grad_copies(step):
        slot = step % BUFFERS
        cols = piece_at(step, grad_cols)
        return (
            pltpu.make_async_copy(grad_stage.at[slot, :o_cols], g_out_hbm.at[:, cols], grad_sems.at[slot, 0]),
            pltpu.make_async_copy(grad_stage.at[slot, o_cols:], g_down_hbm.at[:, cols], grad_sems.at[slot, 1]),
        )

    grad_cols = dy_full.shape[2] // (N_DEVICES)
    first_parts, last_parts = u_gather.pass_piece, u_gather.end_piece
    if with_forward:
        u_at = {1: [0], 2: [1], 4: [2], 7: [3]}
    else:
        u_at = {1: [2], 4: [3], 6: [4], 7: [5]}

    def u_event(at):
        for part in u_at.get(at, ()):
            first_parts(part) if part < SUBS else last_parts(part - SUBS)
        if at == 2 and not with_forward:
            finish_keys_values()

    u_events = [functools.partial(u_event, at) for at in range(N_DEVICES)]
    last_part = max(part for parts in u_at.values() for part in parts) + 1

    def u_step(step, carry):
        run_at(step, u_events)
        if with_forward:
            attend_backward(seq_len // Q_ROWS - 1 - step)
            return carry

        @pl.when(step >= 2)
        def _():
            for item in grad_copies(step - 2):
                item.wait()

        cols = piece_at(step, grad_cols)
        dy_cols = dy_full[:, :, cols].reshape(seq_len, grad_cols)
        slot = step % BUFFERS
        grad_stage[slot, :o_cols] = dot_tn(o_all[...], dy_cols).astype(BF16)
        grad_stage[slot, o_cols:] = dot_tn(hidden[...], dy_cols).astype(BF16)
        for item in grad_copies(step):
            item.start()
        return carry

    if with_forward:
        keeps = [pltpu.make_async_copy(src, dst, grad_sems.at[0, idx]) for idx, (src, dst) in enumerate(((o_all, o_hbm), (hidden, hidden_hbm)))]
        keeps += [pltpu.make_async_copy(dy_full, dy_full_hbm, grad_sems.at[1, 0])]
        for item in keeps:
            item.start()
    loop(N_DEVICES, u_step)
    if with_forward:
        finish_keys_values()
    for shard in (u_gather.partner, u_gather.first_other, u_gather.second_other):
        u_gather.arrived(shard)
        keep_u(shard)
    for shard in (u_gather.first, u_gather.second):
        keep_u(shard)
    for part in range(last_part, 2 * SUBS):
        last_parts(part - SUBS)
    keep_u(u_gather.third)
    u_gather.arrived(u_gather.third_other)
    keep_u(u_gather.third_other)
    for item in keeps if with_forward else grad_copies(N_DEVICES - 2) + grad_copies(N_DEVICES - 1):
        item.wait()
    gather.finish()
    u_gather.finish(0)
    writer.finish()
    keep_dqkv.wait()
    for shard in range(N_DEVICES):
        pltpu.make_async_copy(u_full.at[shard], u_full_hbm.at[shard], u_sems.at[shard]).wait()


def middle(dy_loc, u_loc, w_out, w_down, gate_act, up_act, tables, qkv, attended, layer, tp_size):
    rows, width = dy_loc.shape
    seq_len = rows * tp_size
    o_cols, ff_cols, qkv_cols = width_of(w_out), width_of(w_down), width_of(qkv)
    n_heads = o_cols // HEAD_DIM
    total = o_cols + ff_cols
    outs = [(seq_len, ff_cols), (seq_len, ff_cols), (seq_len, qkv_cols), (tp_size, rows, width)]
    outs += [(o_cols, width), (ff_cols, width)] if attended else [(tp_size, rows, width), (seq_len, o_cols), (seq_len, ff_cols)]
    scratch = [pltpu.VMEM((2, rows, ff_cols), BF16)] * 2
    scratch += [pltpu.VMEM((rows, ff_cols), BF16)] * 2
    scratch += [
        pltpu.VMEM((total, width), BF16),
        pltpu.VMEM((seq_len, qkv_cols), BF16),
        pltpu.VMEM((seq_len, o_cols), BF16),
        pltpu.VMEM((seq_len, o_cols), F32),
        pltpu.VMEM((seq_len, ff_cols), BF16),
        pltpu.VMEM((seq_len, o_cols), BF16),
        pltpu.VMEM((seq_len, qkv_cols), BF16),
        pltpu.VMEM((n_heads, HEAD_DIM, seq_len), F32),
        pltpu.VMEM((n_heads, HEAD_DIM, seq_len), F32),
        pltpu.VMEM((Q_ROWS, seq_len), BF16),
        pltpu.VMEM((Q_ROWS, seq_len), BF16),
        pltpu.VMEM((2, total, width // (N_DEVICES)), BF16),
    ]
    scratch += [pltpu.VMEM(table.shape, F32) for table in tables]
    scratch += gather_scratch(tp_size, rows, width) + gather_scratch(tp_size, rows, width)
    scratch += [
        dma_sems(9),
        dma_sems(2, 2, 2),
        dma_sems(2, 2),
        dma_sems(tp_size),
        pltpu.SemaphoreType.DMA,
        dma_sems(2, 2),
    ]
    return pl.pallas_call(
        functools.partial(middle_kernel, layer, not attended),
        out_shape=[jax.ShapeDtypeStruct(shape, BF16) for shape in outs],
        in_specs=[ANY] * (9 + len(attended)),
        out_specs=[ANY] * len(outs),
        scratch_shapes=scratch,
        compiler_params=params(collective_id=3 + layer),
        name=f'middle_{layer}',
    )(dy_loc, u_loc, w_out, w_down, gate_act, up_act, *tables, qkv, *attended)


def solution(mesh):
    tp_size = mesh.shape['tp']
    assert tp_size == N_DEVICES
    row_spec = P(('dp', 'tp'), None)
    col_spec = P(None, None, 'tp')
    inner_spec = P(None, 'tp', None)

    def device_program(x_loc, dy_loc, norm_gain, w_qkv, w_out, w_gate, w_up, w_down):
        n_layers = height(w_qkv)
        seq_len = height(x_loc) * tp_size
        tables = tuple(jnp.asarray(table) for table in rope_tables(seq_len, FINE))
        assert n_layers == 2
        qkv, gate_act, up_act, hidden, u_loc, *tables = project(x_loc, norm_gain, w_qkv, w_gate, w_up, tables, 0, tp_size)
        y_loc, u_next, attn_out, lse, *projected = block_rest(qkv, hidden, w_out, w_down, x_loc, norm_gain, w_qkv, w_gate, w_up, tables, 0, tp_size)
        saved = ((x_loc, u_loc, qkv, gate_act, up_act, (attn_out, lse)), (y_loc, u_next, *projected, ()))
        grad_cur = dy_loc
        grads, gains = [None] * n_layers, ()
        for layer in reversed(range(n_layers)):
            x_cur, u_loc, qkv, gate_act, up_act, attended = saved[layer]
            d_gate, d_up, d_qkv, u_full, *more = middle(grad_cur, u_loc, w_out, w_down, gate_act, up_act, tables, qkv, attended, layer, tp_size)
            u_full = u_full.reshape(seq_len, u_full.shape[2])
            later_gains = jnp.concatenate(gains, axis=0) if gains else None
            grad_cur, gain_grad, g_qkv, g_gate, g_up = block_input_backward(
                d_qkv, d_gate, d_up, w_qkv, w_gate, w_up, u_full, x_cur, grad_cur, norm_gain, later_gains, layer
            )
            grads[layer] = (g_qkv, g_gate, g_up)
            if layer == n_layers - 1:
                dy_full, attn_out, hidden = more
            gains = (gain_grad,) + gains
        grad_x, g_out, g_down, g_qkv, g_gate, g_up = collect(grad_cur, dy_full.reshape(seq_len, -1), attn_out, hidden, *more, list(zip(*grads)), 8)
        return (grad_x, gains[0], g_qkv, g_out, g_gate, g_up, g_down)

    return jax.shard_map(
        device_program,
        mesh=mesh,
        in_specs=(row_spec, row_spec, P(None, None), col_spec, inner_spec, col_spec, col_spec, inner_spec),
        out_specs=(row_spec, P('dp', None), P('dp', None, 'tp'), P('dp', 'tp', None), P('dp', None, 'tp'), P('dp', None, 'tp'), P('dp', 'tp', None)),
        check_vma=False,
    )
```

```python
import functools

import jax
import jax.numpy as jnp
import numpy as np
from jax import lax
from jax.experimental import pallas as pl
from jax.experimental.pallas import tpu as pltpu
from jax.sharding import PartitionSpec as P

HEAD_DIM = 128
NORM_EPS = 1e-5
ROPE_BASE = 10000.0
SCALE = HEAD_DIM ** -0.5
LOG2E = 1.4426950408889634
VMEM_LIMIT = 64000 * 1024
CORES = 2
N_CHIPS = 4
N_DEVICES = CORES * N_CHIPS
WAYS = 2
BUFFERS = 2
SUBS = 4
Q_ROWS = 256
ROWS_AT_ONCE = 32
FINE = 128
BF16 = jnp.bfloat16
F32 = jnp.float32
ANY = pl.BlockSpec(memory_space=pl.ANY)
VMEM = pl.BlockSpec(memory_space=pltpu.VMEM)
NT = (((1,), (1,)), ((), ()))
TN = (((0,), (0,)), ((), ()))


def height(array):
    return array.shape[0]


def width_of(array):
    return array.shape[1]


def piece_at(idx, size):
    return pl.ds(pl.multiple_of(idx * size, size), size)


def loop(count, body):
    lax.fori_loop(0, count, body, 0)


def dma_sems(*shape):
    return pltpu.SemaphoreType.DMA(shape)


def dot(lhs, rhs):
    return jnp.dot(lhs, rhs, preferred_element_type=F32)


def dot_nt(lhs, rhs):
    return lax.dot_general(lhs, rhs, NT, preferred_element_type=F32)


def dot_tn(lhs, rhs):
    return lax.dot_general(lhs, rhs, TN, preferred_element_type=F32)


def params(collective_id=None, semantics=None):
    if collective_id is None:
        return pltpu.CompilerParams(vmem_limit_bytes=VMEM_LIMIT, dimension_semantics=semantics)
    return pltpu.CompilerParams(vmem_limit_bytes=VMEM_LIMIT, collective_id=collective_id, has_side_effects=True)


def row_mean(values):
    return jnp.mean(values, axis=-1, keepdims=True)


def row_sum(values):
    return jnp.sum(values, axis=-1, keepdims=True)


def rope_tables(seq_len, fine):
    half_dim = HEAD_DIM // 2
    freqs = np.float32(ROPE_BASE) ** (np.float32(-2.0) * np.arange(half_dim, dtype=np.float32) / np.float32(HEAD_DIM))
    tables = []
    for positions in (np.arange(fine), np.arange(0, seq_len, fine)):
        angles = positions.astype(np.float32)[:, None] * freqs[None, :]
        tables += [np.tile(np.cos(angles), 2).astype(np.float32), np.tile(np.sin(angles), 2).astype(np.float32)]
    return tables


def fill_rope(fine_cos, fine_sin, coarse_cos, coarse_sin, cos_ref, sin_ref):
    fine = height(fine_cos)
    sign = jnp.where(lax.broadcasted_iota(jnp.int32, (1, HEAD_DIM), 1) < HEAD_DIM // 2, -1.0, 1.0)

    def body(idx, carry):
        span = piece_at(idx, fine)
        big_cos, big_sin = coarse_cos[pl.ds(idx, 1)], coarse_sin[pl.ds(idx, 1)]
        cos_ref[span] = big_cos * fine_cos[...] - big_sin * fine_sin[...]
        sin_ref[span] = (big_sin * fine_cos[...] + big_cos * fine_sin[...]) * sign
        return carry

    loop(height(cos_ref) // fine, body)


def rotate(values, cos_tab, sin_tab):
    return values * cos_tab + pltpu.roll(values, HEAD_DIM // 2, 1) * sin_tab


def rms_scale(x_f32, gain_row):
    inv_rms = lax.rsqrt(row_mean(x_f32 * x_f32) + NORM_EPS)
    return x_f32 * inv_rms * gain_row


def ring_place():
    me = lax.axis_index('tp')
    chip = me // 2
    core = me % 2
    return me, chip, core


def device_at(chip, core):
    return ((chip + N_CHIPS) % N_CHIPS) * 2 + core


def remote_copy(src, dst, send_sem, recv_sem, peer):
    return pltpu.make_async_remote_copy(
        src_ref=src, dst_ref=dst, send_sem=send_sem, recv_sem=recv_sem, device_id={'tp': peer}, device_id_type=pl.DeviceIdType.MESH
    )


def meet(peers):
    barrier = pltpu.get_barrier_semaphore()
    for peer in peers:
        pl.semaphore_signal(barrier, inc=1, device_id={'tp': peer}, device_id_type=pl.DeviceIdType.MESH)
    pl.semaphore_wait(barrier, len(peers))


OWN_PARTNER, OWN_AHEAD, OWN_BEHIND, FIRST_PARTNER, FIRST_AHEAD, SECOND_PARTNER, THIRD_PARTNER = KINDS = range(7)


class Gather:
    EVERY, EARLY, LATE = range(SUBS), range(SUBS // 2), range(SUBS // 2, SUBS)

    def __init__(self, full, send_sems, recv_sems):
        self.full, self.send_sems, self.recv_sems = full, send_sems, recv_sems
        self.me, chip, core = ring_place()
        turn = 1 - 2 * core
        self.chip, self.core, self.turn = chip, core, turn
        self.partner = device_at(chip, 1 - core)
        self.ahead = device_at(chip + turn, core)
        self.behind = device_at(chip - turn, core)
        self.first = device_at(chip - turn, core)
        self.first_other = device_at(chip + turn, 1 - core)
        self.second = device_at(chip + turn, core)
        self.second_other = device_at(chip - turn, 1 - core)
        self.third = device_at(chip + 2, core)
        self.third_other = device_at(chip + 2, 1 - core)

    def peers(self):
        return self.partner, self.ahead, self.behind

    def piece(self, kind, shard, sub, peer):
        rows = width_of(self.full) // SUBS
        part = self.full.at[shard, pl.ds(sub * rows, rows)]
        return remote_copy(part, part, self.send_sems.at[kind, sub], self.recv_sems.at[shard, sub], peer)

    def send(self, kind, shard, peer, subs=EVERY):
        for sub in subs:
            self.piece(kind, shard, sub, peer).start()

    def sent(self, kind, shard, peer, subs=EVERY):
        for sub in subs:
            self.piece(kind, shard, sub, peer).wait_send()

    def arrived(self, shard, subs=EVERY, pass_on=None):
        for sub in subs:
            self.piece(OWN_PARTNER, shard, sub, self.partner).wait_recv()
            if pass_on is not None:
                self.piece(pass_on, shard, sub, self.partner).start()

    def launch(self, subs=EVERY):
        self.send(OWN_AHEAD, self.me, self.ahead, subs)
        self.send(OWN_PARTNER, self.me, self.partner, subs)

    def turn_back(self):
        self.sent(OWN_AHEAD, self.me, self.ahead, range(SUBS - 1))
        self.send(OWN_BEHIND, self.me, self.behind)

    def pass_ahead(self):
        self.sent(OWN_BEHIND, self.me, self.behind, range(SUBS - 1))
        self.send(FIRST_AHEAD, self.first, self.ahead)

    def launch_both(self):
        self.launch()
        self.send(OWN_BEHIND, self.me, self.behind)

    def pass_piece(self, sub):
        self.piece(OWN_PARTNER, self.first, sub, self.partner).wait_recv()
        self.piece(FIRST_AHEAD, self.first, sub, self.ahead).start()
        self.piece(FIRST_PARTNER, self.first, sub, self.partner).start()
        self.arrived(self.second, (sub,), SECOND_PARTNER)

    def end_piece(self, sub):
        self.arrived(self.third, (sub,), THIRD_PARTNER)

    def events(self, early=False):
        return (
            lambda: None,
            lambda: (self.turn_back(), self.arrived(self.partner)),
            lambda: self.arrived(self.first, pass_on=FIRST_PARTNER),
            lambda: (self.pass_ahead() if early else None, self.arrived(self.first_other)),
            lambda: (None if early else self.pass_ahead(), self.arrived(self.second, pass_on=SECOND_PARTNER)),
            lambda: self.arrived(self.second_other),
            lambda: (self.arrived(self.third, self.EARLY, THIRD_PARTNER), self.arrived(self.third_other, self.EARLY)),
            lambda: (self.arrived(self.third, self.LATE, THIRD_PARTNER), self.arrived(self.third_other, self.LATE)),
        )

    def places(self, step):
        half = width_of(self.full) // 2
        pair = step // 2
        odd = step % BUFFERS
        side = self.turn * (1 - 2 * odd)
        hop = (3 * pair + (pair // 2) * (2 * pair - 5)) % N_CHIPS
        shard = device_at((self.chip + side * hop + N_DEVICES) % N_CHIPS, (self.core + odd) % 2)
        last = step // (N_DEVICES - 2)
        upper = (1 - last) * shard + last * self.third
        lower = (1 - last) * shard + last * self.third_other
        return (upper, last * odd * half), (lower, (1 - last) * half + last * odd * half)

    def finish(self, waited=SUBS - 1):
        self.sent(OWN_PARTNER, self.me, self.partner)
        self.sent(OWN_AHEAD, self.me, self.ahead, range(waited, SUBS))
        self.sent(OWN_BEHIND, self.me, self.behind, range(waited, SUBS))
        self.sent(FIRST_PARTNER, self.first, self.partner)
        self.sent(FIRST_AHEAD, self.first, self.ahead)
        self.sent(SECOND_PARTNER, self.second, self.partner)
        self.sent(THIRD_PARTNER, self.third, self.partner)


def run_at(step, actions):
    for idx, action in enumerate(actions):
        @pl.when(step == idx)
        def _():
            action()


def gather_scratch(tp_size, rows, width):
    return [
        pltpu.VMEM((tp_size, rows, width), BF16),
        dma_sems(len(KINDS), SUBS),
        dma_sems(tp_size, SUBS),
    ]


def half_rows(ref, place, half):
    return ref[place[0], pl.ds(pl.multiple_of(place[1], half), half)]


def both_halves(ref, places, half):
    return jnp.concatenate([half_rows(ref, place, half) for place in places], axis=0)


def table_rows(ref, places, half, rows):
    parts = [ref[pl.ds(pl.multiple_of(shard * rows + row, half), half)] for shard, row in places]
    return jnp.concatenate(parts, axis=0)


class RowWriter:
    def __init__(self, stages, outs, sems, rows):
        self.stages, self.outs, self.sems, self.rows = stages, outs, sems, rows

    def copies(self, slot, places):
        half = self.rows // 2
        items = []
        for idx in range(len(self.outs)):
            for part, (shard, row) in enumerate(places):
                start = pl.multiple_of(shard * self.rows + row, half)
                src = self.stages[idx].at[slot, pl.ds(part * half, half)]
                items.append(pltpu.make_async_copy(src, self.outs[idx].at[pl.ds(start, half)], self.sems.at[idx, slot, part]))
        return items

    def reuse(self, step):
        @pl.when(step >= 2)
        def _():
            for item in self.copies(step % BUFFERS, ((0, 0), (0, 0))):
                item.wait()

    def start(self, step, places):
        for item in self.copies(step % BUFFERS, places):
            item.start()

    def finish(self):
        for slot in range(BUFFERS):
            for item in self.copies(slot, ((0, 0), (0, 0))):
                item.wait()


def project_loads(layer, sources, weights, sems):
    loads, spans, start = [], [], 0
    for idx, src in enumerate(sources):
        spans.append(slice(start, start + src.shape[-1]))
        start += src.shape[-1]
        loads.append(pltpu.make_async_copy(src.at[layer], weights.at[:, spans[-1]], sems.at[idx]))
    return loads, spans


def project_steps(gather, weights, spans, stages, writer, cos_ref, sin_ref, with_hidden):
    rows = width_of(gather.full)
    half = rows // CORES

    def step_body(step, carry):
        run_at(step, gather.events())
        places = gather.places(step)
        slot = step % BUFFERS
        writer.reuse(step)
        cos_tab, sin_tab = table_rows(cos_ref, places, half, rows), table_rows(sin_ref, places, half, rows)
        product = dot(both_halves(gather.full, places, half), weights[...]).astype(BF16)
        qkv, gate, up = (product[:, span] for span in spans)
        for head in range(width_of(qkv) // HEAD_DIM):
            cols = slice(head * HEAD_DIM, (head + 1) * HEAD_DIM)
            part = qkv[:, cols]
            if head % 3 != 2:
                part = rotate(part.astype(F32), cos_tab, sin_tab).astype(BF16)
            stages[0][slot, :, cols] = part
        stages[1][slot] = gate
        stages[2][slot] = up
        if with_hidden:
            stages[3][slot] = (jax.nn.silu(gate.astype(F32)) * up.astype(F32)).astype(BF16)
        writer.start(step, places)
        return carry

    loop(N_DEVICES, step_body)
    gather.finish()
    writer.finish()


def project_kernel(layer, x_ref, gain_ref, w_qkv_hbm, w_gate_hbm, w_up_hbm, *rest):
    tables, rest = rest[:4], rest[4:]
    outs, rest = rest[:4], rest[4:]
    u_hbm, cos_out, sin_out, *rest = rest
    stages, rest = rest[:4], rest[4:]
    cos_ref, sin_ref, weights, full, send_sems, recv_sems, w_sems, keep_sems, out_sems = rest
    rows = width_of(full)
    gather = Gather(full, send_sems, recv_sems)
    loads, spans = project_loads(layer, (w_qkv_hbm, w_gate_hbm, w_up_hbm), weights, w_sems)
    keeps = [
        pltpu.make_async_copy(src, dst, keep_sems.at[idx])
        for idx, (src, dst) in enumerate(((cos_ref, cos_out), (sin_ref, sin_out), (full.at[gather.me], u_hbm)))
    ]
    norm_rows = min(ROWS_AT_ONCE, rows // SUBS)

    def norm(idx, carry):
        span = piece_at(idx, norm_rows)
        normed = rms_scale(x_ref[span].astype(F32), gain_ref[layer:layer + 1]).astype(BF16)
        full[gather.me, span] = normed
        return carry

    for load in loads:
        load.start()
    meet(gather.peers())
    per_piece = rows // SUBS // norm_rows
    for sub in range(SUBS):
        lax.fori_loop(sub * per_piece, (sub + 1) * per_piece, norm, 0)
        gather.launch((sub,))
    fill_rope(*tables, cos_ref, sin_ref)
    for item in keeps:
        item.start()
    for load in loads:
        load.wait()
    project_steps(gather, weights, spans, stages, RowWriter(stages, outs, out_sems, rows), cos_ref, sin_ref, True)
    for item in keeps:
        item.wait()


def project(x_loc, norm_gain, w_qkv, w_gate, w_up, tables, layer, tp_size):
    rows, width = x_loc.shape
    seq_len = rows * tp_size
    out_cols = [item.shape[-1] for item in (w_qkv, w_gate, w_up, w_up)]
    table = (seq_len, HEAD_DIM)
    outs = [jax.ShapeDtypeStruct((seq_len, cols), BF16) for cols in out_cols]
    outs += [jax.ShapeDtypeStruct((rows, width), BF16)] + [jax.ShapeDtypeStruct(table, F32)] * 2
    scratch = [pltpu.VMEM((BUFFERS, rows, cols), BF16) for cols in out_cols]
    scratch += [pltpu.VMEM(table, F32)] * 2
    scratch += [pltpu.VMEM((width, sum(out_cols[:3])), BF16)]
    scratch += gather_scratch(tp_size, rows, width)
    scratch += [dma_sems(3), dma_sems(3), dma_sems(len(out_cols), BUFFERS, CORES)]
    return pl.pallas_call(
        functools.partial(project_kernel, layer),
        out_shape=outs,
        in_specs=[VMEM] * 2 + [ANY] * 3 + [VMEM] * len(tables),
        out_specs=[ANY] * len(outs),
        scratch_shapes=scratch,
        compiler_params=params(collective_id=1 + layer),
        name=f'project_{layer}',
    )(x_loc, norm_gain, w_qkv, w_gate, w_up, *tables)


EACH = 4
PER_STEP = WAYS * EACH
N_BLOCKS = N_CHIPS * PER_STEP
N_PAIRS = (N_BLOCKS - PER_STEP) // 2
SLOTS = 6


def scatter_blocks(peers, load, early, product, beside, tmp, acc, ring, pair_send, pair_recv, ring_send, ring_recv):
    me, chip, core = ring_place()
    partner = device_at(chip, 1 - core)
    meet(peers or (partner, device_at(chip + 1, core), device_at(chip - 1, core)))

    def dest(step, way):
        return (chip + (step + 1) * (WAYS * way - 1) + N_DEVICES) % N_CHIPS

    def to_partner(block, slot):
        return remote_copy(tmp.at[slot, 1 - core], acc.at[block], pair_send.at[slot], pair_recv.at[block], partner)

    def to_next(block):
        peer = device_at(chip + 1 - 2 * (block % WAYS), core)
        return remote_copy(acc.at[block], ring.at[block], ring_send.at[block], ring_recv.at[block], peer)

    def serve_first(block):
        to_partner(block, block % SLOTS).wait_recv()
        acc[block] = acc[block] + tmp[block % SLOTS, core]
        to_next(block).start()

    def first_body(block, carry):
        load(block)
        early(block)

        @pl.when(block >= SLOTS)
        def _():
            to_partner(block - SLOTS, block % SLOTS).wait_send()

        way = block % WAYS
        product(dest(0, way), way * EACH + block // WAYS, 1, tmp.at[pl.ds(block % SLOTS, 1)])
        to_partner(block, block % SLOTS).start()

        @pl.when(block >= 1)
        def _():
            serve_first(block - 1)

        return carry

    loop(PER_STEP, first_body)

    def pair_blocks(pair):
        step, rest = 1 + pair // EACH, pair % EACH
        way, col = rest % WAYS, 2 * (rest // 2)
        block = step * PER_STEP + 2 * col + way
        slot = (PER_STEP + 2 * pair) % SLOTS
        return step, way, col, ((block, slot), (block + 2, slot + 1))

    def body(pair, carry):
        @pl.when(pair < N_PAIRS)
        def _():
            step, way, col, blocks = pair_blocks(pair)
            load(PER_STEP + pair)
            for block, slot in blocks:
                to_partner(block, slot).wait_send()
            product(dest(step, way), way * EACH + col, 2, tmp.at[pl.ds(blocks[0][1], 2)])
            for block, slot in blocks:
                to_partner(block, slot).start()
            beside(pair)

        @pl.when(pair == 0)
        def _():
            serve_first(PER_STEP - 1)

        @pl.when(pair >= 1)
        def _():
            step, way, col, blocks = pair_blocks(pair - 1)
            for block, slot in blocks:
                to_partner(block, slot).wait_recv()
                to_next(block - PER_STEP).wait_recv()
                acc[block] = (acc[block] + tmp[slot, core]) + ring[block - PER_STEP]

                @pl.when(step < N_CHIPS - 1)
                def _():
                    to_next(block).start()

        return carry

    loop(N_PAIRS + 1, body)
    for slot in range(SLOTS):
        to_partner(0, slot).wait_send()
    for block in range(N_BLOCKS - PER_STEP):
        to_next(block).wait_send()
    return lambda cols: acc.at[N_BLOCKS - PER_STEP + 2 * (cols % EACH) + cols // EACH]


def scatter_scratch(rows, width):
    cols = width // PER_STEP
    return [
        pltpu.VMEM((SLOTS, 2, rows, cols), F32),
        pltpu.VMEM((N_BLOCKS, rows, cols), F32),
        pltpu.VMEM((N_BLOCKS - PER_STEP, rows, cols), F32),
        dma_sems(SLOTS),
        dma_sems(N_BLOCKS),
        dma_sems(N_BLOCKS - PER_STEP),
        dma_sems(N_BLOCKS - PER_STEP),
    ]


def start_loads(w_load, row_loads_of, later):
    order = [(block % WAYS) * EACH + block // WAYS for block in range(PER_STEP)]
    needed = [w_load(cols) + (row_loads_of[idx] if idx < WAYS else []) for idx, cols in enumerate(order)]
    for item in needed[0] + needed[1]:
        item.start()

    def load(product):
        for idx in range(PER_STEP):
            @pl.when(product == idx)
            def _():
                for item in needed[idx]:
                    item.wait()
                for item in (needed[idx + WAYS] if idx + WAYS < PER_STEP else []) + later.get(idx, []):
                    item.start()

    return load


def row_loads(pairs, sems, rows, chip):
    def load(order, hop):
        span = pl.ds(pl.multiple_of(((chip + hop) % N_CHIPS) * rows, rows), rows)
        return [pltpu.make_async_copy(src.at[span], dst.at[span], sems.at[idx, order]) for idx, (src, dst) in enumerate(pairs)]

    return [load(order, hop) for order, hop in enumerate((3, 1, 2, 0))]


def block_kernel(layer, qkv_hbm, m_hbm, w_out_hbm, w_down_hbm, x_hbm, gain_ref, w_qkv_hbm, w_gate_hbm, w_up_hbm, cos_hbm, sin_hbm, *rest):
    y_hbm, u_hbm, o_hbm, lse_hbm, *rest = rest
    outs, rest = rest[:3], rest[3:]
    stages, (x_ref, y_ref, *rest) = rest[:3], rest[3:]
    qkv, o_all, lse, m_all, w_out, w_down, weights, cos_ref, sin_ref, row_sems, w_sems, load_sems, out_sems = rest[:13]
    (full, send_sems, recv_sems), scatter = rest[13:16], rest[16:]
    me, chip, core = ring_place()
    rows, width = x_hbm.shape
    block_cols = width // PER_STEP
    loads = row_loads(((m_hbm, m_all),), row_sems, CORES * rows, chip)
    gather = Gather(full, send_sems, recv_sems)
    qkv_load, x_load, *keeps = [
        pltpu.make_async_copy(src, dst, load_sems.at[3 + idx])
        for idx, (src, dst) in enumerate(((qkv_hbm, qkv), (x_hbm, x_ref), (o_all, o_hbm), (lse, lse_hbm), (y_ref, y_hbm), (full.at[me], u_hbm)))
    ]
    keeps, keeps_after = keeps[:2], keeps[2:]
    next_loads, spans = project_loads(layer + 1, (w_qkv_hbm, w_gate_hbm, w_up_hbm), weights, load_sems)
    next_loads += [pltpu.make_async_copy(src, dst, load_sems.at[9 + idx]) for idx, (src, dst) in enumerate(((cos_hbm, cos_ref), (sin_hbm, sin_ref)))]

    def w_load(cols):
        span = pl.ds(cols * block_cols, block_cols)
        return [
            pltpu.make_async_copy(src.at[layer, :, span], dst.at[:, span], w_sems.at[idx, cols])
            for idx, (src, dst) in enumerate(((w_out_hbm, w_out), (w_down_hbm, w_down)))
        ]

    qkv_load.start()
    qkv_load.wait()
    load_first = start_loads(w_load, loads, {4: loads[2], 6: loads[3]})

    def load(product):
        load_first(product)
        for items, at in ((loads[2], PER_STEP), (loads[3], PER_STEP + WAYS * EACH)):
            @pl.when(product == at)
            def _():
                for item in items:
                    item.wait()

        @pl.when(product == PER_STEP)
        def _():
            for item in [x_load] + keeps + next_loads:
                item.start()

    def attend(index):
        def head_rows(q_start):
            def body(head, carry):
                attend_rows(q_start, head, qkv, o_all, lse)
                return carry

            loop(width_of(o_all) // HEAD_DIM, body)

        run_at(index, [functools.partial(head_rows, q_start) for q_start in range(0, height(qkv), Q_ROWS)])

    def early(block):
        turn = block - block // 4 * 2 - block // 6
        dest = (chip + 3 + 2 * turn + turn // 2 * 3) % N_CHIPS
        per_chip = CORES * rows // Q_ROWS

        @pl.when((block == 0) | (block == 1) | (block == 4) | (block == 6))
        def _():
            def body(idx, carry):
                attend(dest * per_chip + idx)
                return carry

            loop(per_chip, body)

    def product(dest, cols, n_cols, out):
        span = piece_at(dest, CORES * rows)
        w_span = pl.ds(pl.multiple_of(cols * block_cols, block_cols), n_cols * block_cols)
        total = dot(o_all[span], w_out[:, w_span]) + dot(m_all[span], w_down[:, w_span])
        for idx in range(n_cols):
            for kind in range(CORES):
                out[idx, kind] = total[kind * rows:(kind + 1) * rows, idx * block_cols:(idx + 1) * block_cols]

    result = scatter_blocks(gather.peers(), load, early, product, lambda pair: None, *scatter)
    norm_rows = min(ROWS_AT_ONCE, rows // SUBS)
    x_load.wait()

    def finish(idx, carry):
        span = piece_at(idx, norm_rows)
        summed = jnp.concatenate([result(cols)[span] for cols in range(PER_STEP)], axis=1)
        y = (x_ref[span].astype(F32) + summed).astype(BF16)
        normed = rms_scale(y.astype(F32), gain_ref[layer + 1:layer + 2]).astype(BF16)
        y_ref[span] = y
        full[me, span] = normed
        return carry

    per_piece = rows // SUBS // norm_rows
    for sub in range(SUBS):
        lax.fori_loop(sub * per_piece, (sub + 1) * per_piece, finish, 0)
        gather.launch((sub,))
    for item in keeps_after:
        item.start()
    for item in next_loads:
        item.wait()
    project_steps(gather, weights, spans, stages, RowWriter(stages, outs, out_sems, rows), cos_ref, sin_ref, False)
    for item in keeps + keeps_after:
        item.wait()


def block_rest(qkv, hidden, w_out, w_down, x_loc, norm_gain, w_qkv, w_gate, w_up, tables, layer, tp_size):
    rows, width = x_loc.shape
    seq_len = height(qkv)
    o_cols, ff_cols = width_of(w_out), width_of(w_down)
    out_cols = [item.shape[-1] for item in (w_qkv, w_gate, w_up)]
    outs = [((rows, width), BF16), ((rows, width), BF16), ((seq_len, o_cols), BF16), ((seq_len, o_cols), F32)]
    outs += [((seq_len, cols), BF16) for cols in out_cols]
    scratch = [pltpu.VMEM((BUFFERS, rows, cols), BF16) for cols in out_cols]
    scratch += [pltpu.VMEM((rows, width), BF16)] * 2
    scratch += [
        pltpu.VMEM(qkv.shape, BF16),
        pltpu.VMEM((seq_len, o_cols), BF16),
        pltpu.VMEM((seq_len, o_cols), F32),
        pltpu.VMEM((seq_len, ff_cols), BF16),
        pltpu.VMEM((o_cols, width), BF16),
        pltpu.VMEM((ff_cols, width), BF16),
        pltpu.VMEM((width, sum(out_cols)), BF16),
    ]
    scratch += [pltpu.VMEM(table.shape, F32) for table in tables]
    scratch += [dma_sems(1, N_CHIPS), dma_sems(CORES, PER_STEP), dma_sems(11), dma_sems(len(out_cols), BUFFERS, CORES)]
    return pl.pallas_call(
        functools.partial(block_kernel, layer),
        out_shape=[jax.ShapeDtypeStruct(*item) for item in outs],
        in_specs=[ANY] * 5 + [VMEM] + [ANY] * 5,
        out_specs=[ANY] * len(outs),
        scratch_shapes=scratch + gather_scratch(tp_size, rows, width) + scatter_scratch(rows, width),
        compiler_params=params(collective_id=5 + layer),
        name=f'block_rest_{layer}',
    )(qkv, hidden, w_out, w_down, x_loc, norm_gain, w_qkv, w_gate, w_up, *tables)


GRAD_ROWS = N_PAIRS // 3


def backward_kernel(layer, dqkv_hbm, dgate_hbm, dup_hbm, w_qkv_hbm, w_gate_hbm, w_up_hbm, u_hbm, x_hbm, dy_hbm, gain_ref, *rest):
    first_layer = layer == 0
    if first_layer:
        later_gains_ref, *rest = rest
    dx_ref, dgain_ref, *rest = rest
    grads, rest = rest[:3], rest[3:]
    acts, rest = rest[:3], rest[3:]
    weights, rest = rest[:3], rest[3:]
    u_all, x_ref, dy_ref, stage, row_sems, w_sems, u_sem, x_sem, dy_sem, stage_sems, *rest = rest
    if first_layer:
        gain_parts, gain_send, gain_recv, *rest = rest
    scatter = rest
    me, chip, core = ring_place()
    rows, width = x_hbm.shape
    block_cols = width // PER_STEP
    loads = row_loads(list(zip((dqkv_hbm, dgate_hbm, dup_hbm), acts)), row_sems, CORES * rows, chip)
    u_load = pltpu.make_async_copy(u_hbm, u_all, u_sem)
    x_loads = [pltpu.make_async_copy(x_hbm, x_ref, x_sem), pltpu.make_async_copy(dy_hbm, dy_ref, dy_sem)]

    def w_load(cols):
        span = pl.ds(cols * block_cols, block_cols)
        return [
            pltpu.make_async_copy(src.at[layer, span], dst.at[span], w_sems.at[idx, cols])
            for idx, (src, dst) in enumerate(zip((w_qkv_hbm, w_gate_hbm, w_up_hbm), weights))
        ]

    load_first = start_loads(w_load, loads, {2: loads[2], 3: loads[3], 4: [u_load] + x_loads})

    def load(product):
        load_first(product)

        @pl.when(product == PER_STEP)
        def _():
            for item in loads[2] + loads[3] + [u_load] + x_loads:
                item.wait()

    def product(dest, cols, n_cols, out):
        span = piece_at(dest, CORES * rows)
        w_span = pl.ds(pl.multiple_of(cols * block_cols, block_cols), n_cols * block_cols)
        total = dot_nt(acts[0][span], weights[0][w_span]) + dot_nt(acts[1][span], weights[1][w_span]) + dot_nt(acts[2][span], weights[2][w_span])
        for idx in range(n_cols):
            for kind in range(CORES):
                out[idx, kind] = total[kind * rows:(kind + 1) * rows, idx * block_cols:(idx + 1) * block_cols]

    grad_rows = width // GRAD_ROWS

    def grad_out(which, part):
        slot = which % BUFFERS
        src = stage.at[slot, :, :width_of(grads[which])]
        return pltpu.make_async_copy(src, grads[which].at[piece_at(part, grad_rows)], stage_sems.at[slot])

    def beside(task):
        part = task // 3
        cols = piece_at(part, grad_rows)
        for turn, which in enumerate((2, 1, 0)):
            @pl.when(task % 3 == turn)
            def _():
                if which == 2:
                    @pl.when(part > 0)
                    def _():
                        grad_out(0, part - 1).wait()
                elif which == 0:
                    grad_out(2, part).wait()
                else:
                    @pl.when(part > 0)
                    def _():
                        grad_out(1, part - 1).wait()
                stage[which % BUFFERS, :, :width_of(grads[which])] = dot_tn(u_all[:, cols], acts[which][...]).astype(BF16)
                grad_out(which, part).start()

    peers = [(me + 1 + idx) % (N_DEVICES) for idx in range(N_DEVICES - 1)] if first_layer else None
    result = scatter_blocks(peers, load, lambda block: None, product, beside, *scatter)
    gain_row = gain_ref[layer:layer + 1]
    dgain = gain_parts.at[me, layer:layer + 1] if first_layer else dgain_ref
    dgain[...] = jnp.zeros_like(dgain)

    def row_values(idx):
        span = piece_at(idx, ROWS_AT_ONCE)
        summed = jnp.concatenate([result(cols)[span] for cols in range(PER_STEP)], axis=1)
        x_f32 = x_ref[span].astype(F32)
        inv_rms = lax.rsqrt(row_mean(x_f32 * x_f32) + NORM_EPS)
        return span, summed.astype(BF16).astype(F32), x_f32, inv_rms

    def gain_rows(idx, carry):
        _, d_normed, x_f32, inv_rms = row_values(idx)
        dgain[...] += jnp.sum(d_normed * (x_f32 * inv_rms), axis=0, keepdims=True)
        return carry

    def input_rows(idx, carry):
        span, d_normed, x_f32, inv_rms = row_values(idx)
        scaled = d_normed * gain_row
        mix = row_mean(scaled * x_f32) * (inv_rms * inv_rms * inv_rms)
        dx_ref[span] = (dy_ref[span].astype(F32) + (scaled * inv_rms - x_f32 * mix)).astype(BF16)
        return carry

    def both_rows(idx, carry):
        gain_rows(idx, carry)
        return input_rows(idx, carry)

    if first_layer:
        loop(rows // ROWS_AT_ONCE, gain_rows)
        gain_parts[me, 1:] = later_gains_ref[...]
        copies = [remote_copy(gain_parts.at[me], gain_parts.at[me], gain_send.at[idx], gain_recv.at[me], peer) for idx, peer in enumerate(peers)]
        for item in copies:
            item.start()
    loop(rows // ROWS_AT_ONCE, input_rows if first_layer else both_rows)
    if first_layer:
        for idx, peer in enumerate(peers):
            remote_copy(gain_parts.at[peer], gain_parts.at[peer], gain_send.at[idx], gain_recv.at[peer], peer).wait_recv()
        total = gain_parts[0]
        for idx in range(1, N_DEVICES):
            total = total + gain_parts[idx]
        dgain_ref[...] = total
        for item in copies:
            item.wait_send()
    grad_out(0, GRAD_ROWS - 1).wait()
    grad_out(1, GRAD_ROWS - 1).wait()


def block_input_backward(d_qkv, d_gate, d_up, w_qkv, w_gate, w_up, u_full, x_loc, dy_loc, norm_gain, later_gains, layer):
    rows, width = x_loc.shape
    seq_len = height(d_qkv)
    n_layers = height(norm_gain)
    all_cols = (w_qkv.shape[2], w_gate.shape[2], w_up.shape[2])
    first_layer = layer == 0
    out_shape = [jax.ShapeDtypeStruct((rows, width), BF16), jax.ShapeDtypeStruct((n_layers if first_layer else 1, width), F32)]
    out_shape += [jax.ShapeDtypeStruct((width, cols), BF16) for cols in all_cols]
    scratch = [pltpu.VMEM((seq_len, cols), BF16) for cols in all_cols]
    scratch += [pltpu.VMEM((width, cols), BF16) for cols in all_cols]
    scratch += [pltpu.VMEM((seq_len, width), BF16)] + [pltpu.VMEM((rows, width), BF16)] * 2 + [pltpu.VMEM((BUFFERS, width // GRAD_ROWS, max(all_cols)), BF16)]
    scratch += [dma_sems(3, N_CHIPS), dma_sems(3, PER_STEP)] + [pltpu.SemaphoreType.DMA] * 3 + [dma_sems(BUFFERS)]
    if first_layer:
        scratch += [pltpu.VMEM((N_DEVICES, n_layers, width), F32), dma_sems(N_DEVICES - 1), dma_sems(N_DEVICES)]
    return pl.pallas_call(
        functools.partial(backward_kernel, layer),
        out_shape=out_shape,
        in_specs=[ANY] * 9 + [VMEM] * (2 if first_layer else 1),
        out_specs=[VMEM] * 2 + [ANY] * 3,
        scratch_shapes=scratch + scatter_scratch(rows, width),
        compiler_params=params(collective_id=7 + layer),
        name=f'block_input_backward_{layer}',
    )(d_qkv, d_gate, d_up, w_qkv, w_gate, w_up, u_full, x_loc, dy_loc, norm_gain, *((later_gains,) if first_layer else ()))


COLLECT_SLOTS = 4


def collect_kernel(moves, steps, dy_hbm, attn_hbm, hidden_hbm, *refs):
    ins, refs = refs[:len(moves)], refs[len(moves):]
    n_outs = 1 + max(out for out, _ in moves)
    outs, refs = refs[:n_outs], refs[n_outs:]
    buffers, refs = refs[:len(moves)], refs[len(moves):]
    dy_full, attn_out, hidden, stage, in_sems, out_sems, whole_sems, dy_sems, grad_sems = refs
    o_cols, cols = width_of(attn_out), width_of(dy_full) // steps

    def move(idx, step, back):
        rows = width_of(buffers[idx])
        span = piece_at(step, rows)
        slot = step % COLLECT_SLOTS
        out, layer = moves[idx]
        dst = outs[out].at[span] if layer is None else outs[out].at[layer, span]
        if back:
            return pltpu.make_async_copy(buffers[idx].at[slot], dst, out_sems.at[idx, slot])
        return pltpu.make_async_copy(ins[idx].at[span], buffers[idx].at[slot], in_sems.at[idx, slot])

    def moves_of(step, back):
        return [move(idx, step, back) for idx in range(len(moves))]

    def dy_load(step):
        span = piece_at(step, cols)
        return pltpu.make_async_copy(dy_hbm.at[:, span], dy_full.at[:, span], dy_sems.at[step])

    def grads(step):
        span = piece_at(step, cols)
        slot = step % BUFFERS
        return (
            pltpu.make_async_copy(stage.at[slot, :o_cols], outs[1].at[1, :, span], grad_sems.at[slot, 0]),
            pltpu.make_async_copy(stage.at[slot, o_cols:], outs[2].at[1, :, span], grad_sems.at[slot, 1]),
        )

    whole = [pltpu.make_async_copy(attn_hbm, attn_out, whole_sems.at[0]), pltpu.make_async_copy(hidden_hbm, hidden, whole_sems.at[1])]
    for item in moves_of(0, False) + whole + [dy_load(0)] + moves_of(1, False) + moves_of(2, False):
        item.start()
    for step in range(1, steps):
        dy_load(step).start()
    for item in whole:
        item.wait()

    def body(step, carry):
        @pl.when((step >= 1) & (step + 2 < steps))
        def _():
            @pl.when(step >= BUFFERS)
            def _():
                for item in moves_of(step - BUFFERS, True):
                    item.wait()

            for item in moves_of(step + 2, False):
                item.start()

        for item in moves_of(step, False):
            item.wait()
        for item in moves_of(step, True):
            item.start()

        @pl.when(step >= 2)
        def _():
            for item in grads(step - 2):
                item.wait()

        dy_load(step).wait()
        dy_cols = dy_full[:, piece_at(step, cols)]
        slot = step % BUFFERS
        stage[slot, :o_cols] = dot_tn(attn_out[...], dy_cols).astype(BF16)
        stage[slot, o_cols:] = dot_tn(hidden[...], dy_cols).astype(BF16)
        for item in grads(step):
            item.start()
        return carry

    loop(steps, body)
    for step in range(steps - COLLECT_SLOTS, steps):
        for item in moves_of(step, True):
            item.wait()
    for item in grads(steps - 2) + grads(steps - 1):
        item.wait()


def collect(grad_x, dy_full, attn_out, hidden, g_out_first, g_down_first, made, steps):
    n_layers = len(made[0])
    assert n_layers == 2
    seq_len, width, o_cols, ff_cols = height(dy_full), width_of(dy_full), width_of(attn_out), width_of(hidden)
    sources = [(grad_x, 0, None), (g_out_first, 1, 0), (g_down_first, 2, 0)]
    sources += [(item, 3 + idx, layer) for idx, layers in enumerate(made) for layer, item in enumerate(layers)]
    moves = [(out, layer) for _, out, layer in sources]
    out_shape = [jax.ShapeDtypeStruct(grad_x.shape, BF16), jax.ShapeDtypeStruct((n_layers, o_cols, width), BF16), jax.ShapeDtypeStruct((n_layers, ff_cols, width), BF16)]
    out_shape += [jax.ShapeDtypeStruct((n_layers,) + layers[0].shape, BF16) for layers in made]
    scratch = [pltpu.VMEM((COLLECT_SLOTS, height(item) // steps, width_of(item)), BF16) for item, _, _ in sources]
    scratch += [pltpu.VMEM(item.shape, BF16) for item in (dy_full, attn_out, hidden)]
    scratch += [
        pltpu.VMEM((2, o_cols + ff_cols, width // steps), BF16),
        pltpu.SemaphoreType.DMA((len(moves), COLLECT_SLOTS)),
        pltpu.SemaphoreType.DMA((len(moves), COLLECT_SLOTS)),
        dma_sems(2),
        dma_sems(steps),
        dma_sems(2, 2),
    ]
    return pl.pallas_call(
        functools.partial(collect_kernel, moves, steps),
        out_shape=out_shape,
        in_specs=[ANY] * (3 + len(moves)),
        out_specs=[ANY] * len(out_shape),
        scratch_shapes=scratch,
        compiler_params=params(),
        name='collect',
    )(dy_full, attn_out, hidden, *[item for item, _, _ in sources])


def causal_tile(size):
    return lax.broadcasted_iota(jnp.int32, (size, size), 0) >= lax.broadcasted_iota(jnp.int32, (size, size), 1)


def masked_scores(query, keys):
    size = height(query)
    q_start = height(keys) - size
    scores = dot_nt(query, keys)
    diagonal = jnp.where(causal_tile(size), scores[:, q_start:], -1e30)
    scores = diagonal if q_start == 0 else jnp.concatenate([scores[:, :q_start], diagonal], axis=1)
    return scores * (SCALE * LOG2E)


def head_cols(head, part, parts):
    return pl.ds(pl.multiple_of((head * parts + part) * HEAD_DIM, HEAD_DIM), HEAD_DIM)


def attend_rows(q_start, head, qkv_ref, o_ref, lse_ref):
    span, seen = slice(q_start, q_start + Q_ROWS), slice(0, q_start + Q_ROWS)
    scores = masked_scores(qkv_ref[span, head_cols(head, 0, 3)], qkv_ref[seen, head_cols(head, 1, 3)])
    row_max = jnp.max(scores, axis=-1, keepdims=True)
    prob = jnp.exp2(scores - row_max)
    norm = row_sum(prob)
    prob = (prob * (1.0 / norm)).astype(BF16)
    o_ref[span, head_cols(head, 0, 1)] = dot(prob, qkv_ref[seen, head_cols(head, 2, 3)]).astype(BF16)
    lse_ref[span, head_cols(head, 0, 1)] = jnp.broadcast_to(row_max + jnp.log2(norm), (Q_ROWS, HEAD_DIM))


def attend_rows_backward(q_start, head, qkv_ref, lse_ref, do_ref, o_ref, cos_ref, sin_ref, dq_ref, dkt_acc, dvt_acc, prob_tmp, ds_tmp):
    span, seen = slice(q_start, q_start + Q_ROWS), slice(0, q_start + Q_ROWS)
    query = qkv_ref[span, head_cols(head, 0, 3)]
    d_out = do_ref[span, head_cols(head, 0, 1)]
    inner = row_sum(d_out.astype(F32) * o_ref[span, head_cols(head, 0, 1)].astype(F32))
    lse = lse_ref[span, head_cols(head, 0, 1)][:, :1]
    for k_start in range(0, q_start + Q_ROWS, Q_ROWS):
        keys = slice(k_start, k_start + Q_ROWS)
        scores = dot_nt(query, qkv_ref[keys, head_cols(head, 1, 3)]) * (SCALE * LOG2E)
        if k_start == q_start:
            scores = jnp.where(causal_tile(Q_ROWS), scores, -1e30)
        prob = jnp.exp2(scores - lse)
        d_prob = dot_nt(d_out, qkv_ref[keys, head_cols(head, 2, 3)]).astype(BF16).astype(F32)
        ds_tmp[:, keys] = (prob * (d_prob - inner) * SCALE).astype(BF16)
        prob_tmp[:, keys] = prob.astype(BF16)
    dvt_acc[head, :, seen] += dot_tn(d_out, prob_tmp[:, seen])
    dkt_acc[head, :, seen] += dot_tn(query, ds_tmp[:, seen])
    d_query = dot(ds_tmp[:, seen], qkv_ref[seen, head_cols(head, 1, 3)]).astype(BF16)
    dq_ref[span, head_cols(head, 0, 3)] = rotate(d_query.astype(F32), cos_ref[span], -sin_ref[span]).astype(BF16)


def middle_kernel(layer, with_forward, dy_hbm, u_hbm, w_out_hbm, w_down_hbm, gate_hbm, up_hbm, cos_hbm, sin_hbm, qkv_hbm, *rest):
    if not with_forward:
        (o_hbm, lse_hbm), rest = rest[:2], rest[2:]
    (dgate_hbm, dup_hbm, dqkv_hbm, u_full_hbm), rest = rest[:4], rest[4:]
    if with_forward:
        (dy_full_hbm, o_hbm, hidden_hbm), rest = rest[:3], rest[3:]
    else:
        (g_out_hbm, g_down_hbm), rest = rest[:2], rest[2:]
    (dgate_stage, dup_stage, gate_in, up_in, weights, qkv, o_all, lse, hidden, d_attn, dqkv, dk_acc, dv_acc, prob_tmp, ds_tmp, grad_stage, cos_ref, sin_ref), rest = rest[:18], rest[18:]
    dy_full, dy_send, dy_recv, u_full, u_send, u_recv, load_sems, out_sems, in_sems, u_sems, dqkv_sem, grad_sems = rest
    rows = width_of(dy_full)
    half = rows // 2
    seq_len = height(qkv)
    n_heads = width_of(o_all) // HEAD_DIM
    o_cols = width_of(o_all)
    gather = Gather(dy_full, dy_send, dy_recv)
    u_gather = Gather(u_full, u_send, u_recv)
    me = gather.me
    own_dy = pltpu.make_async_copy(dy_hbm, dy_full.at[me], load_sems.at[0])
    own_u = pltpu.make_async_copy(u_hbm, u_full.at[me], load_sems.at[1])
    w_loads = [
        pltpu.make_async_copy(w_out_hbm.at[layer], weights.at[:o_cols], load_sems.at[2]),
        pltpu.make_async_copy(w_down_hbm.at[layer], weights.at[o_cols:], load_sems.at[3]),
    ]
    loads = [
        pltpu.make_async_copy(src, dst, load_sems.at[4 + idx])
        for idx, (src, dst) in enumerate([(qkv_hbm, qkv), (cos_hbm, cos_ref), (sin_hbm, sin_ref)] + ([] if with_forward else [(o_hbm, o_all), (lse_hbm, lse)]))
    ]
    writer = RowWriter((dgate_stage, dup_stage), (dgate_hbm, dup_hbm), out_sems, rows)
    own_dy.start()
    meet(gather.peers())
    own_dy.wait()
    gather.launch()
    for item in w_loads + loads + [own_u]:
        item.start()
    dk_acc[...] = jnp.zeros_like(dk_acc)
    dv_acc[...] = jnp.zeros_like(dv_acc)
    for item in w_loads:
        item.wait()

    def both_heads(function, q_start, *args):
        def body(head, carry):
            function(q_start, head, *args)
            return carry

        loop(n_heads, body)

    def attend(index):
        run_at(index, [functools.partial(both_heads, attend_rows, q_start, qkv, o_all, lse) for q_start in range(0, seq_len, Q_ROWS)])

    def attend_backward(index):
        refs = (qkv, lse, d_attn, o_all, cos_ref, sin_ref, dqkv, dk_acc, dv_acc, prob_tmp, ds_tmp)
        run_at(index, [functools.partial(both_heads, attend_rows_backward, q_start, *refs) for q_start in range(0, seq_len, Q_ROWS)])

    def finish_keys_values():
        def body(idx, carry):
            span = piece_at(idx, Q_ROWS)
            for head in range(n_heads):
                d_keys = dk_acc[head, :, span].T.astype(BF16).astype(F32)
                dqkv[span, head_cols(head, 1, 3)] = rotate(d_keys, cos_ref[span], -sin_ref[span]).astype(BF16)
                dqkv[span, head_cols(head, 2, 3)] = dv_acc[head, :, span].T.astype(BF16)
            return carry

        loop(seq_len // Q_ROWS, body)
        keep_dqkv.start()

    keep_dqkv = pltpu.make_async_copy(dqkv, dqkv_hbm, dqkv_sem)

    def dy_rows(step):
        run_at(step, gather.events(early=True))

        @pl.when(step == N_DEVICES - 2)
        def _():
            own_u.wait()
            u_gather.launch_both()
            keep_u(me)

        places = gather.places(step)
        slot = step % BUFFERS
        fetch = []
        for idx, (src, dst) in enumerate(((gate_hbm, gate_in), (up_hbm, up_in))):
            for part, (shard, row) in enumerate(places):
                here = pl.ds(pl.multiple_of(shard * rows + row, half), half)
                fetch.append(pltpu.make_async_copy(src.at[here], dst.at[pl.ds(part * half, half)], in_sems.at[idx, part]))
        for item in fetch:
            item.start()
        writer.reuse(step)
        product = dot_nt(both_halves(dy_full, places, half), weights[...]).astype(BF16)
        d_hidden = product[:, o_cols:].astype(F32)
        for item in fetch:
            item.wait()
        gate, up = gate_in[...].astype(F32), up_in[...].astype(F32)
        sig = jax.nn.sigmoid(gate)
        act = gate * sig
        hidden_rows = (act * up).astype(BF16)
        for part, (shard, row) in enumerate(places):
            here = pl.ds(pl.multiple_of(shard * rows + row, half), half)
            d_attn[here] = product[part * half:(part + 1) * half, :o_cols]
            hidden[here] = hidden_rows[part * half:(part + 1) * half]
        dgate_stage[slot] = (d_hidden * up * (sig + act * (1.0 - sig))).astype(BF16)
        dup_stage[slot] = (d_hidden * act).astype(BF16)
        writer.start(step, places)

    def wait_loads(step):
        @pl.when(step == 0)
        def _():
            for item in loads:
                item.wait()

    def dy_step_forward(step, carry):
        dy_rows(step)
        wait_loads(step)
        attend(seq_len // Q_ROWS - 1 - step)
        return carry

    def dy_step_backward(step, carry):
        @pl.when(step < N_DEVICES)
        def _():
            dy_rows(step)

        wait_loads(step)
        after = step // (N_DEVICES)
        turn = (1 - after) * (step // 2) + after * (step - 5)
        upper, lower = gather.places(turn)
        shard = upper[0] + (turn // 7) * (lower[0] - upper[0])

        @pl.when(step == 10)
        def _():
            u_gather.pass_piece(0)

        @pl.when(step == 12)
        def _():
            u_gather.pass_piece(1)

        @pl.when((step == 0) | (step == 3) | (step == 5) | (step >= N_DEVICES))
        def _():
            attend_backward(shard * rows // Q_ROWS)

        return carry

    def keep_u(shard):
        pltpu.make_async_copy(u_full.at[shard], u_full_hbm.at[shard], u_sems.at[shard]).start()

    if with_forward:
        loop(N_DEVICES, dy_step_forward)
    else:
        loop(N_DEVICES + 5, dy_step_backward)

    def grad_copies(step):
        slot = step % BUFFERS
        cols = piece_at(step, grad_cols)
        return (
            pltpu.make_async_copy(grad_stage.at[slot, :o_cols], g_out_hbm.at[:, cols], grad_sems.at[slot, 0]),
            pltpu.make_async_copy(grad_stage.at[slot, o_cols:], g_down_hbm.at[:, cols], grad_sems.at[slot, 1]),
        )

    grad_cols = dy_full.shape[2] // (N_DEVICES)
    first_parts, last_parts = u_gather.pass_piece, u_gather.end_piece
    if with_forward:
        u_at = {1: [0], 2: [1], 4: [2], 7: [3]}
    else:
        u_at = {1: [2], 4: [3], 6: [4], 7: [5]}

    def u_event(at):
        for part in u_at.get(at, ()):
            first_parts(part) if part < SUBS else last_parts(part - SUBS)
        if at == 2 and not with_forward:
            finish_keys_values()

    u_events = [functools.partial(u_event, at) for at in range(N_DEVICES)]
    last_part = max(part for parts in u_at.values() for part in parts) + 1

    def u_step(step, carry):
        run_at(step, u_events)
        if with_forward:
            attend_backward(seq_len // Q_ROWS - 1 - step)
            return carry

        @pl.when(step >= 2)
        def _():
            for item in grad_copies(step - 2):
                item.wait()

        cols = piece_at(step, grad_cols)
        dy_cols = dy_full[:, :, cols].reshape(seq_len, grad_cols)
        slot = step % BUFFERS
        grad_stage[slot, :o_cols] = dot_tn(o_all[...], dy_cols).astype(BF16)
        grad_stage[slot, o_cols:] = dot_tn(hidden[...], dy_cols).astype(BF16)
        for item in grad_copies(step):
            item.start()
        return carry

    if with_forward:
        keeps = [pltpu.make_async_copy(src, dst, grad_sems.at[0, idx]) for idx, (src, dst) in enumerate(((o_all, o_hbm), (hidden, hidden_hbm)))]
        keeps += [pltpu.make_async_copy(dy_full, dy_full_hbm, grad_sems.at[1, 0])]
        for item in keeps:
            item.start()
    loop(N_DEVICES, u_step)
    if with_forward:
        finish_keys_values()
    for shard in (u_gather.partner, u_gather.first_other, u_gather.second_other):
        u_gather.arrived(shard)
        keep_u(shard)
    for shard in (u_gather.first, u_gather.second):
        keep_u(shard)
    for part in range(last_part, 2 * SUBS):
        last_parts(part - SUBS)
    keep_u(u_gather.third)
    u_gather.arrived(u_gather.third_other)
    keep_u(u_gather.third_other)
    for item in keeps if with_forward else grad_copies(N_DEVICES - 2) + grad_copies(N_DEVICES - 1):
        item.wait()
    gather.finish()
    u_gather.finish(0)
    writer.finish()
    keep_dqkv.wait()
    for shard in range(N_DEVICES):
        pltpu.make_async_copy(u_full.at[shard], u_full_hbm.at[shard], u_sems.at[shard]).wait()


def middle(dy_loc, u_loc, w_out, w_down, gate_act, up_act, tables, qkv, attended, layer, tp_size):
    rows, width = dy_loc.shape
    seq_len = rows * tp_size
    o_cols, ff_cols, qkv_cols = width_of(w_out), width_of(w_down), width_of(qkv)
    n_heads = o_cols // HEAD_DIM
    total = o_cols + ff_cols
    outs = [(seq_len, ff_cols), (seq_len, ff_cols), (seq_len, qkv_cols), (tp_size, rows, width)]
    outs += [(o_cols, width), (ff_cols, width)] if attended else [(tp_size, rows, width), (seq_len, o_cols), (seq_len, ff_cols)]
    scratch = [pltpu.VMEM((2, rows, ff_cols), BF16)] * 2
    scratch += [pltpu.VMEM((rows, ff_cols), BF16)] * 2
    scratch += [
        pltpu.VMEM((total, width), BF16),
        pltpu.VMEM((seq_len, qkv_cols), BF16),
        pltpu.VMEM((seq_len, o_cols), BF16),
        pltpu.VMEM((seq_len, o_cols), F32),
        pltpu.VMEM((seq_len, ff_cols), BF16),
        pltpu.VMEM((seq_len, o_cols), BF16),
        pltpu.VMEM((seq_len, qkv_cols), BF16),
        pltpu.VMEM((n_heads, HEAD_DIM, seq_len), F32),
        pltpu.VMEM((n_heads, HEAD_DIM, seq_len), F32),
        pltpu.VMEM((Q_ROWS, seq_len), BF16),
        pltpu.VMEM((Q_ROWS, seq_len), BF16),
        pltpu.VMEM((2, total, width // (N_DEVICES)), BF16),
    ]
    scratch += [pltpu.VMEM(table.shape, F32) for table in tables]
    scratch += gather_scratch(tp_size, rows, width) + gather_scratch(tp_size, rows, width)
    scratch += [
        dma_sems(9),
        dma_sems(2, 2, 2),
        dma_sems(2, 2),
        dma_sems(tp_size),
        pltpu.SemaphoreType.DMA,
        dma_sems(2, 2),
    ]
    return pl.pallas_call(
        functools.partial(middle_kernel, layer, not attended),
        out_shape=[jax.ShapeDtypeStruct(shape, BF16) for shape in outs],
        in_specs=[ANY] * (9 + len(attended)),
        out_specs=[ANY] * len(outs),
        scratch_shapes=scratch,
        compiler_params=params(collective_id=3 + layer),
        name=f'middle_{layer}',
    )(dy_loc, u_loc, w_out, w_down, gate_act, up_act, *tables, qkv, *attended)


def solution(mesh):
    tp_size = mesh.shape['tp']
    assert tp_size == N_DEVICES
    row_spec = P(('dp', 'tp'), None)
    col_spec = P(None, None, 'tp')
    inner_spec = P(None, 'tp', None)

    def device_program(x_loc, dy_loc, norm_gain, w_qkv, w_out, w_gate, w_up, w_down):
        n_layers = height(w_qkv)
        seq_len = height(x_loc) * tp_size
        tables = tuple(jnp.asarray(table) for table in rope_tables(seq_len, FINE))
        assert n_layers == 2
        qkv, gate_act, up_act, hidden, u_loc, *tables = project(x_loc, norm_gain, w_qkv, w_gate, w_up, tables, 0, tp_size)
        y_loc, u_next, attn_out, lse, *projected = block_rest(qkv, hidden, w_out, w_down, x_loc, norm_gain, w_qkv, w_gate, w_up, tables, 0, tp_size)
        saved = ((x_loc, u_loc, qkv, gate_act, up_act, (attn_out, lse)), (y_loc, u_next, *projected, ()))
        grad_cur = dy_loc
        grads, gains = [None] * n_layers, ()
        for layer in reversed(range(n_layers)):
            x_cur, u_loc, qkv, gate_act, up_act, attended = saved[layer]
            d_gate, d_up, d_qkv, u_full, *more = middle(grad_cur, u_loc, w_out, w_down, gate_act, up_act, tables, qkv, attended, layer, tp_size)
            u_full = u_full.reshape(seq_len, u_full.shape[2])
            later_gains = jnp.concatenate(gains, axis=0) if gains else None
            grad_cur, gain_grad, g_qkv, g_gate, g_up = block_input_backward(
                d_qkv, d_gate, d_up, w_qkv, w_gate, w_up, u_full, x_cur, grad_cur, norm_gain, later_gains, layer
            )
            grads[layer] = (g_qkv, g_gate, g_up)
            if layer == n_layers - 1:
                dy_full, attn_out, hidden = more
            gains = (gain_grad,) + gains
        grad_x, g_out, g_down, g_qkv, g_gate, g_up = collect(grad_cur, dy_full.reshape(seq_len, -1), attn_out, hidden, *more, list(zip(*grads)), 8)
        return (grad_x, gains[0], g_qkv, g_out, g_gate, g_up, g_down)

    return jax.shard_map(
        device_program,
        mesh=mesh,
        in_specs=(row_spec, row_spec, P(None, None), col_spec, inner_spec, col_spec, col_spec, inner_spec),
        out_specs=(row_spec, P('dp', None), P('dp', None, 'tp'), P('dp', 'tp', None), P('dp', None, 'tp'), P('dp', None, 'tp'), P('dp', 'tp', None)),
        check_vma=False,
    )
```

```python
import functools

import jax
import jax.numpy as jnp
import numpy as np
from jax import lax
from jax.experimental import pallas as pl
from jax.experimental.pallas import tpu as pltpu
from jax.sharding import PartitionSpec as P

HEAD_DIM = 128
NORM_EPS = 1e-5
ROPE_BASE = 10000.0
SCALE = HEAD_DIM ** -0.5
LOG2E = 1.4426950408889634
VMEM_LIMIT = 64000 * 1024
CORES = 2
N_CHIPS = 4
N_DEVICES = CORES * N_CHIPS
WAYS = 2
BUFFERS = 2
SUBS = 4
Q_ROWS = 256
ROWS_AT_ONCE = 64
FINE = 128
BF16 = jnp.bfloat16
F32 = jnp.float32
ANY = pl.BlockSpec(memory_space=pl.ANY)
VMEM = pl.BlockSpec(memory_space=pltpu.VMEM)
NT = (((1,), (1,)), ((), ()))
TN = (((0,), (0,)), ((), ()))


def height(array):
    return array.shape[0]


def width_of(array):
    return array.shape[1]


def piece_at(idx, size):
    return pl.ds(pl.multiple_of(idx * size, size), size)


def loop(count, body):
    lax.fori_loop(0, count, body, 0)


def dma_sems(*shape):
    return pltpu.SemaphoreType.DMA(shape)


def dot(lhs, rhs):
    return jnp.dot(lhs, rhs, preferred_element_type=F32)


def dot_nt(lhs, rhs):
    return lax.dot_general(lhs, rhs, NT, preferred_element_type=F32)


def dot_tn(lhs, rhs):
    return lax.dot_general(lhs, rhs, TN, preferred_element_type=F32)


def params(collective_id=None, semantics=None):
    if collective_id is None:
        return pltpu.CompilerParams(vmem_limit_bytes=VMEM_LIMIT, dimension_semantics=semantics)
    return pltpu.CompilerParams(vmem_limit_bytes=VMEM_LIMIT, collective_id=collective_id, has_side_effects=True)


def row_mean(values):
    return jnp.mean(values, axis=-1, keepdims=True)


def row_sum(values):
    return jnp.sum(values, axis=-1, keepdims=True)


def rope_tables(seq_len, fine):
    half_dim = HEAD_DIM // 2
    freqs = np.float32(ROPE_BASE) ** (np.float32(-2.0) * np.arange(half_dim, dtype=np.float32) / np.float32(HEAD_DIM))
    tables = []
    for positions in (np.arange(fine), np.arange(0, seq_len, fine)):
        angles = positions.astype(np.float32)[:, None] * freqs[None, :]
        tables += [np.tile(np.cos(angles), 2).astype(np.float32), np.tile(np.sin(angles), 2).astype(np.float32)]
    return tables


def fill_rope(fine_cos, fine_sin, coarse_cos, coarse_sin, cos_ref, sin_ref):
    fine = height(fine_cos)
    sign = jnp.where(lax.broadcasted_iota(jnp.int32, (1, HEAD_DIM), 1) < HEAD_DIM // 2, -1.0, 1.0)

    def body(idx, carry):
        span = piece_at(idx, fine)
        big_cos, big_sin = coarse_cos[pl.ds(idx, 1)], coarse_sin[pl.ds(idx, 1)]
        cos_ref[span] = big_cos * fine_cos[...] - big_sin * fine_sin[...]
        sin_ref[span] = (big_sin * fine_cos[...] + big_cos * fine_sin[...]) * sign
        return carry

    loop(height(cos_ref) // fine, body)


def rotate(values, cos_tab, sin_tab):
    return values * cos_tab + pltpu.roll(values, HEAD_DIM // 2, 1) * sin_tab


def rms_scale(x_f32, gain_row):
    inv_rms = lax.rsqrt(row_mean(x_f32 * x_f32) + NORM_EPS)
    return x_f32 * inv_rms * gain_row


def ring_place():
    me = lax.axis_index('tp')
    chip = me // 2
    core = me % 2
    return me, chip, core


def device_at(chip, core):
    return ((chip + N_CHIPS) % N_CHIPS) * 2 + core


def remote_copy(src, dst, send_sem, recv_sem, peer):
    return pltpu.make_async_remote_copy(
        src_ref=src, dst_ref=dst, send_sem=send_sem, recv_sem=recv_sem, device_id={'tp': peer}, device_id_type=pl.DeviceIdType.MESH
    )


def meet(peers):
    barrier = pltpu.get_barrier_semaphore()
    for peer in peers:
        pl.semaphore_signal(barrier, inc=1, device_id={'tp': peer}, device_id_type=pl.DeviceIdType.MESH)
    pl.semaphore_wait(barrier, len(peers))


OWN_PARTNER, OWN_AHEAD, OWN_BEHIND, FIRST_PARTNER, FIRST_AHEAD, SECOND_PARTNER, THIRD_PARTNER = KINDS = range(7)


class Gather:
    EVERY, EARLY, LATE = range(SUBS), range(SUBS // 2), range(SUBS // 2, SUBS)

    def __init__(self, full, send_sems, recv_sems):
        self.full, self.send_sems, self.recv_sems = full, send_sems, recv_sems
        self.me, chip, core = ring_place()
        turn = 1 - 2 * core
        self.chip, self.core, self.turn = chip, core, turn
        self.partner = device_at(chip, 1 - core)
        self.ahead = device_at(chip + turn, core)
        self.behind = device_at(chip - turn, core)
        self.first = device_at(chip - turn, core)
        self.first_other = device_at(chip + turn, 1 - core)
        self.second = device_at(chip + turn, core)
        self.second_other = device_at(chip - turn, 1 - core)
        self.third = device_at(chip + 2, core)
        self.third_other = device_at(chip + 2, 1 - core)

    def peers(self):
        return self.partner, self.ahead, self.behind

    def piece(self, kind, shard, sub, peer):
        rows = width_of(self.full) // SUBS
        part = self.full.at[shard, pl.ds(sub * rows, rows)]
        return remote_copy(part, part, self.send_sems.at[kind, sub], self.recv_sems.at[shard, sub], peer)

    def send(self, kind, shard, peer, subs=EVERY):
        for sub in subs:
            self.piece(kind, shard, sub, peer).start()

    def sent(self, kind, shard, peer, subs=EVERY):
        for sub in subs:
            self.piece(kind, shard, sub, peer).wait_send()

    def arrived(self, shard, subs=EVERY, pass_on=None):
        for sub in subs:
            self.piece(OWN_PARTNER, shard, sub, self.partner).wait_recv()
            if pass_on is not None:
                self.piece(pass_on, shard, sub, self.partner).start()

    def launch(self, subs=EVERY):
        self.send(OWN_AHEAD, self.me, self.ahead, subs)
        self.send(OWN_PARTNER, self.me, self.partner, subs)

    def turn_back(self):
        self.sent(OWN_AHEAD, self.me, self.ahead, range(SUBS - 1))
        self.send(OWN_BEHIND, self.me, self.behind)

    def pass_ahead(self):
        self.sent(OWN_BEHIND, self.me, self.behind, range(SUBS - 1))
        self.send(FIRST_AHEAD, self.first, self.ahead)

    def launch_both(self):
        self.launch()
        self.send(OWN_BEHIND, self.me, self.behind)

    def pass_piece(self, sub):
        self.piece(OWN_PARTNER, self.first, sub, self.partner).wait_recv()
        self.piece(FIRST_AHEAD, self.first, sub, self.ahead).start()
        self.piece(FIRST_PARTNER, self.first, sub, self.partner).start()
        self.arrived(self.second, (sub,), SECOND_PARTNER)

    def end_piece(self, sub):
        self.arrived(self.third, (sub,), THIRD_PARTNER)

    def events(self, early=False):
        return (
            lambda: None,
            lambda: (self.turn_back(), self.arrived(self.partner)),
            lambda: self.arrived(self.first, pass_on=FIRST_PARTNER),
            lambda: (self.pass_ahead() if early else None, self.arrived(self.first_other)),
            lambda: (None if early else self.pass_ahead(), self.arrived(self.second, pass_on=SECOND_PARTNER)),
            lambda: self.arrived(self.second_other),
            lambda: (self.arrived(self.third, self.EARLY, THIRD_PARTNER), self.arrived(self.third_other, self.EARLY)),
            lambda: (self.arrived(self.third, self.LATE, THIRD_PARTNER), self.arrived(self.third_other, self.LATE)),
        )

    def places(self, step):
        half = width_of(self.full) // 2
        pair = step // 2
        odd = step % BUFFERS
        side = self.turn * (1 - 2 * odd)
        hop = (3 * pair + (pair // 2) * (2 * pair - 5)) % N_CHIPS
        shard = device_at((self.chip + side * hop + N_DEVICES) % N_CHIPS, (self.core + odd) % 2)
        last = step // (N_DEVICES - 2)
        upper = (1 - last) * shard + last * self.third
        lower = (1 - last) * shard + last * self.third_other
        return (upper, last * odd * half), (lower, (1 - last) * half + last * odd * half)

    def finish(self, waited=SUBS - 1):
        self.sent(OWN_PARTNER, self.me, self.partner)
        self.sent(OWN_AHEAD, self.me, self.ahead, range(waited, SUBS))
        self.sent(OWN_BEHIND, self.me, self.behind, range(waited, SUBS))
        self.sent(FIRST_PARTNER, self.first, self.partner)
        self.sent(FIRST_AHEAD, self.first, self.ahead)
        self.sent(SECOND_PARTNER, self.second, self.partner)
        self.sent(THIRD_PARTNER, self.third, self.partner)


def run_at(step, actions):
    for idx, action in enumerate(actions):
        @pl.when(step == idx)
        def _():
            action()


def gather_scratch(tp_size, rows, width):
    return [
        pltpu.VMEM((tp_size, rows, width), BF16),
        dma_sems(len(KINDS), SUBS),
        dma_sems(tp_size, SUBS),
    ]


def half_rows(ref, place, half):
    return ref[place[0], pl.ds(pl.multiple_of(place[1], half), half)]


def both_halves(ref, places, half):
    return jnp.concatenate([half_rows(ref, place, half) for place in places], axis=0)


def table_rows(ref, places, half, rows):
    parts = [ref[pl.ds(pl.multiple_of(shard * rows + row, half), half)] for shard, row in places]
    return jnp.concatenate(parts, axis=0)


class RowWriter:
    def __init__(self, stages, outs, sems, rows):
        self.stages, self.outs, self.sems, self.rows = stages, outs, sems, rows

    def copies(self, slot, places):
        half = self.rows // 2
        items = []
        for idx in range(len(self.outs)):
            for part, (shard, row) in enumerate(places):
                start = pl.multiple_of(shard * self.rows + row, half)
                src = self.stages[idx].at[slot, pl.ds(part * half, half)]
                items.append(pltpu.make_async_copy(src, self.outs[idx].at[pl.ds(start, half)], self.sems.at[idx, slot, part]))
        return items

    def reuse(self, step):
        @pl.when(step >= 2)
        def _():
            for item in self.copies(step % BUFFERS, ((0, 0), (0, 0))):
                item.wait()

    def start(self, step, places):
        for item in self.copies(step % BUFFERS, places):
            item.start()

    def finish(self):
        for slot in range(BUFFERS):
            for item in self.copies(slot, ((0, 0), (0, 0))):
                item.wait()


def project_loads(layer, sources, weights, sems):
    loads, spans, start = [], [], 0
    for idx, src in enumerate(sources):
        spans.append(slice(start, start + src.shape[-1]))
        start += src.shape[-1]
        loads.append(pltpu.make_async_copy(src.at[layer], weights.at[:, spans[-1]], sems.at[idx]))
    return loads, spans


def project_steps(gather, weights, spans, stages, writer, cos_ref, sin_ref, with_hidden):
    rows = width_of(gather.full)
    half = rows // CORES

    def step_body(step, carry):
        run_at(step, gather.events())
        places = gather.places(step)
        slot = step % BUFFERS
        writer.reuse(step)
        cos_tab, sin_tab = table_rows(cos_ref, places, half, rows), table_rows(sin_ref, places, half, rows)
        product = dot(both_halves(gather.full, places, half), weights[...]).astype(BF16)
        qkv, gate, up = (product[:, span] for span in spans)
        for head in range(width_of(qkv) // HEAD_DIM):
            cols = slice(head * HEAD_DIM, (head + 1) * HEAD_DIM)
            part = qkv[:, cols]
            if head % 3 != 2:
                part = rotate(part.astype(F32), cos_tab, sin_tab).astype(BF16)
            stages[0][slot, :, cols] = part
        stages[1][slot] = gate
        stages[2][slot] = up
        if with_hidden:
            stages[3][slot] = (jax.nn.silu(gate.astype(F32)) * up.astype(F32)).astype(BF16)
        writer.start(step, places)
        return carry

    loop(N_DEVICES, step_body)
    gather.finish()
    writer.finish()


def project_kernel(layer, x_ref, gain_ref, w_qkv_hbm, w_gate_hbm, w_up_hbm, *rest):
    tables, rest = rest[:4], rest[4:]
    outs, rest = rest[:4], rest[4:]
    u_hbm, cos_out, sin_out, *rest = rest
    stages, rest = rest[:4], rest[4:]
    cos_ref, sin_ref, weights, full, send_sems, recv_sems, w_sems, keep_sems, out_sems = rest
    rows = width_of(full)
    gather = Gather(full, send_sems, recv_sems)
    loads, spans = project_loads(layer, (w_qkv_hbm, w_gate_hbm, w_up_hbm), weights, w_sems)
    keeps = [
        pltpu.make_async_copy(src, dst, keep_sems.at[idx])
        for idx, (src, dst) in enumerate(((cos_ref, cos_out), (sin_ref, sin_out), (full.at[gather.me], u_hbm)))
    ]
    norm_rows = min(ROWS_AT_ONCE, rows // SUBS)

    def norm(idx, carry):
        span = piece_at(idx, norm_rows)
        normed = rms_scale(x_ref[span].astype(F32), gain_ref[layer:layer + 1]).astype(BF16)
        full[gather.me, span] = normed
        return carry

    for load in loads:
        load.start()
    meet(gather.peers())
    per_piece = rows // SUBS // norm_rows
    for sub in range(SUBS):
        lax.fori_loop(sub * per_piece, (sub + 1) * per_piece, norm, 0)
        gather.launch((sub,))
    fill_rope(*tables, cos_ref, sin_ref)
    for item in keeps:
        item.start()
    for load in loads:
        load.wait()
    project_steps(gather, weights, spans, stages, RowWriter(stages, outs, out_sems, rows), cos_ref, sin_ref, True)
    for item in keeps:
        item.wait()


def project(x_loc, norm_gain, w_qkv, w_gate, w_up, tables, layer, tp_size):
    rows, width = x_loc.shape
    seq_len = rows * tp_size
    out_cols = [item.shape[-1] for item in (w_qkv, w_gate, w_up, w_up)]
    table = (seq_len, HEAD_DIM)
    outs = [jax.ShapeDtypeStruct((seq_len, cols), BF16) for cols in out_cols]
    outs += [jax.ShapeDtypeStruct((rows, width), BF16)] + [jax.ShapeDtypeStruct(table, F32)] * 2
    scratch = [pltpu.VMEM((BUFFERS, rows, cols), BF16) for cols in out_cols]
    scratch += [pltpu.VMEM(table, F32)] * 2
    scratch += [pltpu.VMEM((width, sum(out_cols[:3])), BF16)]
    scratch += gather_scratch(tp_size, rows, width)
    scratch += [dma_sems(3), dma_sems(3), dma_sems(len(out_cols), BUFFERS, CORES)]
    return pl.pallas_call(
        functools.partial(project_kernel, layer),
        out_shape=outs,
        in_specs=[VMEM] * 2 + [ANY] * 3 + [VMEM] * len(tables),
        out_specs=[ANY] * len(outs),
        scratch_shapes=scratch,
        compiler_params=params(collective_id=1 + layer),
        name=f'project_{layer}',
    )(x_loc, norm_gain, w_qkv, w_gate, w_up, *tables)


EACH = 4
PER_STEP = WAYS * EACH
N_BLOCKS = N_CHIPS * PER_STEP
N_PAIRS = (N_BLOCKS - PER_STEP) // 2
SLOTS = 6


def scatter_blocks(peers, load, early, product, beside, tmp, acc, ring, pair_send, pair_recv, ring_send, ring_recv):
    me, chip, core = ring_place()
    partner = device_at(chip, 1 - core)
    meet(peers or (partner, device_at(chip + 1, core), device_at(chip - 1, core)))

    def dest(step, way):
        return (chip + (step + 1) * (WAYS * way - 1) + N_DEVICES) % N_CHIPS

    def to_partner(block, slot):
        return remote_copy(tmp.at[slot, 1 - core], acc.at[block], pair_send.at[slot], pair_recv.at[block], partner)

    def to_next(block):
        peer = device_at(chip + 1 - 2 * (block % WAYS), core)
        return remote_copy(acc.at[block], ring.at[block], ring_send.at[block], ring_recv.at[block], peer)

    def serve_first(block):
        to_partner(block, block % SLOTS).wait_recv()
        acc[block] = acc[block] + tmp[block % SLOTS, core]
        to_next(block).start()

    def first_body(block, carry):
        load(block)
        early(block)

        @pl.when(block >= SLOTS)
        def _():
            to_partner(block - SLOTS, block % SLOTS).wait_send()

        way = block % WAYS
        product(dest(0, way), way * EACH + block // WAYS, 1, tmp.at[pl.ds(block % SLOTS, 1)])
        to_partner(block, block % SLOTS).start()

        @pl.when(block >= 1)
        def _():
            serve_first(block - 1)

        return carry

    loop(PER_STEP, first_body)

    def pair_blocks(pair):
        step, rest = 1 + pair // EACH, pair % EACH
        way, col = rest % WAYS, 2 * (rest // 2)
        block = step * PER_STEP + 2 * col + way
        slot = (PER_STEP + 2 * pair) % SLOTS
        return step, way, col, ((block, slot), (block + 2, slot + 1))

    def body(pair, carry):
        @pl.when(pair < N_PAIRS)
        def _():
            step, way, col, blocks = pair_blocks(pair)
            load(PER_STEP + pair)
            for block, slot in blocks:
                to_partner(block, slot).wait_send()
            product(dest(step, way), way * EACH + col, 2, tmp.at[pl.ds(blocks[0][1], 2)])
            for block, slot in blocks:
                to_partner(block, slot).start()
            beside(pair)

        @pl.when(pair == 0)
        def _():
            serve_first(PER_STEP - 1)

        @pl.when(pair >= 1)
        def _():
            step, way, col, blocks = pair_blocks(pair - 1)
            for block, slot in blocks:
                to_partner(block, slot).wait_recv()
                to_next(block - PER_STEP).wait_recv()
                acc[block] = (acc[block] + tmp[slot, core]) + ring[block - PER_STEP]

                @pl.when(step < N_CHIPS - 1)
                def _():
                    to_next(block).start()

        return carry

    loop(N_PAIRS + 1, body)
    for slot in range(SLOTS):
        to_partner(0, slot).wait_send()
    for block in range(N_BLOCKS - PER_STEP):
        to_next(block).wait_send()
    return lambda cols: acc.at[N_BLOCKS - PER_STEP + 2 * (cols % EACH) + cols // EACH]


def scatter_scratch(rows, width):
    cols = width // PER_STEP
    return [
        pltpu.VMEM((SLOTS, 2, rows, cols), F32),
        pltpu.VMEM((N_BLOCKS, rows, cols), F32),
        pltpu.VMEM((N_BLOCKS - PER_STEP, rows, cols), F32),
        dma_sems(SLOTS),
        dma_sems(N_BLOCKS),
        dma_sems(N_BLOCKS - PER_STEP),
        dma_sems(N_BLOCKS - PER_STEP),
    ]


def start_loads(w_load, row_loads_of, later):
    order = [(block % WAYS) * EACH + block // WAYS for block in range(PER_STEP)]
    needed = [w_load(cols) + (row_loads_of[idx] if idx < WAYS else []) for idx, cols in enumerate(order)]
    for item in needed[0] + needed[1]:
        item.start()

    def load(product):
        for idx in range(PER_STEP):
            @pl.when(product == idx)
            def _():
                for item in needed[idx]:
                    item.wait()
                for item in (needed[idx + WAYS] if idx + WAYS < PER_STEP else []) + later.get(idx, []):
                    item.start()

    return load


def row_loads(pairs, sems, rows, chip):
    def load(order, hop):
        span = pl.ds(pl.multiple_of(((chip + hop) % N_CHIPS) * rows, rows), rows)
        return [pltpu.make_async_copy(src.at[span], dst.at[span], sems.at[idx, order]) for idx, (src, dst) in enumerate(pairs)]

    return [load(order, hop) for order, hop in enumerate((3, 1, 2, 0))]


def block_kernel(layer, qkv_hbm, m_hbm, w_out_hbm, w_down_hbm, x_hbm, gain_ref, w_qkv_hbm, w_gate_hbm, w_up_hbm, cos_hbm, sin_hbm, *rest):
    y_hbm, u_hbm, o_hbm, lse_hbm, *rest = rest
    outs, rest = rest[:3], rest[3:]
    stages, (x_ref, y_ref, *rest) = rest[:3], rest[3:]
    qkv, o_all, lse, m_all, w_out, w_down, weights, cos_ref, sin_ref, row_sems, w_sems, load_sems, out_sems = rest[:13]
    (full, send_sems, recv_sems), scatter = rest[13:16], rest[16:]
    me, chip, core = ring_place()
    rows, width = x_hbm.shape
    block_cols = width // PER_STEP
    loads = row_loads(((m_hbm, m_all),), row_sems, CORES * rows, chip)
    gather = Gather(full, send_sems, recv_sems)
    qkv_load, x_load, *keeps = [
        pltpu.make_async_copy(src, dst, load_sems.at[3 + idx])
        for idx, (src, dst) in enumerate(((qkv_hbm, qkv), (x_hbm, x_ref), (o_all, o_hbm), (lse, lse_hbm), (y_ref, y_hbm), (full.at[me], u_hbm)))
    ]
    keeps, keeps_after = keeps[:2], keeps[2:]
    next_loads, spans = project_loads(layer + 1, (w_qkv_hbm, w_gate_hbm, w_up_hbm), weights, load_sems)
    next_loads += [pltpu.make_async_copy(src, dst, load_sems.at[9 + idx]) for idx, (src, dst) in enumerate(((cos_hbm, cos_ref), (sin_hbm, sin_ref)))]

    def w_load(cols):
        span = pl.ds(cols * block_cols, block_cols)
        return [
            pltpu.make_async_copy(src.at[layer, :, span], dst.at[:, span], w_sems.at[idx, cols])
            for idx, (src, dst) in enumerate(((w_out_hbm, w_out), (w_down_hbm, w_down)))
        ]

    qkv_load.start()
    qkv_load.wait()
    load_first = start_loads(w_load, loads, {4: loads[2], 6: loads[3]})

    def load(product):
        load_first(product)
        for items, at in ((loads[2], PER_STEP), (loads[3], PER_STEP + WAYS * EACH)):
            @pl.when(product == at)
            def _():
                for item in items:
                    item.wait()

        @pl.when(product == PER_STEP)
        def _():
            for item in [x_load] + keeps + next_loads:
                item.start()

    def attend(index):
        def head_rows(q_start):
            def body(head, carry):
                attend_rows(q_start, head, qkv, o_all, lse)
                return carry

            loop(width_of(o_all) // HEAD_DIM, body)

        run_at(index, [functools.partial(head_rows, q_start) for q_start in range(0, height(qkv), Q_ROWS)])

    def early(block):
        turn = block - block // 4 * 2 - block // 6
        dest = (chip + 3 + 2 * turn + turn // 2 * 3) % N_CHIPS
        per_chip = CORES * rows // Q_ROWS

        @pl.when((block == 0) | (block == 1) | (block == 4) | (block == 6))
        def _():
            def body(idx, carry):
                attend(dest * per_chip + idx)
                return carry

            loop(per_chip, body)

    def product(dest, cols, n_cols, out):
        span = piece_at(dest, CORES * rows)
        w_span = pl.ds(pl.multiple_of(cols * block_cols, block_cols), n_cols * block_cols)
        total = dot(o_all[span], w_out[:, w_span]) + dot(m_all[span], w_down[:, w_span])
        for idx in range(n_cols):
            for kind in range(CORES):
                out[idx, kind] = total[kind * rows:(kind + 1) * rows, idx * block_cols:(idx + 1) * block_cols]

    result = scatter_blocks(gather.peers(), load, early, product, lambda pair: None, *scatter)
    norm_rows = min(ROWS_AT_ONCE, rows // SUBS)
    x_load.wait()

    def finish(idx, carry):
        span = piece_at(idx, norm_rows)
        summed = jnp.concatenate([result(cols)[span] for cols in range(PER_STEP)], axis=1)
        y = (x_ref[span].astype(F32) + summed).astype(BF16)
        normed = rms_scale(y.astype(F32), gain_ref[layer + 1:layer + 2]).astype(BF16)
        y_ref[span] = y
        full[me, span] = normed
        return carry

    per_piece = rows // SUBS // norm_rows
    for sub in range(SUBS):
        lax.fori_loop(sub * per_piece, (sub + 1) * per_piece, finish, 0)
        gather.launch((sub,))
    for item in keeps_after:
        item.start()
    for item in next_loads:
        item.wait()
    project_steps(gather, weights, spans, stages, RowWriter(stages, outs, out_sems, rows), cos_ref, sin_ref, False)
    for item in keeps + keeps_after:
        item.wait()


def block_rest(qkv, hidden, w_out, w_down, x_loc, norm_gain, w_qkv, w_gate, w_up, tables, layer, tp_size):
    rows, width = x_loc.shape
    seq_len = height(qkv)
    o_cols, ff_cols = width_of(w_out), width_of(w_down)
    out_cols = [item.shape[-1] for item in (w_qkv, w_gate, w_up)]
    outs = [((rows, width), BF16), ((rows, width), BF16), ((seq_len, o_cols), BF16), ((seq_len, o_cols), F32)]
    outs += [((seq_len, cols), BF16) for cols in out_cols]
    scratch = [pltpu.VMEM((BUFFERS, rows, cols), BF16) for cols in out_cols]
    scratch += [pltpu.VMEM((rows, width), BF16)] * 2
    scratch += [
        pltpu.VMEM(qkv.shape, BF16),
        pltpu.VMEM((seq_len, o_cols), BF16),
        pltpu.VMEM((seq_len, o_cols), F32),
        pltpu.VMEM((seq_len, ff_cols), BF16),
        pltpu.VMEM((o_cols, width), BF16),
        pltpu.VMEM((ff_cols, width), BF16),
        pltpu.VMEM((width, sum(out_cols)), BF16),
    ]
    scratch += [pltpu.VMEM(table.shape, F32) for table in tables]
    scratch += [dma_sems(1, N_CHIPS), dma_sems(CORES, PER_STEP), dma_sems(11), dma_sems(len(out_cols), BUFFERS, CORES)]
    return pl.pallas_call(
        functools.partial(block_kernel, layer),
        out_shape=[jax.ShapeDtypeStruct(*item) for item in outs],
        in_specs=[ANY] * 5 + [VMEM] + [ANY] * 5,
        out_specs=[ANY] * len(outs),
        scratch_shapes=scratch + gather_scratch(tp_size, rows, width) + scatter_scratch(rows, width),
        compiler_params=params(collective_id=5 + layer),
        name=f'block_rest_{layer}',
    )(qkv, hidden, w_out, w_down, x_loc, norm_gain, w_qkv, w_gate, w_up, *tables)


GRAD_ROWS = N_PAIRS // 3


def backward_kernel(layer, dqkv_hbm, dgate_hbm, dup_hbm, w_qkv_hbm, w_gate_hbm, w_up_hbm, u_hbm, x_hbm, dy_hbm, gain_ref, *rest):
    first_layer = layer == 0
    if first_layer:
        later_gains_ref, *rest = rest
    dx_ref, dgain_ref, *rest = rest
    grads, rest = rest[:3], rest[3:]
    acts, rest = rest[:3], rest[3:]
    weights, rest = rest[:3], rest[3:]
    u_all, x_ref, dy_ref, stage, row_sems, w_sems, u_sem, x_sem, dy_sem, stage_sems, *rest = rest
    if first_layer:
        gain_parts, gain_send, gain_recv, *rest = rest
    scatter = rest
    me, chip, core = ring_place()
    rows, width = x_hbm.shape
    block_cols = width // PER_STEP
    loads = row_loads(list(zip((dqkv_hbm, dgate_hbm, dup_hbm), acts)), row_sems, CORES * rows, chip)
    u_load = pltpu.make_async_copy(u_hbm, u_all, u_sem)
    x_loads = [pltpu.make_async_copy(x_hbm, x_ref, x_sem), pltpu.make_async_copy(dy_hbm, dy_ref, dy_sem)]

    def w_load(cols):
        span = pl.ds(cols * block_cols, block_cols)
        return [
            pltpu.make_async_copy(src.at[layer, span], dst.at[span], w_sems.at[idx, cols])
            for idx, (src, dst) in enumerate(zip((w_qkv_hbm, w_gate_hbm, w_up_hbm), weights))
        ]

    load_first = start_loads(w_load, loads, {2: loads[2], 3: loads[3], 4: [u_load] + x_loads})

    def load(product):
        load_first(product)

        @pl.when(product == PER_STEP)
        def _():
            for item in loads[2] + loads[3] + [u_load] + x_loads:
                item.wait()

    def product(dest, cols, n_cols, out):
        span = piece_at(dest, CORES * rows)
        w_span = pl.ds(pl.multiple_of(cols * block_cols, block_cols), n_cols * block_cols)
        total = dot_nt(acts[0][span], weights[0][w_span]) + dot_nt(acts[1][span], weights[1][w_span]) + dot_nt(acts[2][span], weights[2][w_span])
        for idx in range(n_cols):
            for kind in range(CORES):
                out[idx, kind] = total[kind * rows:(kind + 1) * rows, idx * block_cols:(idx + 1) * block_cols]

    grad_rows = width // GRAD_ROWS

    def grad_out(which, part):
        slot = which % BUFFERS
        src = stage.at[slot, :, :width_of(grads[which])]
        return pltpu.make_async_copy(src, grads[which].at[piece_at(part, grad_rows)], stage_sems.at[slot])

    def beside(task):
        part = task // 3
        cols = piece_at(part, grad_rows)
        for turn, which in enumerate((2, 1, 0)):
            @pl.when(task % 3 == turn)
            def _():
                if which == 2:
                    @pl.when(part > 0)
                    def _():
                        grad_out(0, part - 1).wait()
                elif which == 0:
                    grad_out(2, part).wait()
                else:
                    @pl.when(part > 0)
                    def _():
                        grad_out(1, part - 1).wait()
                stage[which % BUFFERS, :, :width_of(grads[which])] = dot_tn(u_all[:, cols], acts[which][...]).astype(BF16)
                grad_out(which, part).start()

    peers = [(me + 1 + idx) % (N_DEVICES) for idx in range(N_DEVICES - 1)] if first_layer else None
    result = scatter_blocks(peers, load, lambda block: None, product, beside, *scatter)
    gain_row = gain_ref[layer:layer + 1]
    dgain = gain_parts.at[me, layer:layer + 1] if first_layer else dgain_ref
    dgain[...] = jnp.zeros_like(dgain)

    def row_values(idx):
        span = piece_at(idx, ROWS_AT_ONCE)
        summed = jnp.concatenate([result(cols)[span] for cols in range(PER_STEP)], axis=1)
        x_f32 = x_ref[span].astype(F32)
        inv_rms = lax.rsqrt(row_mean(x_f32 * x_f32) + NORM_EPS)
        return span, summed.astype(BF16).astype(F32), x_f32, inv_rms

    def gain_rows(idx, carry):
        _, d_normed, x_f32, inv_rms = row_values(idx)
        dgain[...] += jnp.sum(d_normed * (x_f32 * inv_rms), axis=0, keepdims=True)
        return carry

    def input_rows(idx, carry):
        span, d_normed, x_f32, inv_rms = row_values(idx)
        scaled = d_normed * gain_row
        mix = row_mean(scaled * x_f32) * (inv_rms * inv_rms * inv_rms)
        dx_ref[span] = (dy_ref[span].astype(F32) + (scaled * inv_rms - x_f32 * mix)).astype(BF16)
        return carry

    def both_rows(idx, carry):
        gain_rows(idx, carry)
        return input_rows(idx, carry)

    if first_layer:
        loop(rows // ROWS_AT_ONCE, gain_rows)
        gain_parts[me, 1:] = later_gains_ref[...]
        copies = [remote_copy(gain_parts.at[me], gain_parts.at[me], gain_send.at[idx], gain_recv.at[me], peer) for idx, peer in enumerate(peers)]
        for item in copies:
            item.start()
    loop(rows // ROWS_AT_ONCE, input_rows if first_layer else both_rows)
    if first_layer:
        for idx, peer in enumerate(peers):
            remote_copy(gain_parts.at[peer], gain_parts.at[peer], gain_send.at[idx], gain_recv.at[peer], peer).wait_recv()
        total = gain_parts[0]
        for idx in range(1, N_DEVICES):
            total = total + gain_parts[idx]
        dgain_ref[...] = total
        for item in copies:
            item.wait_send()
    grad_out(0, GRAD_ROWS - 1).wait()
    grad_out(1, GRAD_ROWS - 1).wait()


def block_input_backward(d_qkv, d_gate, d_up, w_qkv, w_gate, w_up, u_full, x_loc, dy_loc, norm_gain, later_gains, layer):
    rows, width = x_loc.shape
    seq_len = height(d_qkv)
    n_layers = height(norm_gain)
    all_cols = (w_qkv.shape[2], w_gate.shape[2], w_up.shape[2])
    first_layer = layer == 0
    out_shape = [jax.ShapeDtypeStruct((rows, width), BF16), jax.ShapeDtypeStruct((n_layers if first_layer else 1, width), F32)]
    out_shape += [jax.ShapeDtypeStruct((width, cols), BF16) for cols in all_cols]
    scratch = [pltpu.VMEM((seq_len, cols), BF16) for cols in all_cols]
    scratch += [pltpu.VMEM((width, cols), BF16) for cols in all_cols]
    scratch += [pltpu.VMEM((seq_len, width), BF16)] + [pltpu.VMEM((rows, width), BF16)] * 2 + [pltpu.VMEM((BUFFERS, width // GRAD_ROWS, max(all_cols)), BF16)]
    scratch += [dma_sems(3, N_CHIPS), dma_sems(3, PER_STEP)] + [pltpu.SemaphoreType.DMA] * 3 + [dma_sems(BUFFERS)]
    if first_layer:
        scratch += [pltpu.VMEM((N_DEVICES, n_layers, width), F32), dma_sems(N_DEVICES - 1), dma_sems(N_DEVICES)]
    return pl.pallas_call(
        functools.partial(backward_kernel, layer),
        out_shape=out_shape,
        in_specs=[ANY] * 9 + [VMEM] * (2 if first_layer else 1),
        out_specs=[VMEM] * 2 + [ANY] * 3,
        scratch_shapes=scratch + scatter_scratch(rows, width),
        compiler_params=params(collective_id=7 + layer),
        name=f'block_input_backward_{layer}',
    )(d_qkv, d_gate, d_up, w_qkv, w_gate, w_up, u_full, x_loc, dy_loc, norm_gain, *((later_gains,) if first_layer else ()))


COLLECT_SLOTS = 4


def collect_kernel(moves, steps, dy_hbm, attn_hbm, hidden_hbm, *refs):
    ins, refs = refs[:len(moves)], refs[len(moves):]
    n_outs = 1 + max(out for out, _ in moves)
    outs, refs = refs[:n_outs], refs[n_outs:]
    buffers, refs = refs[:len(moves)], refs[len(moves):]
    dy_full, attn_out, hidden, stage, in_sems, out_sems, whole_sems, dy_sems, grad_sems = refs
    o_cols, cols = width_of(attn_out), width_of(dy_full) // steps

    def move(idx, step, back):
        rows = width_of(buffers[idx])
        span = piece_at(step, rows)
        slot = step % COLLECT_SLOTS
        out, layer = moves[idx]
        dst = outs[out].at[span] if layer is None else outs[out].at[layer, span]
        if back:
            return pltpu.make_async_copy(buffers[idx].at[slot], dst, out_sems.at[idx, slot])
        return pltpu.make_async_copy(ins[idx].at[span], buffers[idx].at[slot], in_sems.at[idx, slot])

    def moves_of(step, back):
        return [move(idx, step, back) for idx in range(len(moves))]

    def dy_load(step):
        span = piece_at(step, cols)
        return pltpu.make_async_copy(dy_hbm.at[:, span], dy_full.at[:, span], dy_sems.at[step])

    def grads(step):
        span = piece_at(step, cols)
        slot = step % BUFFERS
        return (
            pltpu.make_async_copy(stage.at[slot, :o_cols], outs[1].at[1, :, span], grad_sems.at[slot, 0]),
            pltpu.make_async_copy(stage.at[slot, o_cols:], outs[2].at[1, :, span], grad_sems.at[slot, 1]),
        )

    whole = [pltpu.make_async_copy(attn_hbm, attn_out, whole_sems.at[0]), pltpu.make_async_copy(hidden_hbm, hidden, whole_sems.at[1])]
    for item in moves_of(0, False) + whole + [dy_load(0)] + moves_of(1, False) + moves_of(2, False):
        item.start()
    for step in range(1, steps):
        dy_load(step).start()
    for item in whole:
        item.wait()

    def body(step, carry):
        @pl.when((step >= 1) & (step + 2 < steps))
        def _():
            @pl.when(step >= BUFFERS)
            def _():
                for item in moves_of(step - BUFFERS, True):
                    item.wait()

            for item in moves_of(step + 2, False):
                item.start()

        for item in moves_of(step, False):
            item.wait()
        for item in moves_of(step, True):
            item.start()

        @pl.when(step >= 2)
        def _():
            for item in grads(step - 2):
                item.wait()

        dy_load(step).wait()
        dy_cols = dy_full[:, piece_at(step, cols)]
        slot = step % BUFFERS
        stage[slot, :o_cols] = dot_tn(attn_out[...], dy_cols).astype(BF16)
        stage[slot, o_cols:] = dot_tn(hidden[...], dy_cols).astype(BF16)
        for item in grads(step):
            item.start()
        return carry

    loop(steps, body)
    for step in range(steps - COLLECT_SLOTS, steps):
        for item in moves_of(step, True):
            item.wait()
    for item in grads(steps - 2) + grads(steps - 1):
        item.wait()


def collect(grad_x, dy_full, attn_out, hidden, g_out_first, g_down_first, made, steps):
    n_layers = len(made[0])
    assert n_layers == 2
    seq_len, width, o_cols, ff_cols = height(dy_full), width_of(dy_full), width_of(attn_out), width_of(hidden)
    sources = [(grad_x, 0, None), (g_out_first, 1, 0), (g_down_first, 2, 0)]
    sources += [(item, 3 + idx, layer) for idx, layers in enumerate(made) for layer, item in enumerate(layers)]
    moves = [(out, layer) for _, out, layer in sources]
    out_shape = [jax.ShapeDtypeStruct(grad_x.shape, BF16), jax.ShapeDtypeStruct((n_layers, o_cols, width), BF16), jax.ShapeDtypeStruct((n_layers, ff_cols, width), BF16)]
    out_shape += [jax.ShapeDtypeStruct((n_layers,) + layers[0].shape, BF16) for layers in made]
    scratch = [pltpu.VMEM((COLLECT_SLOTS, height(item) // steps, width_of(item)), BF16) for item, _, _ in sources]
    scratch += [pltpu.VMEM(item.shape, BF16) for item in (dy_full, attn_out, hidden)]
    scratch += [
        pltpu.VMEM((2, o_cols + ff_cols, width // steps), BF16),
        pltpu.SemaphoreType.DMA((len(moves), COLLECT_SLOTS)),
        pltpu.SemaphoreType.DMA((len(moves), COLLECT_SLOTS)),
        dma_sems(2),
        dma_sems(steps),
        dma_sems(2, 2),
    ]
    return pl.pallas_call(
        functools.partial(collect_kernel, moves, steps),
        out_shape=out_shape,
        in_specs=[ANY] * (3 + len(moves)),
        out_specs=[ANY] * len(out_shape),
        scratch_shapes=scratch,
        compiler_params=params(),
        name='collect',
    )(dy_full, attn_out, hidden, *[item for item, _, _ in sources])


def causal_tile(size):
    return lax.broadcasted_iota(jnp.int32, (size, size), 0) >= lax.broadcasted_iota(jnp.int32, (size, size), 1)


def masked_scores(query, keys):
    size = height(query)
    q_start = height(keys) - size
    scores = dot_nt(query, keys)
    diagonal = jnp.where(causal_tile(size), scores[:, q_start:], -1e30)
    scores = diagonal if q_start == 0 else jnp.concatenate([scores[:, :q_start], diagonal], axis=1)
    return scores * (SCALE * LOG2E)


def head_cols(head, part, parts):
    return pl.ds(pl.multiple_of((head * parts + part) * HEAD_DIM, HEAD_DIM), HEAD_DIM)


def attend_rows(q_start, head, qkv_ref, o_ref, lse_ref):
    span, seen = slice(q_start, q_start + Q_ROWS), slice(0, q_start + Q_ROWS)
    scores = masked_scores(qkv_ref[span, head_cols(head, 0, 3)], qkv_ref[seen, head_cols(head, 1, 3)])
    row_max = jnp.max(scores, axis=-1, keepdims=True)
    prob = jnp.exp2(scores - row_max)
    norm = row_sum(prob)
    prob = (prob * (1.0 / norm)).astype(BF16)
    o_ref[span, head_cols(head, 0, 1)] = dot(prob, qkv_ref[seen, head_cols(head, 2, 3)]).astype(BF16)
    lse_ref[span, head_cols(head, 0, 1)] = jnp.broadcast_to(row_max + jnp.log2(norm), (Q_ROWS, HEAD_DIM))


def attend_rows_backward(q_start, head, qkv_ref, lse_ref, do_ref, o_ref, cos_ref, sin_ref, dq_ref, dkt_acc, dvt_acc, prob_tmp, ds_tmp):
    span, seen = slice(q_start, q_start + Q_ROWS), slice(0, q_start + Q_ROWS)
    query = qkv_ref[span, head_cols(head, 0, 3)]
    d_out = do_ref[span, head_cols(head, 0, 1)]
    inner = row_sum(d_out.astype(F32) * o_ref[span, head_cols(head, 0, 1)].astype(F32))
    lse = lse_ref[span, head_cols(head, 0, 1)][:, :1]
    for k_start in range(0, q_start + Q_ROWS, Q_ROWS):
        keys = slice(k_start, k_start + Q_ROWS)
        scores = dot_nt(query, qkv_ref[keys, head_cols(head, 1, 3)]) * (SCALE * LOG2E)
        if k_start == q_start:
            scores = jnp.where(causal_tile(Q_ROWS), scores, -1e30)
        prob = jnp.exp2(scores - lse)
        d_prob = dot_nt(d_out, qkv_ref[keys, head_cols(head, 2, 3)]).astype(BF16).astype(F32)
        ds_tmp[:, keys] = (prob * (d_prob - inner) * SCALE).astype(BF16)
        prob_tmp[:, keys] = prob.astype(BF16)
    dvt_acc[head, :, seen] += dot_tn(d_out, prob_tmp[:, seen])
    dkt_acc[head, :, seen] += dot_tn(query, ds_tmp[:, seen])
    d_query = dot(ds_tmp[:, seen], qkv_ref[seen, head_cols(head, 1, 3)]).astype(BF16)
    dq_ref[span, head_cols(head, 0, 3)] = rotate(d_query.astype(F32), cos_ref[span], -sin_ref[span]).astype(BF16)


def middle_kernel(layer, with_forward, dy_hbm, u_hbm, w_out_hbm, w_down_hbm, gate_hbm, up_hbm, cos_hbm, sin_hbm, qkv_hbm, *rest):
    if not with_forward:
        (o_hbm, lse_hbm), rest = rest[:2], rest[2:]
    (dgate_hbm, dup_hbm, dqkv_hbm, u_full_hbm), rest = rest[:4], rest[4:]
    if with_forward:
        (dy_full_hbm, o_hbm, hidden_hbm), rest = rest[:3], rest[3:]
    else:
        (g_out_hbm, g_down_hbm), rest = rest[:2], rest[2:]
    (dgate_stage, dup_stage, gate_in, up_in, weights, qkv, o_all, lse, hidden, d_attn, dqkv, dk_acc, dv_acc, prob_tmp, ds_tmp, grad_stage, cos_ref, sin_ref), rest = rest[:18], rest[18:]
    dy_full, dy_send, dy_recv, u_full, u_send, u_recv, load_sems, out_sems, in_sems, u_sems, dqkv_sem, grad_sems = rest
    rows = width_of(dy_full)
    half = rows // 2
    seq_len = height(qkv)
    n_heads = width_of(o_all) // HEAD_DIM
    o_cols = width_of(o_all)
    gather = Gather(dy_full, dy_send, dy_recv)
    u_gather = Gather(u_full, u_send, u_recv)
    me = gather.me
    own_dy = pltpu.make_async_copy(dy_hbm, dy_full.at[me], load_sems.at[0])
    own_u = pltpu.make_async_copy(u_hbm, u_full.at[me], load_sems.at[1])
    w_loads = [
        pltpu.make_async_copy(w_out_hbm.at[layer], weights.at[:o_cols], load_sems.at[2]),
        pltpu.make_async_copy(w_down_hbm.at[layer], weights.at[o_cols:], load_sems.at[3]),
    ]
    loads = [
        pltpu.make_async_copy(src, dst, load_sems.at[4 + idx])
        for idx, (src, dst) in enumerate([(qkv_hbm, qkv), (cos_hbm, cos_ref), (sin_hbm, sin_ref)] + ([] if with_forward else [(o_hbm, o_all), (lse_hbm, lse)]))
    ]
    writer = RowWriter((dgate_stage, dup_stage), (dgate_hbm, dup_hbm), out_sems, rows)
    own_dy.start()
    meet(gather.peers())
    own_dy.wait()
    gather.launch()
    for item in w_loads + loads + [own_u]:
        item.start()
    dk_acc[...] = jnp.zeros_like(dk_acc)
    dv_acc[...] = jnp.zeros_like(dv_acc)
    for item in w_loads:
        item.wait()

    def both_heads(function, q_start, *args):
        def body(head, carry):
            function(q_start, head, *args)
            return carry

        loop(n_heads, body)

    def attend(index):
        run_at(index, [functools.partial(both_heads, attend_rows, q_start, qkv, o_all, lse) for q_start in range(0, seq_len, Q_ROWS)])

    def attend_backward(index):
        refs = (qkv, lse, d_attn, o_all, cos_ref, sin_ref, dqkv, dk_acc, dv_acc, prob_tmp, ds_tmp)
        run_at(index, [functools.partial(both_heads, attend_rows_backward, q_start, *refs) for q_start in range(0, seq_len, Q_ROWS)])

    def finish_keys_values():
        def body(idx, carry):
            span = piece_at(idx, Q_ROWS)
            for head in range(n_heads):
                d_keys = dk_acc[head, :, span].T.astype(BF16).astype(F32)
                dqkv[span, head_cols(head, 1, 3)] = rotate(d_keys, cos_ref[span], -sin_ref[span]).astype(BF16)
                dqkv[span, head_cols(head, 2, 3)] = dv_acc[head, :, span].T.astype(BF16)
            return carry

        loop(seq_len // Q_ROWS, body)
        keep_dqkv.start()

    keep_dqkv = pltpu.make_async_copy(dqkv, dqkv_hbm, dqkv_sem)

    def dy_rows(step):
        run_at(step, gather.events(early=True))

        @pl.when(step == N_DEVICES - 2)
        def _():
            own_u.wait()
            u_gather.launch_both()
            keep_u(me)

        places = gather.places(step)
        slot = step % BUFFERS
        fetch = []
        for idx, (src, dst) in enumerate(((gate_hbm, gate_in), (up_hbm, up_in))):
            for part, (shard, row) in enumerate(places):
                here = pl.ds(pl.multiple_of(shard * rows + row, half), half)
                fetch.append(pltpu.make_async_copy(src.at[here], dst.at[pl.ds(part * half, half)], in_sems.at[idx, part]))
        for item in fetch:
            item.start()
        writer.reuse(step)
        product = dot_nt(both_halves(dy_full, places, half), weights[...]).astype(BF16)
        d_hidden = product[:, o_cols:].astype(F32)
        for item in fetch:
            item.wait()
        gate, up = gate_in[...].astype(F32), up_in[...].astype(F32)
        sig = jax.nn.sigmoid(gate)
        act = gate * sig
        hidden_rows = (act * up).astype(BF16)
        for part, (shard, row) in enumerate(places):
            here = pl.ds(pl.multiple_of(shard * rows + row, half), half)
            d_attn[here] = product[part * half:(part + 1) * half, :o_cols]
            hidden[here] = hidden_rows[part * half:(part + 1) * half]
        dgate_stage[slot] = (d_hidden * up * (sig + act * (1.0 - sig))).astype(BF16)
        dup_stage[slot] = (d_hidden * act).astype(BF16)
        writer.start(step, places)

    def wait_loads(step):
        @pl.when(step == 0)
        def _():
            for item in loads:
                item.wait()

    def dy_step_forward(step, carry):
        dy_rows(step)
        wait_loads(step)
        attend(seq_len // Q_ROWS - 1 - step)
        return carry

    def dy_step_backward(step, carry):
        @pl.when(step < N_DEVICES)
        def _():
            dy_rows(step)

        wait_loads(step)
        after = step // (N_DEVICES)
        turn = (1 - after) * (step // 2) + after * (step - 5)
        upper, lower = gather.places(turn)
        shard = upper[0] + (turn // 7) * (lower[0] - upper[0])

        @pl.when(step == 10)
        def _():
            u_gather.pass_piece(0)

        @pl.when(step == 12)
        def _():
            u_gather.pass_piece(1)

        @pl.when((step == 0) | (step == 3) | (step == 5) | (step >= N_DEVICES))
        def _():
            attend_backward(shard * rows // Q_ROWS)

        return carry

    def keep_u(shard):
        pltpu.make_async_copy(u_full.at[shard], u_full_hbm.at[shard], u_sems.at[shard]).start()

    if with_forward:
        loop(N_DEVICES, dy_step_forward)
    else:
        loop(N_DEVICES + 5, dy_step_backward)

    def grad_copies(step):
        slot = step % BUFFERS
        cols = piece_at(step, grad_cols)
        return (
            pltpu.make_async_copy(grad_stage.at[slot, :o_cols], g_out_hbm.at[:, cols], grad_sems.at[slot, 0]),
            pltpu.make_async_copy(grad_stage.at[slot, o_cols:], g_down_hbm.at[:, cols], grad_sems.at[slot, 1]),
        )

    grad_cols = dy_full.shape[2] // (N_DEVICES)
    first_parts, last_parts = u_gather.pass_piece, u_gather.end_piece
    if with_forward:
        u_at = {1: [0], 2: [1], 4: [2], 7: [3]}
    else:
        u_at = {1: [2], 4: [3], 6: [4], 7: [5]}

    def u_event(at):
        for part in u_at.get(at, ()):
            first_parts(part) if part < SUBS else last_parts(part - SUBS)
        if at == 2 and not with_forward:
            finish_keys_values()

    u_events = [functools.partial(u_event, at) for at in range(N_DEVICES)]
    last_part = max(part for parts in u_at.values() for part in parts) + 1

    def u_step(step, carry):
        run_at(step, u_events)
        if with_forward:
            attend_backward(seq_len // Q_ROWS - 1 - step)
            return carry

        @pl.when(step >= 2)
        def _():
            for item in grad_copies(step - 2):
                item.wait()

        cols = piece_at(step, grad_cols)
        dy_cols = dy_full[:, :, cols].reshape(seq_len, grad_cols)
        slot = step % BUFFERS
        grad_stage[slot, :o_cols] = dot_tn(o_all[...], dy_cols).astype(BF16)
        grad_stage[slot, o_cols:] = dot_tn(hidden[...], dy_cols).astype(BF16)
        for item in grad_copies(step):
            item.start()
        return carry

    if with_forward:
        keeps = [pltpu.make_async_copy(src, dst, grad_sems.at[0, idx]) for idx, (src, dst) in enumerate(((o_all, o_hbm), (hidden, hidden_hbm)))]
        keeps += [pltpu.make_async_copy(dy_full, dy_full_hbm, grad_sems.at[1, 0])]
        for item in keeps:
            item.start()
    loop(N_DEVICES, u_step)
    if with_forward:
        finish_keys_values()
    for shard in (u_gather.partner, u_gather.first_other, u_gather.second_other):
        u_gather.arrived(shard)
        keep_u(shard)
    for shard in (u_gather.first, u_gather.second):
        keep_u(shard)
    for part in range(last_part, 2 * SUBS):
        last_parts(part - SUBS)
    keep_u(u_gather.third)
    u_gather.arrived(u_gather.third_other)
    keep_u(u_gather.third_other)
    for item in keeps if with_forward else grad_copies(N_DEVICES - 2) + grad_copies(N_DEVICES - 1):
        item.wait()
    gather.finish()
    u_gather.finish(0)
    writer.finish()
    keep_dqkv.wait()
    for shard in range(N_DEVICES):
        pltpu.make_async_copy(u_full.at[shard], u_full_hbm.at[shard], u_sems.at[shard]).wait()


def middle(dy_loc, u_loc, w_out, w_down, gate_act, up_act, tables, qkv, attended, layer, tp_size):
    rows, width = dy_loc.shape
    seq_len = rows * tp_size
    o_cols, ff_cols, qkv_cols = width_of(w_out), width_of(w_down), width_of(qkv)
    n_heads = o_cols // HEAD_DIM
    total = o_cols + ff_cols
    outs = [(seq_len, ff_cols), (seq_len, ff_cols), (seq_len, qkv_cols), (tp_size, rows, width)]
    outs += [(o_cols, width), (ff_cols, width)] if attended else [(tp_size, rows, width), (seq_len, o_cols), (seq_len, ff_cols)]
    scratch = [pltpu.VMEM((2, rows, ff_cols), BF16)] * 2
    scratch += [pltpu.VMEM((rows, ff_cols), BF16)] * 2
    scratch += [
        pltpu.VMEM((total, width), BF16),
        pltpu.VMEM((seq_len, qkv_cols), BF16),
        pltpu.VMEM((seq_len, o_cols), BF16),
        pltpu.VMEM((seq_len, o_cols), F32),
        pltpu.VMEM((seq_len, ff_cols), BF16),
        pltpu.VMEM((seq_len, o_cols), BF16),
        pltpu.VMEM((seq_len, qkv_cols), BF16),
        pltpu.VMEM((n_heads, HEAD_DIM, seq_len), F32),
        pltpu.VMEM((n_heads, HEAD_DIM, seq_len), F32),
        pltpu.VMEM((Q_ROWS, seq_len), BF16),
        pltpu.VMEM((Q_ROWS, seq_len), BF16),
        pltpu.VMEM((2, total, width // (N_DEVICES)), BF16),
    ]
    scratch += [pltpu.VMEM(table.shape, F32) for table in tables]
    scratch += gather_scratch(tp_size, rows, width) + gather_scratch(tp_size, rows, width)
    scratch += [
        dma_sems(9),
        dma_sems(2, 2, 2),
        dma_sems(2, 2),
        dma_sems(tp_size),
        pltpu.SemaphoreType.DMA,
        dma_sems(2, 2),
    ]
    return pl.pallas_call(
        functools.partial(middle_kernel, layer, not attended),
        out_shape=[jax.ShapeDtypeStruct(shape, BF16) for shape in outs],
        in_specs=[ANY] * (9 + len(attended)),
        out_specs=[ANY] * len(outs),
        scratch_shapes=scratch,
        compiler_params=params(collective_id=3 + layer),
        name=f'middle_{layer}',
    )(dy_loc, u_loc, w_out, w_down, gate_act, up_act, *tables, qkv, *attended)


def solution(mesh):
    tp_size = mesh.shape['tp']
    assert tp_size == N_DEVICES
    row_spec = P(('dp', 'tp'), None)
    col_spec = P(None, None, 'tp')
    inner_spec = P(None, 'tp', None)

    def device_program(x_loc, dy_loc, norm_gain, w_qkv, w_out, w_gate, w_up, w_down):
        n_layers = height(w_qkv)
        seq_len = height(x_loc) * tp_size
        tables = tuple(jnp.asarray(table) for table in rope_tables(seq_len, FINE))
        assert n_layers == 2
        qkv, gate_act, up_act, hidden, u_loc, *tables = project(x_loc, norm_gain, w_qkv, w_gate, w_up, tables, 0, tp_size)
        y_loc, u_next, attn_out, lse, *projected = block_rest(qkv, hidden, w_out, w_down, x_loc, norm_gain, w_qkv, w_gate, w_up, tables, 0, tp_size)
        saved = ((x_loc, u_loc, qkv, gate_act, up_act, (attn_out, lse)), (y_loc, u_next, *projected, ()))
        grad_cur = dy_loc
        grads, gains = [None] * n_layers, ()
        for layer in reversed(range(n_layers)):
            x_cur, u_loc, qkv, gate_act, up_act, attended = saved[layer]
            d_gate, d_up, d_qkv, u_full, *more = middle(grad_cur, u_loc, w_out, w_down, gate_act, up_act, tables, qkv, attended, layer, tp_size)
            u_full = u_full.reshape(seq_len, u_full.shape[2])
            later_gains = jnp.concatenate(gains, axis=0) if gains else None
            grad_cur, gain_grad, g_qkv, g_gate, g_up = block_input_backward(
                d_qkv, d_gate, d_up, w_qkv, w_gate, w_up, u_full, x_cur, grad_cur, norm_gain, later_gains, layer
            )
            grads[layer] = (g_qkv, g_gate, g_up)
            if layer == n_layers - 1:
                dy_full, attn_out, hidden = more
            gains = (gain_grad,) + gains
        grad_x, g_out, g_down, g_qkv, g_gate, g_up = collect(grad_cur, dy_full.reshape(seq_len, -1), attn_out, hidden, *more, list(zip(*grads)), 8)
        return (grad_x, gains[0], g_qkv, g_out, g_gate, g_up, g_down)

    return jax.shard_map(
        device_program,
        mesh=mesh,
        in_specs=(row_spec, row_spec, P(None, None), col_spec, inner_spec, col_spec, col_spec, inner_spec),
        out_specs=(row_spec, P('dp', None), P('dp', None, 'tp'), P('dp', 'tp', None), P('dp', None, 'tp'), P('dp', None, 'tp'), P('dp', 'tp', None)),
        check_vma=False,
    )
```
